8 devices in a mesh: data: 1 (over z), tp: 8 (over y, x, core).
Axes of the slice: x: 2, y: 2, z: 1, core: 2. Of those that a mesh axis runs over, the one named last changes fastest.
Arguments:
- x_in: bfloat16 [8192, 2048], P('data')
- w_gate: bfloat16 [2048, 8192], P(None, 'tp')
- w_up: bfloat16 [2048, 8192], P(None, 'tp')
- w_down: bfloat16 [8192, 2048], P('tp')
- residual: bfloat16 [8192, 2048], P(('data', 'tp'))
- norm_gain: float32 [2048], replicated
Outputs:
- output 1: bfloat16 [8192, 2048], P(('data', 'tp'))
- output 2: bfloat16 [8192, 2048], P(('data', 'tp'))
All inputs are finite; a program needn't handle non-finite values.
Results may differ from the reference program's by a relative error of at most 0.00647001.
Values are sent between devices in bfloat16 or wider.
A program may use at most 1 GiB of HBM per device.

```python
import jax
import jax.numpy as jnp
from jax import lax

T = 8192
D = 2048
F = 8192
TP = 8
F_SHARD = F // TP
EPS = 1e-5


def setup_inputs(seed: int = 0, part: int = 0) -> dict:
    key = jax.random.key(seed)
    shared = jax.random.split(key, 4)
    local = jax.random.split(jax.random.fold_in(key, part), 2)
    x_in = jax.random.normal(local[0], (T, D), jnp.float32).astype(jnp.bfloat16)
    residual = jax.random.normal(local[1], (T, D), jnp.float32).astype(jnp.bfloat16)
    w_gate = (jax.random.normal(shared[0], (D, F), jnp.float32) * D ** -0.5).astype(jnp.bfloat16)
    w_up = (jax.random.normal(shared[1], (D, F), jnp.float32) * D ** -0.5).astype(jnp.bfloat16)
    w_down = (jax.random.normal(shared[2], (F, D), jnp.float32) * (2.0 / F) ** 0.5).astype(jnp.bfloat16)
    norm_gain = 1.0 + 0.3 * jax.random.normal(shared[3], (D,), jnp.float32)
    return {"x_in": x_in, "w_gate": w_gate, "w_up": w_up, "w_down": w_down, "residual": residual, "norm_gain": norm_gain}


def reference(x_in, w_gate, w_up, w_down, residual, norm_gain):
    gate_shards = w_gate.reshape(D, TP, F_SHARD).transpose(1, 0, 2)
    up_shards = w_up.reshape(D, TP, F_SHARD).transpose(1, 0, 2)
    down_shards = w_down.reshape(TP, F_SHARD, D)

    def add_shard(running, shard_w):
        gate_cols, up_cols, down_rows = shard_w
        gate_val = jnp.dot(x_in, gate_cols, preferred_element_type=jnp.float32)
        up_val = jnp.dot(x_in, up_cols, preferred_element_type=jnp.float32)
        hidden = (jax.nn.silu(gate_val) * up_val).astype(jnp.bfloat16)
        part_prod = jnp.dot(hidden, down_rows, preferred_element_type=jnp.float32).astype(jnp.bfloat16)
        return running + part_prod.astype(jnp.float32), None

    y_sum = lax.scan(add_shard, jnp.zeros((T, D), jnp.float32), (gate_shards, up_shards, down_shards))[0]
    hidden_sum = residual.astype(jnp.float32) + y_sum
    mean_sq = jnp.mean(hidden_sum * hidden_sum, axis=-1, keepdims=True)
    normed = hidden_sum * lax.rsqrt(mean_sq + EPS) * norm_gain
    return hidden_sum.astype(jnp.bfloat16), normed.astype(jnp.bfloat16)
```

```python
import functools

import jax
import jax.numpy as jnp
from jax import lax
from jax.experimental import pallas as pl
from jax.experimental.pallas import tpu as pltpu
from jax.sharding import PartitionSpec as P

EPS = 1e-5
ROWS = 256
HALF = 128
BLOCK = 1024
STEPS = BLOCK // ROWS
D = 2048
F = 1024
RELAY_SLOTS = 5
SUM_SLOTS = 3
FIRST = 2 * STEPS
SECOND = 4 * STEPS
TILES = 8 * STEPS


def kernel(x_hbm, wg_hbm, wu_hbm, wd_hbm, res_hbm, gain_ref, h_hbm, n_hbm, sum_in, x_buf, wg, wu, wd, hid, tiles, relay_in, sib_in, sum_out, sum_ld, res_ld, h_out, n_out,
           x_sem, w_sem, relay_ssem, relay_rsem, sib_ssem, sib_rsem, sum_ssem, sum_rsem, ld_sem, res_sem, out_sem):
    me = lax.axis_index("tp")
    c, cx, cy = me % 2, (me // 2) % 2, me // 4
    sib = cy * 4 + cx * 2 + (1 - c)
    xn = cy * 4 + (1 - cx) * 2
    yn = (1 - cy) * 4 + cx * 2

    barrier = pltpu.get_barrier_semaphore()
    for dev in (sib, xn, xn + 1, yn, yn + 1):
        pl.semaphore_signal(barrier, inc=1, device_id={"tp": dev}, device_id_type=pl.DeviceIdType.MESH)

    def row_of(i):
        first = 1 - (i + TILES - FIRST) // TILES
        last = (i + FIRST) // TILES
        mid = 1 - first - last
        p = i - FIRST
        q = p % 4
        direction = q % 2
        r = i - FIRST - SECOND
        ty = first * (1 - cy) + mid * (cy + direction * (1 - 2 * cy)) + last * cy
        tx = first * (1 - cx) + mid * (cx + (1 - direction) * (1 - 2 * cx)) + last * cx
        tc = first * (i % 2) + mid * ((1 - c) + (q // 2) * (2 * c - 1)) + last * ((1 - c) + ((r + TILES) // STEPS - TILES // STEPS) * (2 * c - 1))
        k = first * (i // 2) + mid * (p // 4) + last * (i % STEPS)
        return pl.multiple_of((ty * 4 + tx * 2 + tc) * BLOCK + k * ROWS, ROWS)

    def x_copy(i):
        return pltpu.make_async_copy(x_hbm.at[pl.ds(row_of(i), ROWS)], x_buf.at[i % 2], x_sem.at[i % 2])

    def w_copies():
        return [pltpu.make_async_copy(src, dst, w_sem.at[j]) for j, (src, dst) in enumerate(((wg_hbm, wg), (wu_hbm, wu), (wd_hbm, wd)))]

    x_copy(0).start()
    for copy in w_copies():
        copy.start()

    def relay_copy(i):
        via = (1 - c) * xn + c * yn + i % 2
        return pltpu.make_async_remote_copy(
            src_ref=tiles.at[i % RELAY_SLOTS], dst_ref=relay_in.at[1 - c, i // 2], send_sem=relay_ssem.at[i % RELAY_SLOTS],
            recv_sem=relay_rsem.at[1 - c, i // 2], device_id={"tp": via}, device_id_type=pl.DeviceIdType.MESH)

    def relay_arrival(group, k):
        return pltpu.make_async_remote_copy(
            src_ref=relay_in.at[group, k], dst_ref=relay_in.at[group, k], send_sem=relay_ssem.at[0],
            recv_sem=relay_rsem.at[group, k], device_id={"tp": sib}, device_id_type=pl.DeviceIdType.MESH)

    def sib_copy(slot, group, k):
        return pltpu.make_async_remote_copy(
            src_ref=tiles.at[RELAY_SLOTS + slot], dst_ref=sib_in.at[group, k], send_sem=sib_ssem.at[slot],
            recv_sem=sib_rsem.at[group, k], device_id={"tp": sib}, device_id_type=pl.DeviceIdType.MESH)

    def sum_copy(direction, k, half):
        slot = k % SUM_SLOTS
        to = (1 - direction) * xn + direction * yn + c
        return pltpu.make_async_remote_copy(
            src_ref=sum_out.at[direction, slot, pl.ds(half * HALF, HALF)], dst_ref=sum_in.at[direction, k, half],
            send_sem=sum_ssem.at[direction, slot, half], recv_sem=sum_rsem.at[direction, k, half],
            device_id={"tp": to}, device_id_type=pl.DeviceIdType.MESH)

    def ffn(x_ref, out_ref):
        for n in range(F // 256):
            cols = slice(n * 256, (n + 1) * 256)
            gate = jnp.dot(x_ref[...], wg[:, cols], preferred_element_type=jnp.float32)
            up = jnp.dot(x_ref[...], wu[:, cols], preferred_element_type=jnp.float32)
            hid[:, cols] = (gate * jax.nn.sigmoid(gate) * up).astype(jnp.bfloat16)
        for n in range(D // 512):
            cols = slice(n * 512, (n + 1) * 512)
            out_ref[:, cols] = jnp.dot(hid[...], wd[:, cols], preferred_element_type=jnp.float32).astype(jnp.bfloat16)

    for copy in w_copies():
        copy.wait()
    pl.semaphore_wait(barrier, 5)

    @pl.loop(0, TILES)
    def _(i):
        first = 1 - (i + TILES - FIRST) // TILES
        last = (i + FIRST) // TILES
        mid = 1 - first - last
        p = i - FIRST
        q = p % 4
        direction = q % 2
        k_mid = p // 4
        k_last = i % STEPS
        is_relay = i < FIRST
        is_sib = jnp.logical_and(i >= FIRST, jnp.logical_and(i < FIRST + SECOND, q < 2))
        is_sum = jnp.logical_and(i >= FIRST, jnp.logical_and(i < FIRST + SECOND, q >= 2))
        is_own_sib = jnp.logical_and(i >= FIRST + SECOND, i < FIRST + SECOND + STEPS)
        is_final = i >= FIRST + SECOND + STEPS
        sending = mid * (q // 2) + last * ((i - FIRST - SECOND + TILES) // STEPS - TILES // STEPS)
        slot = first * (i % RELAY_SLOTS) + (1 - first) * (RELAY_SLOTS + sending * 2 + (1 - sending) * (i % 2))

        @pl.when(i + 1 < TILES)
        def _():
            x_copy(i + 1).start()

        x_copy(i).wait()

        @pl.when(jnp.logical_and(is_relay, i >= RELAY_SLOTS))
        def _():
            relay_copy(i - RELAY_SLOTS).wait_send()

        @pl.when(jnp.logical_and(jnp.logical_or(is_sib, is_own_sib), i >= FIRST + 4))
        def _():
            sib_copy(i % 2, 0, 0).wait_send()

        @pl.when(is_final)
        def _():
            pltpu.make_async_copy(res_hbm.at[pl.ds(pl.multiple_of(k_last * ROWS, ROWS), ROWS)], res_ld, res_sem).start()

        ffn(x_buf.at[i % 2], tiles.at[slot])

        @pl.when(is_relay)
        def _():
            relay_copy(i).start()

        @pl.when(is_sib)
        def _():
            sib_copy(i % 2, direction, k_mid).start()

        @pl.when(is_own_sib)
        def _():
            sib_copy(i % 2, 2, k_last).start()

        @pl.when(is_sum)
        def _():
            sib_copy(0, direction, k_mid).wait_recv()
            relay_arrival(direction, k_mid).wait_recv()

            @pl.when(k_mid >= SUM_SLOTS)
            def _():
                for half in range(2):
                    sum_copy(direction, k_mid - SUM_SLOTS, half).wait_send()

            for half in range(2):
                @pl.loop(0, HALF // 16)
                def _(b):
                    rows = pl.ds(pl.multiple_of(half * HALF + b * 16, 16), 16)
                    total = tiles[RELAY_SLOTS + 2, rows].astype(jnp.float32) + sib_in[direction, k_mid, rows].astype(jnp.float32)
                    sum_out[direction, k_mid % SUM_SLOTS, rows] = total + relay_in[direction, k_mid, rows].astype(jnp.float32)

                sum_copy(direction, k_mid, half).start()

        @pl.when(is_final)
        def _():
            sib_copy(0, 2, k_last).wait_recv()
            pltpu.make_async_copy(res_hbm.at[pl.ds(0, ROWS)], res_ld, res_sem).wait()
            for half in range(2):
                for d in range(2):
                    sum_copy(d, k_last, half).wait_recv()
                loads = [pltpu.make_async_copy(sum_in.at[d, k_last, half], sum_ld.at[d], ld_sem.at[d]) for d in range(2)]
                for load in loads:
                    load.start()

                def stores(k):
                    rows = pl.ds(pl.multiple_of(k * ROWS + half * HALF, HALF), HALF)
                    return [pltpu.make_async_copy(h_out.at[half], h_hbm.at[rows], out_sem.at[half, 0]),
                            pltpu.make_async_copy(n_out.at[half], n_hbm.at[rows], out_sem.at[half, 1])]

                @pl.when(k_last > 0)
                def _():
                    for store in stores(k_last - 1):
                        store.wait()

                for load in loads:
                    load.wait()

                @pl.loop(0, HALF // 16)
                def _(b):
                    here = pl.ds(pl.multiple_of(b * 16, 16), 16)
                    rows = pl.ds(pl.multiple_of(half * HALF + b * 16, 16), 16)
                    y_sum = tiles[RELAY_SLOTS + 2, rows].astype(jnp.float32) + sib_in[2, k_last, rows].astype(jnp.float32)
                    y_sum = y_sum + (sum_ld[0, here] + sum_ld[1, here])
                    h = res_ld[rows].astype(jnp.float32) + y_sum
                    mean_sq = jnp.mean(h * h, axis=-1, keepdims=True)
                    h_out[half, here] = h.astype(jnp.bfloat16)
                    n_out[half, here] = (h * lax.rsqrt(mean_sq + EPS) * gain_ref[...]).astype(jnp.bfloat16)

                for store in stores(k_last):
                    store.start()

    for s in range(RELAY_SLOTS):
        relay_copy(FIRST - RELAY_SLOTS + s).wait_send()
    for s in range(2):
        sib_copy(s, 0, 0).wait_send()
    for d in range(2):
        for k in range(STEPS - SUM_SLOTS, STEPS):
            for half in range(2):
                sum_copy(d, k, half).wait_send()
    for half in range(2):
        rows = pl.ds((STEPS - 1) * ROWS + half * HALF, HALF)
        pltpu.make_async_copy(h_out.at[half], h_hbm.at[rows], out_sem.at[half, 0]).wait()
        pltpu.make_async_copy(n_out.at[half], n_hbm.at[rows], out_sem.at[half, 1]).wait()


def solution(mesh):
    def local_block(x_in, w_gate, w_up, w_down, residual, norm_gain):
        hbm = pl.BlockSpec(memory_space=pltpu.HBM)
        h, n, _ = pl.pallas_call(
            kernel,
            out_shape=(
                jax.ShapeDtypeStruct((BLOCK, D), jnp.bfloat16),
                jax.ShapeDtypeStruct((BLOCK, D), jnp.bfloat16),
                jax.ShapeDtypeStruct((2, STEPS, 2, HALF, D), jnp.float32),
            ),
            in_specs=[hbm] * 5 + [pl.BlockSpec(memory_space=pltpu.VMEM)],
            out_specs=(hbm, hbm, hbm),
            scratch_shapes=[
                pltpu.VMEM((2, ROWS, D), jnp.bfloat16),
                pltpu.VMEM((D, F), jnp.bfloat16),
                pltpu.VMEM((D, F), jnp.bfloat16),
                pltpu.VMEM((F, D), jnp.bfloat16),
                pltpu.VMEM((ROWS, F), jnp.bfloat16),
                pltpu.VMEM((RELAY_SLOTS + 3, ROWS, D), jnp.bfloat16),
                pltpu.VMEM((2, STEPS, ROWS, D), jnp.bfloat16),
                pltpu.VMEM((3, STEPS, ROWS, D), jnp.bfloat16),
                pltpu.VMEM((2, SUM_SLOTS, ROWS, D), jnp.float32),
                pltpu.VMEM((2, HALF, D), jnp.float32),
                pltpu.VMEM((ROWS, D), jnp.bfloat16),
                pltpu.VMEM((2, HALF, D), jnp.bfloat16),
                pltpu.VMEM((2, HALF, D), jnp.bfloat16),
                pltpu.SemaphoreType.DMA((2,)),
                pltpu.SemaphoreType.DMA((3,)),
                pltpu.SemaphoreType.DMA((RELAY_SLOTS,)),
                pltpu.SemaphoreType.DMA((2, STEPS)),
                pltpu.SemaphoreType.DMA((2,)),
                pltpu.SemaphoreType.DMA((3, STEPS)),
                pltpu.SemaphoreType.DMA((2, SUM_SLOTS, 2)),
                pltpu.SemaphoreType.DMA((2, STEPS, 2)),
                pltpu.SemaphoreType.DMA((2,)),
                pltpu.SemaphoreType.DMA,
                pltpu.SemaphoreType.DMA((2, 2)),
            ],
            compiler_params=pltpu.CompilerParams(collective_id=0, has_side_effects=True, vmem_limit_bytes=67000000),
            name="mlp_reduce",
        )(x_in, w_gate, w_up, w_down, residual, norm_gain.reshape(1, D))
        return h, n

    row_spec = P(("data", "tp"), None)
    return jax.shard_map(local_block, mesh=mesh, in_specs=(P("data", None), P(None, "tp"), P(None, "tp"), P("tp", None), row_spec, P(None)), out_specs=(row_spec, row_spec), check_vma=False)
```

```python
import functools

import jax
import jax.numpy as jnp
from jax import lax
from jax.experimental import pallas as pl
from jax.experimental.pallas import tpu as pltpu
from jax.sharding import PartitionSpec as P

EPS = 1e-5
ROWS = 256
CHUNKS = 4
COLS = (256, 256, 512)
HALF = 128
BLOCK = 1024
STEPS = BLOCK // ROWS
D = 2048
F = 1024
RELAY_SLOTS = 3
SUM_SLOTS = 2
FIRST = 2 * STEPS
SECOND = 4 * STEPS
TILES = 8 * STEPS


def kernel(x_hbm, wg_hbm, wu_hbm, wd_hbm, res_hbm, gain_ref, h_ref, n_ref, sum_in, x_buf, wg, wu, wd, hid, tiles, relay_in, sib_in, sum_out, sum_last, sum_ld, res_ld,
           x_sem, w_sem, relay_ssem, relay_rsem, sib_ssem, sib_rsem, sum_ssem, sum_rsem, ld_sem, res_sem):
    me = lax.axis_index("tp")
    c, cx, cy = me % 2, (me // 2) % 2, me // 4
    sib = cy * 4 + cx * 2 + (1 - c)
    xn = cy * 4 + (1 - cx) * 2
    yn = (1 - cy) * 4 + cx * 2

    barrier = pltpu.get_barrier_semaphore()
    for dev in (sib, xn, xn + 1, yn, yn + 1):
        pl.semaphore_signal(barrier, inc=1, device_id={"tp": dev}, device_id_type=pl.DeviceIdType.MESH)

    def row_of(i):
        first = 1 - (i + TILES - FIRST) // TILES
        last = (i + FIRST) // TILES
        mid = 1 - first - last
        p = i - FIRST
        q = p % 4
        direction = q % 2
        r = i - FIRST - SECOND
        ty = first * (1 - cy) + mid * (cy + direction * (1 - 2 * cy)) + last * cy
        tx = first * (1 - cx) + mid * (cx + (1 - direction) * (1 - 2 * cx)) + last * cx
        tc = first * (i % 2) + mid * ((1 - c) + (q // 2) * (2 * c - 1)) + last * ((1 - c) + ((r + TILES) // STEPS - TILES // STEPS) * (2 * c - 1))
        k = first * (i // 2) + mid * (p // 4) + last * (i % STEPS)
        return pl.multiple_of((ty * 4 + tx * 2 + tc) * BLOCK + k * ROWS, ROWS)

    def x_copy(i):
        return pltpu.make_async_copy(x_hbm.at[pl.ds(row_of(i), ROWS)], x_buf.at[i % 2], x_sem.at[i % 2])

    def w_copy(j, n):
        src, dst = ((wg_hbm, wg), (wu_hbm, wu), (wd_hbm, wd))[j]
        cols = pl.ds(n * COLS[j], COLS[j])
        return pltpu.make_async_copy(src.at[:, cols], dst.at[:, cols], w_sem.at[j, n])

    x_copy(0).start()
    for n in range(CHUNKS):
        w_copy(0, n).start()
        w_copy(1, n).start()
    for n in range(CHUNKS):
        w_copy(2, n).start()
    x_copy(1).start()

    def relay_copy(i):
        via = (1 - c) * xn + c * yn + i % 2
        return pltpu.make_async_remote_copy(
            src_ref=tiles.at[i % RELAY_SLOTS], dst_ref=relay_in.at[1 - c, i // 2], send_sem=relay_ssem.at[i % RELAY_SLOTS],
            recv_sem=relay_rsem.at[1 - c, i // 2], device_id={"tp": via}, device_id_type=pl.DeviceIdType.MESH)

    def relay_arrival(group, k):
        return pltpu.make_async_remote_copy(
            src_ref=relay_in.at[group, k], dst_ref=relay_in.at[group, k], send_sem=relay_ssem.at[0],
            recv_sem=relay_rsem.at[group, k], device_id={"tp": sib}, device_id_type=pl.DeviceIdType.MESH)

    def sib_copy(slot, group, k):
        return pltpu.make_async_remote_copy(
            src_ref=tiles.at[RELAY_SLOTS + slot], dst_ref=sib_in.at[group, k], send_sem=sib_ssem.at[slot],
            recv_sem=sib_rsem.at[group, k], device_id={"tp": sib}, device_id_type=pl.DeviceIdType.MESH)

    def sum_copy(direction, k, half, in_vmem=False):
        slot = k % SUM_SLOTS
        to = (1 - direction) * xn + direction * yn + c
        return pltpu.make_async_remote_copy(
            src_ref=sum_out.at[direction, slot, pl.ds(half * HALF, HALF)], dst_ref=sum_last.at[direction] if in_vmem else sum_in.at[direction, k, half],
            send_sem=sum_ssem.at[direction, slot, half], recv_sem=sum_rsem.at[direction, k, half],
            device_id={"tp": to}, device_id_type=pl.DeviceIdType.MESH)

    def ffn(x_ref, out_ref, loading=False):
        for n in range(CHUNKS):
            cols = slice(n * COLS[0], (n + 1) * COLS[0])
            if loading:
                w_copy(0, n).wait()
                w_copy(1, n).wait()
            gate = jnp.dot(x_ref[...], wg[:, cols], preferred_element_type=jnp.float32)
            up = jnp.dot(x_ref[...], wu[:, cols], preferred_element_type=jnp.float32)
            hid[:, cols] = (gate * jax.nn.sigmoid(gate) * up).astype(jnp.bfloat16)
        for n in range(CHUNKS):
            cols = slice(n * COLS[2], (n + 1) * COLS[2])
            if loading:
                w_copy(2, n).wait()
            out_ref[:, cols] = jnp.dot(hid[...], wd[:, cols], preferred_element_type=jnp.float32).astype(jnp.bfloat16)

    x_copy(0).wait()
    ffn(x_buf.at[0], tiles.at[0], loading=True)
    pl.semaphore_wait(barrier, 5)
    relay_copy(0).start()

    @pl.loop(1, TILES)
    def _(i):
        first = 1 - (i + TILES - FIRST) // TILES
        last = (i + FIRST) // TILES
        mid = 1 - first - last
        p = i - FIRST
        q = p % 4
        direction = q % 2
        k_mid = p // 4
        k_last = i % STEPS
        is_relay = i < FIRST
        is_sib = jnp.logical_and(i >= FIRST, jnp.logical_and(i < FIRST + SECOND, q < 2))
        is_sum = jnp.logical_and(i >= FIRST, jnp.logical_and(i < FIRST + SECOND, q >= 2))
        is_own_sib = jnp.logical_and(i >= FIRST + SECOND, i < FIRST + SECOND + STEPS)
        is_final = i >= FIRST + SECOND + STEPS
        sending = mid * (q // 2) + last * ((i - FIRST - SECOND + TILES) // STEPS - TILES // STEPS)
        slot = first * (i % RELAY_SLOTS) + (1 - first) * (RELAY_SLOTS + sending * 2 + (1 - sending) * (i % 2))

        @pl.when(i + 1 < TILES)
        def _():
            x_copy(i + 1).start()

        x_copy(i).wait()

        @pl.when(jnp.logical_and(is_relay, i >= RELAY_SLOTS))
        def _():
            relay_copy(i - RELAY_SLOTS).wait_send()

        @pl.when(jnp.logical_and(jnp.logical_or(is_sib, is_own_sib), i >= FIRST + 4))
        def _():
            sib_copy(i % 2, 0, 0).wait_send()

        @pl.when(is_final)
        def _():
            pltpu.make_async_copy(res_hbm.at[pl.ds(pl.multiple_of(k_last * ROWS, ROWS), ROWS)], res_ld, res_sem).start()

        ffn(x_buf.at[i % 2], tiles.at[slot])

        @pl.when(is_relay)
        def _():
            relay_copy(i).start()

        @pl.when(is_sib)
        def _():
            sib_copy(i % 2, direction, k_mid).start()

        @pl.when(is_own_sib)
        def _():
            sib_copy(i % 2, 2, k_last).start()

        @pl.when(is_sum)
        def _():
            sib_copy(0, direction, k_mid).wait_recv()
            relay_arrival(direction, k_mid).wait_recv()

            @pl.when(k_mid >= SUM_SLOTS)
            def _():
                for half in range(2):
                    sum_copy(direction, k_mid - SUM_SLOTS, half).wait_send()

            for half in range(2):
                @pl.loop(0, HALF // 16)
                def _(b):
                    rows = pl.ds(pl.multiple_of(half * HALF + b * 16, 16), 16)
                    total = tiles[RELAY_SLOTS + 2, rows].astype(jnp.float32) + sib_in[direction, k_mid, rows].astype(jnp.float32)
                    sum_out[direction, k_mid % SUM_SLOTS, rows] = total + relay_in[direction, k_mid, rows].astype(jnp.float32)

                if half == 0:
                    sum_copy(direction, k_mid, half).start()
                else:
                    @pl.when(k_mid < STEPS - 1)
                    def _():
                        sum_copy(direction, k_mid, 1).start()

                    @pl.when(k_mid == STEPS - 1)
                    def _():
                        sum_copy(direction, k_mid, 1, in_vmem=True).start()

        @pl.when(is_final)
        def _():
            sib_copy(0, 2, k_last).wait_recv()
            pltpu.make_async_copy(res_hbm.at[pl.ds(0, ROWS)], res_ld, res_sem).wait()
            def finish(half, sums):
                @pl.loop(0, HALF // 16)
                def _(b):
                    here = pl.ds(pl.multiple_of(b * 16, 16), 16)
                    rows = pl.ds(pl.multiple_of(half * HALF + b * 16, 16), 16)
                    out = pl.ds(pl.multiple_of(k_last * ROWS + half * HALF + b * 16, 16), 16)
                    y_sum = tiles[RELAY_SLOTS + 2, rows].astype(jnp.float32) + sib_in[2, k_last, rows].astype(jnp.float32)
                    y_sum = y_sum + (sums[0, here] + sums[1, here])
                    h = res_ld[rows].astype(jnp.float32) + y_sum
                    mean_sq = jnp.mean(h * h, axis=-1, keepdims=True)
                    h_ref[out] = h.astype(jnp.bfloat16)
                    n_ref[out] = (h * lax.rsqrt(mean_sq + EPS) * gain_ref[...]).astype(jnp.bfloat16)

            def finish_hbm(half):
                loads = [pltpu.make_async_copy(sum_in.at[d, k_last, half], sum_ld.at[d], ld_sem.at[d]) for d in range(2)]
                for d in range(2):
                    sum_copy(d, k_last, half).wait_recv()
                    loads[d].start()
                for load in loads:
                    load.wait()
                finish(half, sum_ld)

            finish_hbm(0)

            @pl.when(k_last < STEPS - 1)
            def _():
                finish_hbm(1)

            @pl.when(k_last == STEPS - 1)
            def _():
                for d in range(2):
                    sum_copy(d, STEPS - 1, 1, in_vmem=True).wait_recv()
                finish(1, sum_last)

    for s in range(RELAY_SLOTS):
        relay_copy(FIRST - RELAY_SLOTS + s).wait_send()
    for s in range(2):
        sib_copy(s, 0, 0).wait_send()
    for d in range(2):
        for k in range(STEPS - SUM_SLOTS, STEPS):
            for half in range(2):
                sum_copy(d, k, half).wait_send()

def store_kernel(h_ref, n_ref, h_hbm, n_hbm, sem):
    copies = []
    for b in range(4):
        rows = pl.ds(b * (BLOCK // 4), BLOCK // 4)
        copies.append(pltpu.make_async_copy(h_ref.at[rows], h_hbm.at[rows], sem.at[0, b]))
        copies.append(pltpu.make_async_copy(n_ref.at[rows], n_hbm.at[rows], sem.at[1, b]))
    for copy in copies:
        copy.start()
    for copy in copies:
        copy.wait()


def solution(mesh):
    def local_block(x_in, w_gate, w_up, w_down, residual, norm_gain):
        hbm = pl.BlockSpec(memory_space=pltpu.HBM)
        vmem = pl.BlockSpec(memory_space=pltpu.VMEM)
        h, n, _ = pl.pallas_call(
            kernel,
            out_shape=(
                pltpu.VMEM((BLOCK, D), jnp.bfloat16),
                pltpu.VMEM((BLOCK, D), jnp.bfloat16),
                jax.ShapeDtypeStruct((2, STEPS, 2, HALF, D), jnp.float32),
            ),
            in_specs=[hbm] * 5 + [vmem],
            out_specs=(vmem, vmem, hbm),
            scratch_shapes=[
                pltpu.VMEM((2, ROWS, D), jnp.bfloat16),
                pltpu.VMEM((D, F), jnp.bfloat16),
                pltpu.VMEM((D, F), jnp.bfloat16),
                pltpu.VMEM((F, D), jnp.bfloat16),
                pltpu.VMEM((ROWS, F), jnp.bfloat16),
                pltpu.VMEM((RELAY_SLOTS + 3, ROWS, D), jnp.bfloat16),
                pltpu.VMEM((2, STEPS, ROWS, D), jnp.bfloat16),
                pltpu.VMEM((3, STEPS, ROWS, D), jnp.bfloat16),
                pltpu.VMEM((2, SUM_SLOTS, ROWS, D), jnp.float32),
                pltpu.VMEM((2, HALF, D), jnp.float32),
                pltpu.VMEM((2, HALF, D), jnp.float32),
                pltpu.VMEM((ROWS, D), jnp.bfloat16),
                pltpu.SemaphoreType.DMA((2,)),
                pltpu.SemaphoreType.DMA((3, CHUNKS)),
                pltpu.SemaphoreType.DMA((RELAY_SLOTS,)),
                pltpu.SemaphoreType.DMA((2, STEPS)),
                pltpu.SemaphoreType.DMA((2,)),
                pltpu.SemaphoreType.DMA((3, STEPS)),
                pltpu.SemaphoreType.DMA((2, SUM_SLOTS, 2)),
                pltpu.SemaphoreType.DMA((2, STEPS, 2)),
                pltpu.SemaphoreType.DMA((2,)),
                pltpu.SemaphoreType.DMA,
            ],
            compiler_params=pltpu.CompilerParams(collective_id=0, has_side_effects=True, vmem_limit_bytes=58000000),
            name="mlp_reduce",
        )(x_in, w_gate, w_up, w_down, residual, norm_gain.reshape(1, D))
        return pl.pallas_call(
            store_kernel,
            out_shape=(jax.ShapeDtypeStruct((BLOCK, D), jnp.bfloat16), jax.ShapeDtypeStruct((BLOCK, D), jnp.bfloat16)),
            in_specs=[vmem, vmem],
            out_specs=(hbm, hbm),
            scratch_shapes=[pltpu.SemaphoreType.DMA((2, 4))],
            compiler_params=pltpu.CompilerParams(vmem_limit_bytes=1048576),
            name="store",
        )(*(pltpu.with_memory_space_constraint(a, pltpu.VMEM) for a in (h, n)))

    row_spec = P(("data", "tp"), None)
    return jax.shard_map(local_block, mesh=mesh, in_specs=(P("data", None), P(None, "tp"), P(None, "tp"), P("tp", None), row_spec, P(None)), out_specs=(row_spec, row_spec), check_vma=False)
```

```python
import functools

import jax
import jax.numpy as jnp
from jax import lax
from jax.experimental import pallas as pl
from jax.experimental.pallas import tpu as pltpu
from jax.sharding import PartitionSpec as P

EPS = 1e-5
ROWS = 256
CHUNKS = 4
COLS = (256, 256, 512)
HALF = 128
BLOCK = 1024
STEPS = BLOCK // ROWS
D = 2048
F = 1024
RELAY_SLOTS = 3
SUM_SLOTS = 2
FIRST = 2 * STEPS
SECOND = 4 * STEPS
TILES = 8 * STEPS


def kernel(x_hbm, wg_hbm, wu_hbm, wd_hbm, res_hbm, gain_ref, h_ref, n_ref, sum_in, x_buf, wg, wu, wd, hid, tiles, relay_in, sib_in, sum_out, sum_last, sum_ld, res_ld,
           x_sem, w_sem, relay_ssem, relay_rsem, sib_ssem, sib_rsem, sum_ssem, sum_rsem, ld_sem, res_sem):
    me = lax.axis_index("tp")
    c, cx, cy = me % 2, (me // 2) % 2, me // 4
    sib = cy * 4 + cx * 2 + (1 - c)
    xn = cy * 4 + (1 - cx) * 2
    yn = (1 - cy) * 4 + cx * 2

    barrier = pltpu.get_barrier_semaphore()
    for dev in (sib, xn, xn + 1, yn, yn + 1):
        pl.semaphore_signal(barrier, inc=1, device_id={"tp": dev}, device_id_type=pl.DeviceIdType.MESH)

    def row_of(i):
        first = 1 - (i + TILES - FIRST) // TILES
        last = (i + FIRST) // TILES
        mid = 1 - first - last
        p = i - FIRST
        q = p % 4
        direction = q % 2
        r = i - FIRST - SECOND
        ty = first * (1 - cy) + mid * (cy + direction * (1 - 2 * cy)) + last * cy
        tx = first * (1 - cx) + mid * (cx + (1 - direction) * (1 - 2 * cx)) + last * cx
        tc = first * (i % 2) + mid * ((1 - c) + (q // 2) * (2 * c - 1)) + last * ((1 - c) + ((r + TILES) // STEPS - TILES // STEPS) * (2 * c - 1))
        k = first * (i // 2) + mid * (p // 4) + last * (i % STEPS)
        return pl.multiple_of((ty * 4 + tx * 2 + tc) * BLOCK + k * ROWS, ROWS)

    def x_copy(i):
        return pltpu.make_async_copy(x_hbm.at[pl.ds(row_of(i), ROWS)], x_buf.at[i % 2], x_sem.at[i % 2])

    def w_copy(j, n):
        src, dst = ((wg_hbm, wg), (wu_hbm, wu), (wd_hbm, wd))[j]
        cols = pl.ds(n * COLS[j], COLS[j])
        return pltpu.make_async_copy(src.at[:, cols], dst.at[:, cols], w_sem.at[j, n])

    x_copy(0).start()
    for n in range(CHUNKS):
        w_copy(0, n).start()
        w_copy(1, n).start()
    for n in range(CHUNKS):
        w_copy(2, n).start()
    x_copy(1).start()

    def relay_copy(i):
        k = i // 2
        turn = (k + c) % 2
        via = (1 - turn) * xn + turn * yn + i % 2
        return pltpu.make_async_remote_copy(
            src_ref=tiles.at[i % RELAY_SLOTS], dst_ref=relay_in.at[1 - turn, k], send_sem=relay_ssem.at[i % RELAY_SLOTS],
            recv_sem=relay_rsem.at[1 - turn, k], device_id={"tp": via}, device_id_type=pl.DeviceIdType.MESH)

    def relay_arrival(group, k):
        return pltpu.make_async_remote_copy(
            src_ref=relay_in.at[group, k], dst_ref=relay_in.at[group, k], send_sem=relay_ssem.at[0],
            recv_sem=relay_rsem.at[group, k], device_id={"tp": sib}, device_id_type=pl.DeviceIdType.MESH)

    def sib_copy(slot, group, k):
        return pltpu.make_async_remote_copy(
            src_ref=tiles.at[RELAY_SLOTS + slot], dst_ref=sib_in.at[group, k], send_sem=sib_ssem.at[slot],
            recv_sem=sib_rsem.at[group, k], device_id={"tp": sib}, device_id_type=pl.DeviceIdType.MESH)

    def sum_copy(direction, k, half, in_vmem=False):
        slot = k % SUM_SLOTS
        to = (1 - direction) * xn + direction * yn + c
        return pltpu.make_async_remote_copy(
            src_ref=sum_out.at[direction, slot, pl.ds(half * HALF, HALF)], dst_ref=sum_last.at[direction] if in_vmem else sum_in.at[direction, k, half],
            send_sem=sum_ssem.at[direction, slot, half], recv_sem=sum_rsem.at[direction, k, half],
            device_id={"tp": to}, device_id_type=pl.DeviceIdType.MESH)

    def ffn(x_ref, out_ref, loading=False):
        for n in range(CHUNKS):
            cols = slice(n * COLS[0], (n + 1) * COLS[0])
            if loading:
                w_copy(0, n).wait()
                w_copy(1, n).wait()
            gate = jnp.dot(x_ref[...], wg[:, cols], preferred_element_type=jnp.float32)
            up = jnp.dot(x_ref[...], wu[:, cols], preferred_element_type=jnp.float32)
            hid[:, cols] = (gate * jax.nn.sigmoid(gate) * up).astype(jnp.bfloat16)
        for n in range(CHUNKS):
            cols = slice(n * COLS[2], (n + 1) * COLS[2])
            if loading:
                w_copy(2, n).wait()
            out_ref[:, cols] = jnp.dot(hid[...], wd[:, cols], preferred_element_type=jnp.float32).astype(jnp.bfloat16)

    x_copy(0).wait()
    ffn(x_buf.at[0], tiles.at[0], loading=True)
    pl.semaphore_wait(barrier, 5)
    relay_copy(0).start()

    @pl.loop(1, TILES)
    def _(i):
        first = 1 - (i + TILES - FIRST) // TILES
        last = (i + FIRST) // TILES
        mid = 1 - first - last
        p = i - FIRST
        q = p % 4
        direction = q % 2
        k_mid = p // 4
        k_last = i % STEPS
        is_relay = i < FIRST
        is_sib = jnp.logical_and(i >= FIRST, jnp.logical_and(i < FIRST + SECOND, q < 2))
        is_sum = jnp.logical_and(i >= FIRST, jnp.logical_and(i < FIRST + SECOND, q >= 2))
        is_own_sib = jnp.logical_and(i >= FIRST + SECOND, i < FIRST + SECOND + STEPS)
        is_final = i >= FIRST + SECOND + STEPS
        sending = mid * (q // 2) + last * ((i - FIRST - SECOND + TILES) // STEPS - TILES // STEPS)
        slot = first * (i % RELAY_SLOTS) + (1 - first) * (RELAY_SLOTS + sending * 2 + (1 - sending) * (i % 2))

        @pl.when(i + 1 < TILES)
        def _():
            x_copy(i + 1).start()

        x_copy(i).wait()

        @pl.when(jnp.logical_and(is_relay, i >= RELAY_SLOTS))
        def _():
            relay_copy(i - RELAY_SLOTS).wait_send()

        @pl.when(jnp.logical_and(jnp.logical_or(is_sib, is_own_sib), i >= FIRST + 4))
        def _():
            sib_copy(i % 2, 0, 0).wait_send()

        @pl.when(is_final)
        def _():
            pltpu.make_async_copy(res_hbm.at[pl.ds(pl.multiple_of(k_last * ROWS, ROWS), ROWS)], res_ld, res_sem).start()

        ffn(x_buf.at[i % 2], tiles.at[slot])

        @pl.when(is_relay)
        def _():
            relay_copy(i).start()

        @pl.when(is_sib)
        def _():
            sib_copy(i % 2, direction, k_mid).start()

        @pl.when(is_own_sib)
        def _():
            sib_copy(i % 2, 2, k_last).start()

        @pl.when(is_sum)
        def _():
            sib_copy(0, direction, k_mid).wait_recv()
            relay_arrival(direction, k_mid).wait_recv()

            @pl.when(k_mid >= SUM_SLOTS)
            def _():
                for half in range(2):
                    sum_copy(direction, k_mid - SUM_SLOTS, half).wait_send()

            for half in range(2):
                @pl.loop(0, HALF // 16)
                def _(b):
                    rows = pl.ds(pl.multiple_of(half * HALF + b * 16, 16), 16)
                    total = tiles[RELAY_SLOTS + 2, rows].astype(jnp.float32) + sib_in[direction, k_mid, rows].astype(jnp.float32)
                    sum_out[direction, k_mid % SUM_SLOTS, rows] = total + relay_in[direction, k_mid, rows].astype(jnp.float32)

                if half == 0:
                    sum_copy(direction, k_mid, half).start()
                else:
                    @pl.when(k_mid < STEPS - 1)
                    def _():
                        sum_copy(direction, k_mid, 1).start()

                    @pl.when(k_mid == STEPS - 1)
                    def _():
                        sum_copy(direction, k_mid, 1, in_vmem=True).start()

        @pl.when(is_final)
        def _():
            sib_copy(0, 2, k_last).wait_recv()
            pltpu.make_async_copy(res_hbm.at[pl.ds(0, ROWS)], res_ld, res_sem).wait()
            def finish(half, sums):
                @pl.loop(0, HALF // 16)
                def _(b):
                    here = pl.ds(pl.multiple_of(b * 16, 16), 16)
                    rows = pl.ds(pl.multiple_of(half * HALF + b * 16, 16), 16)
                    out = pl.ds(pl.multiple_of(k_last * ROWS + half * HALF + b * 16, 16), 16)
                    y_sum = tiles[RELAY_SLOTS + 2, rows].astype(jnp.float32) + sib_in[2, k_last, rows].astype(jnp.float32)
                    y_sum = y_sum + (sums[0, here] + sums[1, here])
                    h = res_ld[rows].astype(jnp.float32) + y_sum
                    mean_sq = jnp.mean(h * h, axis=-1, keepdims=True)
                    h_ref[out] = h.astype(jnp.bfloat16)
                    n_ref[out] = (h * lax.rsqrt(mean_sq + EPS) * gain_ref[...]).astype(jnp.bfloat16)

            def finish_hbm(half):
                loads = [pltpu.make_async_copy(sum_in.at[d, k_last, half], sum_ld.at[d], ld_sem.at[d]) for d in range(2)]
                for d in range(2):
                    sum_copy(d, k_last, half).wait_recv()
                    loads[d].start()
                for load in loads:
                    load.wait()
                finish(half, sum_ld)

            finish_hbm(0)

            @pl.when(k_last < STEPS - 1)
            def _():
                finish_hbm(1)

            @pl.when(k_last == STEPS - 1)
            def _():
                for d in range(2):
                    sum_copy(d, STEPS - 1, 1, in_vmem=True).wait_recv()
                finish(1, sum_last)

    for s in range(RELAY_SLOTS):
        relay_copy(FIRST - RELAY_SLOTS + s).wait_send()
    for s in range(2):
        sib_copy(s, 0, 0).wait_send()
    for d in range(2):
        for k in range(STEPS - SUM_SLOTS, STEPS):
            for half in range(2):
                sum_copy(d, k, half).wait_send()

def store_kernel(h_ref, n_ref, h_hbm, n_hbm, sem):
    copies = []
    for b in range(4):
        rows = pl.ds(b * (BLOCK // 4), BLOCK // 4)
        copies.append(pltpu.make_async_copy(h_ref.at[rows], h_hbm.at[rows], sem.at[0, b]))
        copies.append(pltpu.make_async_copy(n_ref.at[rows], n_hbm.at[rows], sem.at[1, b]))
    for copy in copies:
        copy.start()
    for copy in copies:
        copy.wait()


def solution(mesh):
    def local_block(x_in, w_gate, w_up, w_down, residual, norm_gain):
        hbm = pl.BlockSpec(memory_space=pltpu.HBM)
        vmem = pl.BlockSpec(memory_space=pltpu.VMEM)
        h, n, _ = pl.pallas_call(
            kernel,
            out_shape=(
                pltpu.VMEM((BLOCK, D), jnp.bfloat16),
                pltpu.VMEM((BLOCK, D), jnp.bfloat16),
                jax.ShapeDtypeStruct((2, STEPS, 2, HALF, D), jnp.float32),
            ),
            in_specs=[hbm] * 5 + [vmem],
            out_specs=(vmem, vmem, hbm),
            scratch_shapes=[
                pltpu.VMEM((2, ROWS, D), jnp.bfloat16),
                pltpu.VMEM((D, F), jnp.bfloat16),
                pltpu.VMEM((D, F), jnp.bfloat16),
                pltpu.VMEM((F, D), jnp.bfloat16),
                pltpu.VMEM((ROWS, F), jnp.bfloat16),
                pltpu.VMEM((RELAY_SLOTS + 3, ROWS, D), jnp.bfloat16),
                pltpu.VMEM((2, STEPS, ROWS, D), jnp.bfloat16),
                pltpu.VMEM((3, STEPS, ROWS, D), jnp.bfloat16),
                pltpu.VMEM((2, SUM_SLOTS, ROWS, D), jnp.float32),
                pltpu.VMEM((2, HALF, D), jnp.float32),
                pltpu.VMEM((2, HALF, D), jnp.float32),
                pltpu.VMEM((ROWS, D), jnp.bfloat16),
                pltpu.SemaphoreType.DMA((2,)),
                pltpu.SemaphoreType.DMA((3, CHUNKS)),
                pltpu.SemaphoreType.DMA((RELAY_SLOTS,)),
                pltpu.SemaphoreType.DMA((2, STEPS)),
                pltpu.SemaphoreType.DMA((2,)),
                pltpu.SemaphoreType.DMA((3, STEPS)),
                pltpu.SemaphoreType.DMA((2, SUM_SLOTS, 2)),
                pltpu.SemaphoreType.DMA((2, STEPS, 2)),
                pltpu.SemaphoreType.DMA((2,)),
                pltpu.SemaphoreType.DMA,
            ],
            compiler_params=pltpu.CompilerParams(collective_id=0, has_side_effects=True, vmem_limit_bytes=58000000),
            name="mlp_reduce",
        )(x_in, w_gate, w_up, w_down, residual, norm_gain.reshape(1, D))
        return pl.pallas_call(
            store_kernel,
            out_shape=(jax.ShapeDtypeStruct((BLOCK, D), jnp.bfloat16), jax.ShapeDtypeStruct((BLOCK, D), jnp.bfloat16)),
            in_specs=[vmem, vmem],
            out_specs=(hbm, hbm),
            scratch_shapes=[pltpu.SemaphoreType.DMA((2, 4))],
            compiler_params=pltpu.CompilerParams(vmem_limit_bytes=1048576),
            name="store",
        )(*(pltpu.with_memory_space_constraint(a, pltpu.VMEM) for a in (h, n)))

    row_spec = P(("data", "tp"), None)
    return jax.shard_map(local_block, mesh=mesh, in_specs=(P("data", None), P(None, "tp"), P(None, "tp"), P("tp", None), row_spec, P(None)), out_specs=(row_spec, row_spec), check_vma=False)
```

```python
import functools

import jax
import jax.numpy as jnp
from jax import lax
from jax.experimental import pallas as pl
from jax.experimental.pallas import tpu as pltpu
from jax.sharding import PartitionSpec as P

EPS = 1e-5
ROWS = 256
CHUNKS = 4
COLS = (256, 256, 512)
HALF = 128
BLOCK = 1024
STEPS = BLOCK // ROWS
D = 2048
F = 1024
RELAY_SLOTS = 3
SUM_SLOTS = 2
FIRST = 2 * STEPS
SECOND = 4 * STEPS
TILES = 8 * STEPS


def kernel(x_hbm, wg_hbm, wu_hbm, wd_hbm, res_hbm, gain_ref, h_ref, n_ref, sum_in, x_buf, wg, wu, wd, hid, tiles, relay_in, sib_in, sum_out, sum_last, sum_ld, res_ld,
           x_sem, w_sem, relay_ssem, relay_rsem, sib_ssem, sib_rsem, sum_ssem, sum_rsem, ld_sem, res_sem):
    me = lax.axis_index("tp")
    c, cx, cy = me % 2, (me // 2) % 2, me // 4
    sib = cy * 4 + cx * 2 + (1 - c)
    xn = cy * 4 + (1 - cx) * 2
    yn = (1 - cy) * 4 + cx * 2

    barrier = pltpu.get_barrier_semaphore()
    for dev in (sib, xn, xn + 1, yn, yn + 1):
        pl.semaphore_signal(barrier, inc=1, device_id={"tp": dev}, device_id_type=pl.DeviceIdType.MESH)

    def row_of(i):
        first = 1 - (i + TILES - FIRST) // TILES
        last = (i + FIRST) // TILES
        mid = 1 - first - last
        p = i - FIRST
        q = p % 4
        direction = (1 - c) + (q // 2) * (2 * c - 1)
        r = i - FIRST - SECOND
        ty = first * (1 - cy) + mid * (cy + direction * (1 - 2 * cy)) + last * cy
        tx = first * (1 - cx) + mid * (cx + (1 - direction) * (1 - 2 * cx)) + last * cx
        tc = first * (i % 2) + mid * (q % 2) + last * ((1 - c) + ((r + TILES) // STEPS - TILES // STEPS) * (2 * c - 1))
        k = first * (i // 2) + mid * (p // 4) + last * (i % STEPS)
        return pl.multiple_of((ty * 4 + tx * 2 + tc) * BLOCK + k * ROWS, ROWS)

    def x_copy(i):
        return pltpu.make_async_copy(x_hbm.at[pl.ds(row_of(i), ROWS)], x_buf.at[i % 2], x_sem.at[i % 2])

    def w_copy(j, n):
        src, dst = ((wg_hbm, wg), (wu_hbm, wu), (wd_hbm, wd))[j]
        cols = pl.ds(n * COLS[j], COLS[j])
        return pltpu.make_async_copy(src.at[:, cols], dst.at[:, cols], w_sem.at[j, n])

    x_copy(0).start()
    for n in range(CHUNKS):
        w_copy(0, n).start()
        w_copy(1, n).start()
    for n in range(CHUNKS):
        w_copy(2, n).start()
    x_copy(1).start()

    out_chip = (1 - c) * xn + c * yn

    def relay_copy(i):
        return pltpu.make_async_remote_copy(
            src_ref=tiles.at[i % RELAY_SLOTS], dst_ref=relay_in.at[i % 2, i // 2], send_sem=relay_ssem.at[i % RELAY_SLOTS],
            recv_sem=relay_rsem.at[i % 2, i // 2], device_id={"tp": out_chip + 1 - c}, device_id_type=pl.DeviceIdType.MESH)

    def sib_copy(slot, group, k):
        return pltpu.make_async_remote_copy(
            src_ref=tiles.at[RELAY_SLOTS + slot], dst_ref=sib_in.at[group, k], send_sem=sib_ssem.at[slot],
            recv_sem=sib_rsem.at[group, k], device_id={"tp": sib}, device_id_type=pl.DeviceIdType.MESH)

    def sum_copy(j, k, half, in_vmem=False):
        slot = k % SUM_SLOTS
        return pltpu.make_async_remote_copy(
            src_ref=sum_out.at[j, slot, pl.ds(half * HALF, HALF)], dst_ref=sum_last.at[c] if in_vmem else sum_in.at[c, k, half],
            send_sem=sum_ssem.at[j, slot, half], recv_sem=sum_rsem.at[c, k, half],
            device_id={"tp": out_chip + j}, device_id_type=pl.DeviceIdType.MESH)

    def sum_arrival(d, k, half, in_vmem=False):
        here = sum_last.at[d] if in_vmem else sum_in.at[d, k, half]
        return pltpu.make_async_remote_copy(
            src_ref=here, dst_ref=here, send_sem=sum_ssem.at[0, 0, 0], recv_sem=sum_rsem.at[d, k, half],
            device_id={"tp": sib}, device_id_type=pl.DeviceIdType.MESH)

    def ffn(x_ref, out_ref, loading=False):
        for n in range(CHUNKS):
            cols = slice(n * COLS[0], (n + 1) * COLS[0])
            if loading:
                w_copy(0, n).wait()
                w_copy(1, n).wait()
            gate = jnp.dot(x_ref[...], wg[:, cols], preferred_element_type=jnp.float32)
            up = jnp.dot(x_ref[...], wu[:, cols], preferred_element_type=jnp.float32)
            hid[:, cols] = (gate * jax.nn.sigmoid(gate) * up).astype(jnp.bfloat16)
        for n in range(CHUNKS):
            cols = slice(n * COLS[2], (n + 1) * COLS[2])
            if loading:
                w_copy(2, n).wait()
            out_ref[:, cols] = jnp.dot(hid[...], wd[:, cols], preferred_element_type=jnp.float32).astype(jnp.bfloat16)

    x_copy(0).wait()
    ffn(x_buf.at[0], tiles.at[0], loading=True)
    pl.semaphore_wait(barrier, 5)
    relay_copy(0).start()

    @pl.loop(1, TILES)
    def _(i):
        first = 1 - (i + TILES - FIRST) // TILES
        last = (i + FIRST) // TILES
        mid = 1 - first - last
        p = i - FIRST
        q = p % 4
        j = q % 2
        k_mid = p // 4
        k_last = i % STEPS
        is_relay = i < FIRST
        is_sib = jnp.logical_and(i >= FIRST, jnp.logical_and(i < FIRST + SECOND, q < 2))
        is_sum = jnp.logical_and(i >= FIRST, jnp.logical_and(i < FIRST + SECOND, q >= 2))
        is_own_sib = jnp.logical_and(i >= FIRST + SECOND, i < FIRST + SECOND + STEPS)
        is_final = i >= FIRST + SECOND + STEPS
        sending = mid * (q // 2) + last * ((i - FIRST - SECOND + TILES) // STEPS - TILES // STEPS)
        slot = first * (i % RELAY_SLOTS) + (1 - first) * (RELAY_SLOTS + sending * 2 + (1 - sending) * (i % 2))

        @pl.when(i + 1 < TILES)
        def _():
            x_copy(i + 1).start()

        x_copy(i).wait()

        @pl.when(jnp.logical_and(is_relay, i >= RELAY_SLOTS))
        def _():
            relay_copy(i - RELAY_SLOTS).wait_send()

        @pl.when(jnp.logical_and(jnp.logical_or(is_sib, is_own_sib), i >= FIRST + 4))
        def _():
            sib_copy(i % 2, 0, 0).wait_send()

        @pl.when(is_final)
        def _():
            pltpu.make_async_copy(res_hbm.at[pl.ds(pl.multiple_of(k_last * ROWS, ROWS), ROWS)], res_ld, res_sem).start()

        ffn(x_buf.at[i % 2], tiles.at[slot])

        @pl.when(is_relay)
        def _():
            relay_copy(i).start()

        @pl.when(is_sib)
        def _():
            sib_copy(i % 2, j, k_mid).start()

        @pl.when(is_own_sib)
        def _():
            sib_copy(i % 2, 2, k_last).start()

        @pl.when(is_sum)
        def _():
            sib_copy(0, j, k_mid).wait_recv()
            relay_copy(2 * k_mid + j).wait_recv()

            @pl.when(k_mid >= SUM_SLOTS)
            def _():
                for half in range(2):
                    sum_copy(j, k_mid - SUM_SLOTS, half).wait_send()

            for half in range(2):
                @pl.loop(0, HALF // 16)
                def _(b):
                    rows = pl.ds(pl.multiple_of(half * HALF + b * 16, 16), 16)
                    total = tiles[RELAY_SLOTS + 2, rows].astype(jnp.float32) + sib_in[j, k_mid, rows].astype(jnp.float32)
                    sum_out[j, k_mid % SUM_SLOTS, rows] = total + relay_in[j, k_mid, rows].astype(jnp.float32)

                if half == 0:
                    sum_copy(j, k_mid, half).start()
                else:
                    @pl.when(k_mid < STEPS - 1)
                    def _():
                        sum_copy(j, k_mid, 1).start()

                    @pl.when(k_mid == STEPS - 1)
                    def _():
                        sum_copy(j, k_mid, 1, in_vmem=True).start()

        @pl.when(is_final)
        def _():
            sib_copy(0, 2, k_last).wait_recv()
            pltpu.make_async_copy(res_hbm.at[pl.ds(0, ROWS)], res_ld, res_sem).wait()
            def finish(half, sums):
                @pl.loop(0, HALF // 16)
                def _(b):
                    here = pl.ds(pl.multiple_of(b * 16, 16), 16)
                    rows = pl.ds(pl.multiple_of(half * HALF + b * 16, 16), 16)
                    out = pl.ds(pl.multiple_of(k_last * ROWS + half * HALF + b * 16, 16), 16)
                    y_sum = tiles[RELAY_SLOTS + 2, rows].astype(jnp.float32) + sib_in[2, k_last, rows].astype(jnp.float32)
                    y_sum = y_sum + (sums[0, here] + sums[1, here])
                    h = res_ld[rows].astype(jnp.float32) + y_sum
                    mean_sq = jnp.mean(h * h, axis=-1, keepdims=True)
                    h_ref[out] = h.astype(jnp.bfloat16)
                    n_ref[out] = (h * lax.rsqrt(mean_sq + EPS) * gain_ref[...]).astype(jnp.bfloat16)

            def finish_hbm(half):
                loads = [pltpu.make_async_copy(sum_in.at[d, k_last, half], sum_ld.at[d], ld_sem.at[d]) for d in range(2)]
                for d in range(2):
                    sum_arrival(d, k_last, half).wait_recv()
                    loads[d].start()
                for load in loads:
                    load.wait()
                finish(half, sum_ld)

            finish_hbm(0)

            @pl.when(k_last < STEPS - 1)
            def _():
                finish_hbm(1)

            @pl.when(k_last == STEPS - 1)
            def _():
                for d in range(2):
                    sum_arrival(d, STEPS - 1, 1, in_vmem=True).wait_recv()
                finish(1, sum_last)

    for s in range(RELAY_SLOTS):
        relay_copy(FIRST - RELAY_SLOTS + s).wait_send()
    for s in range(2):
        sib_copy(s, 0, 0).wait_send()
    for d in range(2):
        for k in range(STEPS - SUM_SLOTS, STEPS):
            for half in range(2):
                sum_copy(d, k, half).wait_send()

def store_kernel(h_ref, n_ref, h_hbm, n_hbm, sem):
    copies = []
    for b in range(4):
        rows = pl.ds(b * (BLOCK // 4), BLOCK // 4)
        copies.append(pltpu.make_async_copy(h_ref.at[rows], h_hbm.at[rows], sem.at[0, b]))
        copies.append(pltpu.make_async_copy(n_ref.at[rows], n_hbm.at[rows], sem.at[1, b]))
    for copy in copies:
        copy.start()
    for copy in copies:
        copy.wait()


def solution(mesh):
    def local_block(x_in, w_gate, w_up, w_down, residual, norm_gain):
        hbm = pl.BlockSpec(memory_space=pltpu.HBM)
        vmem = pl.BlockSpec(memory_space=pltpu.VMEM)
        h, n, _ = pl.pallas_call(
            kernel,
            out_shape=(
                pltpu.VMEM((BLOCK, D), jnp.bfloat16),
                pltpu.VMEM((BLOCK, D), jnp.bfloat16),
                jax.ShapeDtypeStruct((2, STEPS, 2, HALF, D), jnp.float32),
            ),
            in_specs=[hbm] * 5 + [vmem],
            out_specs=(vmem, vmem, hbm),
            scratch_shapes=[
                pltpu.VMEM((2, ROWS, D), jnp.bfloat16),
                pltpu.VMEM((D, F), jnp.bfloat16),
                pltpu.VMEM((D, F), jnp.bfloat16),
                pltpu.VMEM((F, D), jnp.bfloat16),
                pltpu.VMEM((ROWS, F), jnp.bfloat16),
                pltpu.VMEM((RELAY_SLOTS + 3, ROWS, D), jnp.bfloat16),
                pltpu.VMEM((2, STEPS, ROWS, D), jnp.bfloat16),
                pltpu.VMEM((3, STEPS, ROWS, D), jnp.bfloat16),
                pltpu.VMEM((2, SUM_SLOTS, ROWS, D), jnp.float32),
                pltpu.VMEM((2, HALF, D), jnp.float32),
                pltpu.VMEM((2, HALF, D), jnp.float32),
                pltpu.VMEM((ROWS, D), jnp.bfloat16),
                pltpu.SemaphoreType.DMA((2,)),
                pltpu.SemaphoreType.DMA((3, CHUNKS)),
                pltpu.SemaphoreType.DMA((RELAY_SLOTS,)),
                pltpu.SemaphoreType.DMA((2, STEPS)),
                pltpu.SemaphoreType.DMA((2,)),
                pltpu.SemaphoreType.DMA((3, STEPS)),
                pltpu.SemaphoreType.DMA((2, SUM_SLOTS, 2)),
                pltpu.SemaphoreType.DMA((2, STEPS, 2)),
                pltpu.SemaphoreType.DMA((2,)),
                pltpu.SemaphoreType.DMA,
            ],
            compiler_params=pltpu.CompilerParams(collective_id=0, has_side_effects=True, vmem_limit_bytes=58000000),
            name="mlp_reduce",
        )(x_in, w_gate, w_up, w_down, residual, norm_gain.reshape(1, D))
        return pl.pallas_call(
            store_kernel,
            out_shape=(jax.ShapeDtypeStruct((BLOCK, D), jnp.bfloat16), jax.ShapeDtypeStruct((BLOCK, D), jnp.bfloat16)),
            in_specs=[vmem, vmem],
            out_specs=(hbm, hbm),
            scratch_shapes=[pltpu.SemaphoreType.DMA((2, 4))],
            compiler_params=pltpu.CompilerParams(vmem_limit_bytes=1048576),
            name="store",
        )(*(pltpu.with_memory_space_constraint(a, pltpu.VMEM) for a in (h, n)))

    row_spec = P(("data", "tp"), None)
    return jax.shard_map(local_block, mesh=mesh, in_specs=(P("data", None), P(None, "tp"), P(None, "tp"), P("tp", None), row_spec, P(None)), out_specs=(row_spec, row_spec), check_vma=False)
```

```python
import functools

import jax
import jax.numpy as jnp
from jax import lax
from jax.experimental import pallas as pl
from jax.experimental.pallas import tpu as pltpu
from jax.sharding import PartitionSpec as P

EPS = 1e-5
ROWS = 256
CHUNKS = 4
COLS = (256, 256, 512)
HALF = 128
BLOCK = 1024
STEPS = BLOCK // ROWS
D = 2048
F = 1024
HID_SLOTS = 6
SUM_SLOTS = 2
FIRST = 2 * STEPS
SECOND = FIRST + STEPS
THIRD = SECOND + 4 * STEPS
TILES = 8 * STEPS


def kernel(x_hbm, wg_hbm, wu_hbm, wd_hbm, res_hbm, gain_ref, h_ref, n_ref, sum_in, x_buf, wg, wu, wd, wd_relay, hid, tiles, hid_in, sib_in, sum_out, sum_last, sum_ld, res_ld,
           x_sem, w_sem, wr_sem, relay_ssem, relay_rsem, sib_ssem, sib_rsem, sum_ssem, sum_rsem, ld_sem, res_sem):
    me = lax.axis_index("tp")
    c, cx, cy = me % 2, (me // 2) % 2, me // 4
    sib = cy * 4 + cx * 2 + (1 - c)
    xn = cy * 4 + (1 - cx) * 2
    yn = (1 - cy) * 4 + cx * 2

    barrier = pltpu.get_barrier_semaphore()
    for dev in (sib, xn, xn + 1, yn, yn + 1):
        pl.semaphore_signal(barrier, inc=1, device_id={"tp": dev}, device_id_type=pl.DeviceIdType.MESH)

    def kinds(i):
        past_first, past_second, past_third = (i + TILES - FIRST) // TILES, (i + TILES - SECOND) // TILES, (i + TILES - THIRD) // TILES
        return 1 - past_first, past_first - past_second, past_second - past_third, past_third

    def row_of(i):
        diag, to_sib, to_chip, kept = kinds(i)
        q = i % 4
        direction = (1 - c) + (q // 2) * (2 * c - 1)
        ty = diag * (1 - cy) + to_chip * (cy + direction * (1 - 2 * cy)) + (to_sib + kept) * cy
        tx = diag * (1 - cx) + to_chip * (cx + (1 - direction) * (1 - 2 * cx)) + (to_sib + kept) * cx
        tc = (diag + to_chip) * (i % 2) + to_sib * (1 - c) + kept * c
        k = diag * (i // 2) + to_chip * ((i - SECOND) // 4) + (to_sib + kept) * (i % STEPS)
        return pl.multiple_of((ty * 4 + tx * 2 + tc) * BLOCK + k * ROWS, ROWS)

    def x_copy(i):
        return pltpu.make_async_copy(x_hbm.at[pl.ds(row_of(i), ROWS)], x_buf.at[i % 2], x_sem.at[i % 2])

    def w_copy(j, n):
        src, dst = ((wg_hbm, wg), (wu_hbm, wu), (wd_hbm, wd))[j]
        cols = pl.ds(n * COLS[j], COLS[j])
        return pltpu.make_async_copy(src.at[:, cols], dst.at[:, cols], w_sem.at[j, n])

    x_copy(0).start()
    for n in range(CHUNKS):
        w_copy(0, n).start()
        w_copy(1, n).start()
    for n in range(CHUNKS):
        w_copy(2, n).start()
    x_copy(1).start()

    out_chip = (1 - c) * xn + c * yn

    def w_relay_copy():
        return pltpu.make_async_remote_copy(
            src_ref=wd_hbm, dst_ref=wd_relay, send_sem=wr_sem.at[0], recv_sem=wr_sem.at[1],
            device_id={"tp": out_chip + 1 - c}, device_id_type=pl.DeviceIdType.MESH)

    def relay_copy(i):
        return pltpu.make_async_remote_copy(
            src_ref=hid.at[i % HID_SLOTS], dst_ref=hid_in.at[i % 2, i // 2], send_sem=relay_ssem.at[i % HID_SLOTS],
            recv_sem=relay_rsem.at[i % 2, i // 2], device_id={"tp": out_chip + 1 - c}, device_id_type=pl.DeviceIdType.MESH)

    def sib_copy(slot, group, k):
        return pltpu.make_async_remote_copy(
            src_ref=tiles.at[slot], dst_ref=sib_in.at[group, k], send_sem=sib_ssem.at[slot],
            recv_sem=sib_rsem.at[group, k], device_id={"tp": sib}, device_id_type=pl.DeviceIdType.MESH)

    def sum_copy(j, k, half, in_vmem=False):
        slot = k % SUM_SLOTS
        return pltpu.make_async_remote_copy(
            src_ref=sum_out.at[j, slot, pl.ds(half * HALF, HALF)], dst_ref=sum_last.at[c] if in_vmem else sum_in.at[c, k, half],
            send_sem=sum_ssem.at[j, slot, half], recv_sem=sum_rsem.at[c, k, half],
            device_id={"tp": out_chip + j}, device_id_type=pl.DeviceIdType.MESH)

    def sum_arrival(d, k, half, in_vmem=False):
        here = sum_last.at[d] if in_vmem else sum_in.at[d, k, half]
        return pltpu.make_async_remote_copy(
            src_ref=here, dst_ref=here, send_sem=sum_ssem.at[0, 0, 0], recv_sem=sum_rsem.at[d, k, half],
            device_id={"tp": sib}, device_id_type=pl.DeviceIdType.MESH)

    def gate_up(x_ref, out_ref, loading=False):
        for n in range(CHUNKS):
            cols = slice(n * COLS[0], (n + 1) * COLS[0])
            if loading:
                w_copy(0, n).wait()
                w_copy(1, n).wait()
            gate = jnp.dot(x_ref[...], wg[:, cols], preferred_element_type=jnp.float32)
            up = jnp.dot(x_ref[...], wu[:, cols], preferred_element_type=jnp.float32)
            out_ref[:, cols] = (gate * jax.nn.sigmoid(gate) * up).astype(jnp.bfloat16)

    pl.semaphore_wait(barrier, 5)
    w_relay_copy().start()
    x_copy(0).wait()
    gate_up(x_buf.at[0], hid.at[0], loading=True)
    relay_copy(0).start()
    for n in range(CHUNKS):
        w_copy(2, n).wait()

    @pl.loop(1, TILES)
    def _(i):
        diag, to_sib, to_chip, kept = kinds(i)
        j = i % 2
        k_chip = (i - SECOND) // 4
        k_own = i % STEPS
        stays = to_chip * (i % 4 // 2) + kept
        is_relay = i < FIRST
        in_chip = jnp.logical_and(i >= SECOND, i < THIRD)
        is_own_sib = jnp.logical_and(i >= FIRST, i < SECOND)
        is_sib = jnp.logical_and(in_chip, i % 4 < 2)
        is_sum = jnp.logical_and(in_chip, i % 4 >= 2)
        is_final = i >= THIRD

        @pl.when(i + 1 < TILES)
        def _():
            x_copy(i + 1).start()

        x_copy(i).wait()

        @pl.when(jnp.logical_and(is_relay, i >= HID_SLOTS))
        def _():
            relay_copy(i - HID_SLOTS).wait_send()

        @pl.when(jnp.logical_and(jnp.logical_or(is_sib, is_own_sib), i >= FIRST + 2))
        def _():
            sib_copy(j, 0, 0).wait_send()

        @pl.when(is_final)
        def _():
            pltpu.make_async_copy(res_hbm.at[pl.ds(pl.multiple_of(k_own * ROWS, ROWS), ROWS)], res_ld, res_sem).start()

        hid_slot = diag * (i % HID_SLOTS) + (1 - diag) * HID_SLOTS
        gate_up(x_buf.at[i % 2], hid.at[hid_slot])

        @pl.when(is_relay)
        def _():
            relay_copy(i).start()

        @pl.when(i >= FIRST)
        def _():
            slot = stays * 2 + (1 - stays) * j
            for n in range(CHUNKS):
                cols = slice(n * COLS[2], (n + 1) * COLS[2])
                tiles[slot, :, cols] = jnp.dot(hid[HID_SLOTS], wd[:, cols], preferred_element_type=jnp.float32).astype(jnp.bfloat16)

        @pl.when(is_sib)
        def _():
            sib_copy(j, j, k_chip).start()

        @pl.when(is_own_sib)
        def _():
            sib_copy(j, 2, k_own).start()

        @pl.when(is_sum)
        def _():
            sib_copy(0, j, k_chip).wait_recv()
            relay_copy(2 * k_chip + j).wait_recv()

            @pl.when(i == SECOND + 2)
            def _():
                w_relay_copy().wait_recv()

            @pl.when(k_chip >= SUM_SLOTS)
            def _():
                for half in range(2):
                    sum_copy(j, k_chip - SUM_SLOTS, half).wait_send()

            for n in range(CHUNKS):
                cols = slice(n * COLS[2], (n + 1) * COLS[2])
                relayed = jnp.dot(hid_in[j, k_chip], wd_relay[:, cols], preferred_element_type=jnp.float32).astype(jnp.bfloat16)
                total = tiles[2, :, cols].astype(jnp.float32) + sib_in[j, k_chip, :, cols].astype(jnp.float32)
                sum_out[j, k_chip % SUM_SLOTS, :, cols] = total + relayed.astype(jnp.float32)

            sum_copy(j, k_chip, 0).start()

            @pl.when(k_chip < STEPS - 1)
            def _():
                sum_copy(j, k_chip, 1).start()

            @pl.when(k_chip == STEPS - 1)
            def _():
                sum_copy(j, k_chip, 1, in_vmem=True).start()

        @pl.when(is_final)
        def _():
            sib_copy(0, 2, k_own).wait_recv()
            pltpu.make_async_copy(res_hbm.at[pl.ds(0, ROWS)], res_ld, res_sem).wait()
            def finish(half, sums):
                @pl.loop(0, HALF // 16)
                def _(b):
                    here = pl.ds(pl.multiple_of(b * 16, 16), 16)
                    rows = pl.ds(pl.multiple_of(half * HALF + b * 16, 16), 16)
                    out = pl.ds(pl.multiple_of(k_own * ROWS + half * HALF + b * 16, 16), 16)
                    y_sum = tiles[2, rows].astype(jnp.float32) + sib_in[2, k_own, rows].astype(jnp.float32)
                    y_sum = y_sum + (sums[0, here] + sums[1, here])
                    h = res_ld[rows].astype(jnp.float32) + y_sum
                    mean_sq = jnp.mean(h * h, axis=-1, keepdims=True)
                    h_ref[out] = h.astype(jnp.bfloat16)
                    n_ref[out] = (h * lax.rsqrt(mean_sq + EPS) * gain_ref[...]).astype(jnp.bfloat16)

            def finish_hbm(half):
                loads = [pltpu.make_async_copy(sum_in.at[d, k_own, half], sum_ld.at[d], ld_sem.at[d]) for d in range(2)]
                for d in range(2):
                    sum_arrival(d, k_own, half).wait_recv()
                    loads[d].start()
                for load in loads:
                    load.wait()
                finish(half, sum_ld)

            finish_hbm(0)

            @pl.when(k_own < STEPS - 1)
            def _():
                finish_hbm(1)

            @pl.when(k_own == STEPS - 1)
            def _():
                for d in range(2):
                    sum_arrival(d, STEPS - 1, 1, in_vmem=True).wait_recv()
                finish(1, sum_last)

    w_relay_copy().wait_send()
    for s in range(HID_SLOTS):
        relay_copy(FIRST - HID_SLOTS + s).wait_send()
    for s in range(2):
        sib_copy(s, 0, 0).wait_send()
    for d in range(2):
        for k in range(STEPS - SUM_SLOTS, STEPS):
            for half in range(2):
                sum_copy(d, k, half).wait_send()

def store_kernel(h_ref, n_ref, h_hbm, n_hbm, sem):
    copies = []
    for b in range(4):
        rows = pl.ds(b * (BLOCK // 4), BLOCK // 4)
        copies.append(pltpu.make_async_copy(h_ref.at[rows], h_hbm.at[rows], sem.at[0, b]))
        copies.append(pltpu.make_async_copy(n_ref.at[rows], n_hbm.at[rows], sem.at[1, b]))
    for copy in copies:
        copy.start()
    for copy in copies:
        copy.wait()


def solution(mesh):
    def local_block(x_in, w_gate, w_up, w_down, residual, norm_gain):
        hbm = pl.BlockSpec(memory_space=pltpu.HBM)
        vmem = pl.BlockSpec(memory_space=pltpu.VMEM)
        h, n, _ = pl.pallas_call(
            kernel,
            out_shape=(
                pltpu.VMEM((BLOCK, D), jnp.bfloat16),
                pltpu.VMEM((BLOCK, D), jnp.bfloat16),
                jax.ShapeDtypeStruct((2, STEPS, 2, HALF, D), jnp.float32),
            ),
            in_specs=[hbm] * 5 + [vmem],
            out_specs=(vmem, vmem, hbm),
            scratch_shapes=[
                pltpu.VMEM((2, ROWS, D), jnp.bfloat16),
                pltpu.VMEM((D, F), jnp.bfloat16),
                pltpu.VMEM((D, F), jnp.bfloat16),
                pltpu.VMEM((F, D), jnp.bfloat16),
                pltpu.VMEM((F, D), jnp.bfloat16),
                pltpu.VMEM((HID_SLOTS + 1, ROWS, F), jnp.bfloat16),
                pltpu.VMEM((3, ROWS, D), jnp.bfloat16),
                pltpu.VMEM((2, STEPS, ROWS, F), jnp.bfloat16),
                pltpu.VMEM((3, STEPS, ROWS, D), jnp.bfloat16),
                pltpu.VMEM((2, SUM_SLOTS, ROWS, D), jnp.float32),
                pltpu.VMEM((2, HALF, D), jnp.float32),
                pltpu.VMEM((2, HALF, D), jnp.float32),
                pltpu.VMEM((ROWS, D), jnp.bfloat16),
                pltpu.SemaphoreType.DMA((2,)),
                pltpu.SemaphoreType.DMA((3, CHUNKS)),
                pltpu.SemaphoreType.DMA((2,)),
                pltpu.SemaphoreType.DMA((HID_SLOTS,)),
                pltpu.SemaphoreType.DMA((2, STEPS)),
                pltpu.SemaphoreType.DMA((2,)),
                pltpu.SemaphoreType.DMA((3, STEPS)),
                pltpu.SemaphoreType.DMA((2, SUM_SLOTS, 2)),
                pltpu.SemaphoreType.DMA((2, STEPS, 2)),
                pltpu.SemaphoreType.DMA((2,)),
                pltpu.SemaphoreType.DMA,
            ],
            compiler_params=pltpu.CompilerParams(collective_id=0, has_side_effects=True, vmem_limit_bytes=58000000),
            name="mlp_reduce",
        )(x_in, w_gate, w_up, w_down, residual, norm_gain.reshape(1, D))
        return pl.pallas_call(
            store_kernel,
            out_shape=(jax.ShapeDtypeStruct((BLOCK, D), jnp.bfloat16), jax.ShapeDtypeStruct((BLOCK, D), jnp.bfloat16)),
            in_specs=[vmem, vmem],
            out_specs=(hbm, hbm),
            scratch_shapes=[pltpu.SemaphoreType.DMA((2, 4))],
            compiler_params=pltpu.CompilerParams(vmem_limit_bytes=1048576),
            name="store",
        )(*(pltpu.with_memory_space_constraint(a, pltpu.VMEM) for a in (h, n)))

    row_spec = P(("data", "tp"), None)
    return jax.shard_map(local_block, mesh=mesh, in_specs=(P("data", None), P(None, "tp"), P(None, "tp"), P("tp", None), row_spec, P(None)), out_specs=(row_spec, row_spec), check_vma=False)
```

```python
import functools

import jax
import jax.numpy as jnp
from jax import lax
from jax.experimental import pallas as pl
from jax.experimental.pallas import tpu as pltpu
from jax.sharding import PartitionSpec as P

EPS = 1e-5
ROWS = 256
CHUNKS = 4
COLS = (256, 256, 512)
HALF = 128
LATE = 32
BLOCK = 1024
STEPS = BLOCK // ROWS
D = 2048
F = 1024
HID_SLOTS = 6
SUM_SLOTS = 2
FIRST = 2 * STEPS
SECOND = FIRST + STEPS
THIRD = SECOND + 4 * STEPS
TILES = 8 * STEPS


def kernel(x_hbm, wg_hbm, wu_hbm, wd_hbm, res_hbm, gain_hbm, h_ref, n_ref, sum_in, x_buf, wg, wu, wd, wd_relay, hid, tiles, hid_in, sib_in, sum_out, sum_last, sum_ld, res_ld, gain_ref,
           x_sem, w_sem, wr_sem, relay_ssem, relay_rsem, sib_ssem, sib_rsem, sum_ssem, sum_rsem, ld_sem, res_sem, gain_sem):
    me = lax.axis_index("tp")
    c, cx, cy = me % 2, (me // 2) % 2, me // 4
    sib = cy * 4 + cx * 2 + (1 - c)
    xn = cy * 4 + (1 - cx) * 2
    yn = (1 - cy) * 4 + cx * 2

    barrier = pltpu.get_barrier_semaphore()
    for dev in (sib, (1 - c) * (yn + 1) + c * xn, (1 - c) * xn + c * (yn + 1)):
        pl.semaphore_signal(barrier, inc=1, device_id={"tp": dev}, device_id_type=pl.DeviceIdType.MESH)

    def kinds(i):
        past_first, past_second, past_third = (i + TILES - FIRST) // TILES, (i + TILES - SECOND) // TILES, (i + TILES - THIRD) // TILES
        return 1 - past_first, past_first - past_second, past_second - past_third, past_third

    def row_of(i):
        diag, to_sib, to_chip, kept = kinds(i)
        q = i % 4
        direction = (1 - c) + (q // 2) * (2 * c - 1)
        ty = diag * (1 - cy) + to_chip * (cy + direction * (1 - 2 * cy)) + (to_sib + kept) * cy
        tx = diag * (1 - cx) + to_chip * (cx + (1 - direction) * (1 - 2 * cx)) + (to_sib + kept) * cx
        tc = (diag + to_chip) * (i % 2) + to_sib * (1 - c) + kept * c
        k = diag * (i // 2) + to_chip * ((i - SECOND) // 4) + (to_sib + kept) * (i % STEPS)
        return pl.multiple_of((ty * 4 + tx * 2 + tc) * BLOCK + k * ROWS, ROWS)

    def x_copy(i):
        return pltpu.make_async_copy(x_hbm.at[pl.ds(row_of(i), ROWS)], x_buf.at[i % 2], x_sem.at[i % 2])

    def w_copy(j, n):
        src, dst = ((wg_hbm, wg), (wu_hbm, wu), (wd_hbm, wd))[j]
        cols = pl.ds(n * COLS[j], COLS[j])
        return pltpu.make_async_copy(src.at[:, cols], dst.at[:, cols], w_sem.at[j, n])

    x_copy(0).start()
    for n in range(CHUNKS):
        w_copy(0, n).start()
        w_copy(1, n).start()
    for n in range(CHUNKS):
        w_copy(2, n).start()
    x_copy(1).start()
    gain_copy = pltpu.make_async_copy(gain_hbm, gain_ref, gain_sem)
    gain_copy.start()

    out_chip = (1 - c) * xn + c * yn

    def w_relay_copy():
        return pltpu.make_async_remote_copy(
            src_ref=wd_hbm, dst_ref=wd_relay, send_sem=wr_sem.at[0], recv_sem=wr_sem.at[1],
            device_id={"tp": out_chip + 1 - c}, device_id_type=pl.DeviceIdType.MESH)

    def relay_copy(i):
        return pltpu.make_async_remote_copy(
            src_ref=hid.at[i % HID_SLOTS], dst_ref=hid_in.at[i % 2, i // 2], send_sem=relay_ssem.at[i % HID_SLOTS],
            recv_sem=relay_rsem.at[i % 2, i // 2], device_id={"tp": out_chip + 1 - c}, device_id_type=pl.DeviceIdType.MESH)

    def sib_copy(slot, group, k):
        return pltpu.make_async_remote_copy(
            src_ref=tiles.at[slot], dst_ref=sib_in.at[group, k], send_sem=sib_ssem.at[slot],
            recv_sem=sib_rsem.at[group, k], device_id={"tp": sib}, device_id_type=pl.DeviceIdType.MESH)

    def piece(part):
        return (pl.ds(0, HALF), pl.ds(HALF, HALF), pl.ds(HALF, HALF - LATE), pl.ds(ROWS - LATE, LATE))[part]

    def landing(d, k, part):
        if part < 2:
            return sum_in.at[d, k, part]
        return sum_last.at[d, pl.ds(0, HALF - LATE) if part == 2 else pl.ds(HALF - LATE, LATE)]

    def sum_copy(j, k, part):
        slot = k % SUM_SLOTS
        return pltpu.make_async_remote_copy(
            src_ref=sum_out.at[j, slot, piece(part)], dst_ref=landing(c, k, part),
            send_sem=sum_ssem.at[j, slot, part], recv_sem=sum_rsem.at[c, k, part],
            device_id={"tp": out_chip + j}, device_id_type=pl.DeviceIdType.MESH)

    def sum_arrival(d, k, part):
        return pltpu.make_async_remote_copy(
            src_ref=landing(d, k, part), dst_ref=landing(d, k, part), send_sem=sum_ssem.at[0, 0, 0], recv_sem=sum_rsem.at[d, k, part],
            device_id={"tp": sib}, device_id_type=pl.DeviceIdType.MESH)

    def gate_up(x_ref, out_ref, loading=False):
        for n in range(CHUNKS):
            cols = slice(n * COLS[0], (n + 1) * COLS[0])
            if loading:
                w_copy(0, n).wait()
                w_copy(1, n).wait()
            gate = jnp.dot(x_ref[...], wg[:, cols], preferred_element_type=jnp.float32)
            up = jnp.dot(x_ref[...], wu[:, cols], preferred_element_type=jnp.float32)
            out_ref[:, cols] = (gate * jax.nn.sigmoid(gate) * up).astype(jnp.bfloat16)

    pl.semaphore_wait(barrier, 3)
    w_relay_copy().start()
    x_copy(0).wait()
    gate_up(x_buf.at[0], hid.at[0], loading=True)
    relay_copy(0).start()
    for n in range(CHUNKS):
        w_copy(2, n).wait()
    gain_copy.wait()

    @pl.loop(1, TILES)
    def _(i):
        diag, to_sib, to_chip, kept = kinds(i)
        j = i % 2
        k_chip = (i - SECOND) // 4
        k_own = i % STEPS
        stays = to_chip * (i % 4 // 2) + kept
        is_relay = i < FIRST
        in_chip = jnp.logical_and(i >= SECOND, i < THIRD)
        is_own_sib = jnp.logical_and(i >= FIRST, i < SECOND)
        is_sib = jnp.logical_and(in_chip, i % 4 < 2)
        is_sum = jnp.logical_and(in_chip, i % 4 >= 2)
        is_final = i >= THIRD

        @pl.when(i + 1 < TILES)
        def _():
            x_copy(i + 1).start()

        x_copy(i).wait()

        @pl.when(jnp.logical_and(is_relay, i >= HID_SLOTS))
        def _():
            relay_copy(i - HID_SLOTS).wait_send()

        @pl.when(jnp.logical_and(jnp.logical_or(is_sib, is_own_sib), i >= FIRST + 2))
        def _():
            sib_copy(j, 0, 0).wait_send()

        @pl.when(is_final)
        def _():
            pltpu.make_async_copy(res_hbm.at[pl.ds(pl.multiple_of(k_own * ROWS, ROWS), ROWS)], res_ld, res_sem).start()

        hid_slot = diag * (i % HID_SLOTS) + (1 - diag) * HID_SLOTS
        gate_up(x_buf.at[i % 2], hid.at[hid_slot])

        @pl.when(is_relay)
        def _():
            relay_copy(i).start()

        @pl.when(i >= FIRST)
        def _():
            slot = stays * 2 + (1 - stays) * j
            for n in range(CHUNKS):
                cols = slice(n * COLS[2], (n + 1) * COLS[2])
                tiles[slot, :, cols] = jnp.dot(hid[HID_SLOTS], wd[:, cols], preferred_element_type=jnp.float32).astype(jnp.bfloat16)

        @pl.when(is_sib)
        def _():
            sib_copy(j, j, k_chip).start()

        @pl.when(is_own_sib)
        def _():
            sib_copy(j, 2, k_own).start()

        @pl.when(is_sum)
        def _():
            sib_copy(0, j, k_chip).wait_recv()
            relay_copy(2 * k_chip + j).wait_recv()

            @pl.when(i == SECOND + 2)
            def _():
                w_relay_copy().wait_recv()

            @pl.when(k_chip >= SUM_SLOTS)
            def _():
                for half in range(2):
                    sum_copy(j, k_chip - SUM_SLOTS, half).wait_send()

            for n in range(CHUNKS):
                cols = slice(n * COLS[2], (n + 1) * COLS[2])
                relayed = jnp.dot(hid_in[j, k_chip], wd_relay[:, cols], preferred_element_type=jnp.float32).astype(jnp.bfloat16)
                total = tiles[2, :, cols].astype(jnp.float32) + sib_in[j, k_chip, :, cols].astype(jnp.float32)
                sum_out[j, k_chip % SUM_SLOTS, :, cols] = total + relayed.astype(jnp.float32)

            sum_copy(j, k_chip, 0).start()

            @pl.when(k_chip < STEPS - 1)
            def _():
                sum_copy(j, k_chip, 1).start()

            @pl.when(k_chip == STEPS - 1)
            def _():
                for part in (2, 3):
                    sum_copy(j, k_chip, part).start()

        @pl.when(is_final)
        def _():
            sib_copy(0, 2, k_own).wait_recv()
            pltpu.make_async_copy(res_hbm.at[pl.ds(0, ROWS)], res_ld, res_sem).wait()
            def finish(start, rows, sums, sums_start):
                @pl.loop(0, rows // 16)
                def _(b):
                    here = pl.ds(pl.multiple_of(sums_start + b * 16, 16), 16)
                    tile = pl.ds(pl.multiple_of(start + b * 16, 16), 16)
                    out = pl.ds(pl.multiple_of(k_own * ROWS + start + b * 16, 16), 16)
                    y_sum = tiles[2, tile].astype(jnp.float32) + sib_in[2, k_own, tile].astype(jnp.float32)
                    y_sum = y_sum + (sums[0, here] + sums[1, here])
                    h = res_ld[tile].astype(jnp.float32) + y_sum
                    mean_sq = jnp.mean(h * h, axis=-1, keepdims=True)
                    h_ref[out] = h.astype(jnp.bfloat16)
                    n_ref[out] = (h * lax.rsqrt(mean_sq + EPS) * gain_ref[...]).astype(jnp.bfloat16)

            def finish_hbm(half):
                loads = [pltpu.make_async_copy(sum_in.at[d, k_own, half], sum_ld.at[d], ld_sem.at[d]) for d in range(2)]
                for d in range(2):
                    sum_arrival(d, k_own, half).wait_recv()
                    loads[d].start()
                for load in loads:
                    load.wait()
                finish(half * HALF, HALF, sum_ld, 0)

            finish_hbm(0)

            @pl.when(k_own < STEPS - 1)
            def _():
                finish_hbm(1)

            @pl.when(k_own == STEPS - 1)
            def _():
                for part, rows in ((2, HALF - LATE), (3, LATE)):
                    for d in range(2):
                        sum_arrival(d, STEPS - 1, part).wait_recv()
                    start = (part - 2) * (HALF - LATE)
                    finish(HALF + start, rows, sum_last, start)

    w_relay_copy().wait_send()
    for s in range(HID_SLOTS):
        relay_copy(FIRST - HID_SLOTS + s).wait_send()
    for s in range(2):
        sib_copy(s, 0, 0).wait_send()
    for j in range(2):
        for k in range(STEPS - SUM_SLOTS, STEPS):
            for part in ((0, 1) if k < STEPS - 1 else (0, 2, 3)):
                sum_copy(j, k, part).wait_send()


def store_kernel(h_ref, n_ref, h_hbm, n_hbm, sem):
    copies = []
    for b in range(4):
        rows = pl.ds(b * (BLOCK // 4), BLOCK // 4)
        copies.append(pltpu.make_async_copy(h_ref.at[rows], h_hbm.at[rows], sem.at[0, b]))
        copies.append(pltpu.make_async_copy(n_ref.at[rows], n_hbm.at[rows], sem.at[1, b]))
    for copy in copies:
        copy.start()
    for copy in copies:
        copy.wait()


def solution(mesh):
    def local_block(x_in, w_gate, w_up, w_down, residual, norm_gain):
        hbm = pl.BlockSpec(memory_space=pltpu.HBM)
        vmem = pl.BlockSpec(memory_space=pltpu.VMEM)
        h, n, _ = pl.pallas_call(
            kernel,
            out_shape=(
                pltpu.VMEM((BLOCK, D), jnp.bfloat16),
                pltpu.VMEM((BLOCK, D), jnp.bfloat16),
                jax.ShapeDtypeStruct((2, STEPS, 2, HALF, D), jnp.float32),
            ),
            in_specs=[hbm] * 6,
            out_specs=(vmem, vmem, hbm),
            scratch_shapes=[
                pltpu.VMEM((2, ROWS, D), jnp.bfloat16),
                pltpu.VMEM((D, F), jnp.bfloat16),
                pltpu.VMEM((D, F), jnp.bfloat16),
                pltpu.VMEM((F, D), jnp.bfloat16),
                pltpu.VMEM((F, D), jnp.bfloat16),
                pltpu.VMEM((HID_SLOTS + 1, ROWS, F), jnp.bfloat16),
                pltpu.VMEM((3, ROWS, D), jnp.bfloat16),
                pltpu.VMEM((2, STEPS, ROWS, F), jnp.bfloat16),
                pltpu.VMEM((3, STEPS, ROWS, D), jnp.bfloat16),
                pltpu.VMEM((2, SUM_SLOTS, ROWS, D), jnp.float32),
                pltpu.VMEM((2, HALF, D), jnp.float32),
                pltpu.VMEM((2, HALF, D), jnp.float32),
                pltpu.VMEM((ROWS, D), jnp.bfloat16),
                pltpu.VMEM((1, D), jnp.float32),
                pltpu.SemaphoreType.DMA((2,)),
                pltpu.SemaphoreType.DMA((3, CHUNKS)),
                pltpu.SemaphoreType.DMA((2,)),
                pltpu.SemaphoreType.DMA((HID_SLOTS,)),
                pltpu.SemaphoreType.DMA((2, STEPS)),
                pltpu.SemaphoreType.DMA((2,)),
                pltpu.SemaphoreType.DMA((3, STEPS)),
                pltpu.SemaphoreType.DMA((2, SUM_SLOTS, 4)),
                pltpu.SemaphoreType.DMA((2, STEPS, 4)),
                pltpu.SemaphoreType.DMA((2,)),
                pltpu.SemaphoreType.DMA,
                pltpu.SemaphoreType.DMA,
            ],
            compiler_params=pltpu.CompilerParams(collective_id=0, has_side_effects=True, vmem_limit_bytes=58000000),
            name="mlp_reduce",
        )(x_in, w_gate, w_up, w_down, residual, norm_gain.reshape(1, D))
        return pl.pallas_call(
            store_kernel,
            out_shape=(jax.ShapeDtypeStruct((BLOCK, D), jnp.bfloat16), jax.ShapeDtypeStruct((BLOCK, D), jnp.bfloat16)),
            in_specs=[vmem, vmem],
            out_specs=(hbm, hbm),
            scratch_shapes=[pltpu.SemaphoreType.DMA((2, 4))],
            compiler_params=pltpu.CompilerParams(vmem_limit_bytes=1048576),
            name="store",
        )(*(pltpu.with_memory_space_constraint(a, pltpu.VMEM) for a in (h, n)))

    row_spec = P(("data", "tp"), None)
    return jax.shard_map(local_block, mesh=mesh, in_specs=(P("data", None), P(None, "tp"), P(None, "tp"), P("tp", None), row_spec, P(None)), out_specs=(row_spec, row_spec), check_vma=False)
```

```python
import functools

import jax
import jax.numpy as jnp
from jax import lax
from jax.experimental import pallas as pl
from jax.experimental.pallas import tpu as pltpu
from jax.sharding import PartitionSpec as P

EPS = 1e-5
ROWS = 256
CHUNKS = 4
HALF = 128
LATE = 32
BLOCK = 1024
STEPS = BLOCK // ROWS
D = 2048
F = 1024
HID_COLS = F // CHUNKS
OUT_COLS = D // CHUNKS
HID_SLOTS = 8
SUM_SLOTS = 2
FIRST = 2 * STEPS
SECOND = FIRST + STEPS
THIRD = SECOND + 4 * STEPS
TILES = 8 * STEPS


def kernel(x_hbm, wg_hbm, wu_hbm, wd_hbm, res_hbm, gain_hbm, h_ref, n_ref, sum_in, sib_own, x_buf, wg, wu, wd, wd_relay, hid, tiles, hid_in, sib_in, sum_out, sum_last, sum_ld, res_ld, sib_ld, gain_ref,
           x_sem, w_sem, wr_sem, relay_ssem, relay_rsem, sib_ssem, sib_rsem, sum_ssem, sum_rsem, ld_sem, res_sem, sibld_sem, gain_sem):
    me = lax.axis_index("tp")
    c, cx, cy = me % 2, (me // 2) % 2, me // 4
    sib = cy * 4 + cx * 2 + (1 - c)
    xn = cy * 4 + (1 - cx) * 2
    yn = (1 - cy) * 4 + cx * 2

    barrier = pltpu.get_barrier_semaphore()
    for dev in (sib, (1 - c) * (yn + 1) + c * xn, (1 - c) * xn + c * (yn + 1)):
        pl.semaphore_signal(barrier, inc=1, device_id={"tp": dev}, device_id_type=pl.DeviceIdType.MESH)

    def kinds(i):
        past_first, past_second, past_third = (i + TILES - FIRST) // TILES, (i + TILES - SECOND) // TILES, (i + TILES - THIRD) // TILES
        return 1 - past_first, past_first - past_second, past_second - past_third, past_third

    def row_of(i):
        diag, to_sib, to_chip, kept = kinds(i)
        q = i % 4
        direction = (1 - c) + (q // 2) * (2 * c - 1)
        ty = diag * (1 - cy) + to_chip * (cy + direction * (1 - 2 * cy)) + (to_sib + kept) * cy
        tx = diag * (1 - cx) + to_chip * (cx + (1 - direction) * (1 - 2 * cx)) + (to_sib + kept) * cx
        tc = (diag + to_chip) * (i % 2) + to_sib * (1 - c) + kept * c
        k = diag * (i // 2) + to_chip * ((i - SECOND) // 4) + (to_sib + kept) * (i % STEPS)
        return pl.multiple_of((ty * 4 + tx * 2 + tc) * BLOCK + k * ROWS, ROWS)

    def x_copy(i):
        return pltpu.make_async_copy(x_hbm.at[pl.ds(row_of(i), ROWS)], x_buf.at[i % 2], x_sem.at[i % 2])

    def wd_copy(n):
        rows = pl.ds(n * (F // CHUNKS), F // CHUNKS)
        return pltpu.make_async_copy(wd_hbm.at[rows], wd.at[rows], w_sem.at[2 + n])

    for n in range(CHUNKS):
        wd_copy(n).start()
    early = [pltpu.make_async_copy(wg_hbm, wg, w_sem.at[0]), pltpu.make_async_copy(wu_hbm, wu, w_sem.at[1]), pltpu.make_async_copy(gain_hbm, gain_ref, gain_sem)]
    for copy in early:
        copy.start()
    x_copy(0).start()

    out_chip = (1 - c) * xn + c * yn

    def w_relay_copy(n):
        rows = pl.ds(n * (F // CHUNKS), F // CHUNKS)
        return pltpu.make_async_remote_copy(
            src_ref=wd.at[rows], dst_ref=wd_relay.at[rows], send_sem=wr_sem.at[0, n], recv_sem=wr_sem.at[1, n],
            device_id={"tp": out_chip + 1 - c}, device_id_type=pl.DeviceIdType.MESH)

    def relay_copy(i):
        return pltpu.make_async_remote_copy(
            src_ref=hid.at[i % HID_SLOTS], dst_ref=hid_in.at[i % 2, i // 2], send_sem=relay_ssem.at[i % HID_SLOTS],
            recv_sem=relay_rsem.at[i % 2, i // 2], device_id={"tp": out_chip + 1 - c}, device_id_type=pl.DeviceIdType.MESH)

    def sib_copy(slot, group, k):
        to_hbm = isinstance(group, int) and group == 2
        return pltpu.make_async_remote_copy(
            src_ref=tiles.at[slot], dst_ref=sib_own.at[k] if to_hbm else sib_in.at[group, k], send_sem=sib_ssem.at[slot],
            recv_sem=sib_rsem.at[group, k], device_id={"tp": sib}, device_id_type=pl.DeviceIdType.MESH)

    def piece(part):
        return (pl.ds(0, HALF), pl.ds(HALF, HALF), pl.ds(HALF, HALF - LATE), pl.ds(ROWS - LATE, LATE))[part]

    def landing(d, k, part):
        if part < 2:
            return sum_in.at[d, k, part]
        return sum_last.at[d, pl.ds(0, HALF - LATE) if part == 2 else pl.ds(HALF - LATE, LATE)]

    def sum_copy(j, k, part):
        slot = k % SUM_SLOTS
        return pltpu.make_async_remote_copy(
            src_ref=sum_out.at[j, slot, piece(part)], dst_ref=landing(c, k, part),
            send_sem=sum_ssem.at[j, slot, part], recv_sem=sum_rsem.at[c, k, part],
            device_id={"tp": out_chip + j}, device_id_type=pl.DeviceIdType.MESH)

    def sum_arrival(d, k, part):
        return pltpu.make_async_remote_copy(
            src_ref=landing(d, k, part), dst_ref=landing(d, k, part), send_sem=sum_ssem.at[0, 0, 0], recv_sem=sum_rsem.at[d, k, part],
            device_id={"tp": sib}, device_id_type=pl.DeviceIdType.MESH)

    pl.semaphore_wait(barrier, 3)
    for n in range(CHUNKS):
        wd_copy(n).wait()
        w_relay_copy(n).start()
    w_relay_copy(0).wait_recv()
    for copy in early:
        copy.wait()

    @pl.loop(0, TILES)
    def _(i):
        diag, to_sib, to_chip, kept = kinds(i)
        j = i % 2
        k_chip = (i - SECOND) // 4
        k_own = i % STEPS
        stays = to_chip * (i % 4 // 2) + kept
        is_relay = i < FIRST
        in_chip = jnp.logical_and(i >= SECOND, i < THIRD)
        is_own_sib = jnp.logical_and(i >= FIRST, i < SECOND)
        is_sib = jnp.logical_and(in_chip, i % 4 < 2)
        is_sum = jnp.logical_and(in_chip, i % 4 >= 2)
        is_final = i >= THIRD

        @pl.when(i + 1 < TILES)
        def _():
            x_copy(i + 1).start()

        x_copy(i).wait()

        @pl.when(jnp.logical_and(is_relay, i >= HID_SLOTS))
        def _():
            relay_copy(i - HID_SLOTS).wait_send()

        @pl.when(jnp.logical_and(jnp.logical_or(is_sib, is_own_sib), i >= FIRST + 2))
        def _():
            sib_copy(j, 0, 0).wait_send()

        def res_copy():
            return pltpu.make_async_copy(res_hbm.at[pl.ds(pl.multiple_of(k_own * ROWS, ROWS), ROWS)], res_ld, res_sem)

        def sib_load():
            return pltpu.make_async_copy(sib_own.at[k_own], sib_ld, sibld_sem)

        def sum_load(d, half):
            return pltpu.make_async_copy(sum_in.at[d, k_own, half], sum_ld.at[d, pl.ds(half * HALF, HALF)], ld_sem.at[d, half])

        @pl.when(is_final)
        def _():
            res_copy().start()
            sib_copy(0, 2, k_own).wait_recv()
            sib_load().start()
            for d in range(2):
                sum_arrival(d, k_own, 0).wait_recv()
                sum_load(d, 0).start()

            @pl.when(k_own < STEPS - 1)
            def _():
                for d in range(2):
                    sum_arrival(d, k_own, 1).wait_recv()
                    sum_load(d, 1).start()

        hid_slot = diag * (i % HID_SLOTS) + (1 - diag) * HID_SLOTS
        for n in range(CHUNKS):
            cols = slice(n * HID_COLS, (n + 1) * HID_COLS)
            gate = jnp.dot(x_buf[j], wg[:, cols], preferred_element_type=jnp.float32)
            up = jnp.dot(x_buf[j], wu[:, cols], preferred_element_type=jnp.float32)
            hid[hid_slot, :, cols] = (gate * jax.nn.sigmoid(gate) * up).astype(jnp.bfloat16)

        @pl.when(is_relay)
        def _():
            relay_copy(i).start()

        @pl.when(i >= FIRST)
        def _():
            slot = stays * 2 + (1 - stays) * j
            for n in range(CHUNKS):
                cols = slice(n * OUT_COLS, (n + 1) * OUT_COLS)
                tiles[slot, :, cols] = jnp.dot(hid[HID_SLOTS], wd[:, cols], preferred_element_type=jnp.float32).astype(jnp.bfloat16)

        @pl.when(is_sib)
        def _():
            sib_copy(j, j, k_chip).start()

        @pl.when(is_own_sib)
        def _():
            sib_copy(j, 2, k_own).start()

        @pl.when(is_sum)
        def _():
            sib_copy(0, j, k_chip).wait_recv()
            relay_copy(2 * k_chip + j).wait_recv()

            @pl.when(i == SECOND + 2)
            def _():
                for n in range(1, CHUNKS):
                    w_relay_copy(n).wait_recv()

            @pl.when(k_chip >= SUM_SLOTS)
            def _():
                for half in range(2):
                    sum_copy(j, k_chip - SUM_SLOTS, half).wait_send()

            for n in range(CHUNKS):
                cols = slice(n * OUT_COLS, (n + 1) * OUT_COLS)
                relayed = jnp.dot(hid_in[j, k_chip], wd_relay[:, cols], preferred_element_type=jnp.float32).astype(jnp.bfloat16)
                total = tiles[2, :, cols].astype(jnp.float32) + sib_in[j, k_chip, :, cols].astype(jnp.float32)
                sum_out[j, k_chip % SUM_SLOTS, :, cols] = total + relayed.astype(jnp.float32)

            sum_copy(j, k_chip, 0).start()

            @pl.when(k_chip < STEPS - 1)
            def _():
                sum_copy(j, k_chip, 1).start()

            @pl.when(k_chip == STEPS - 1)
            def _():
                for part in (2, 3):
                    sum_copy(j, k_chip, part).start()

        @pl.when(is_final)
        def _():
            res_copy().wait()
            sib_load().wait()

            def finish(start, rows, sums, sums_start):
                @pl.loop(0, rows // 16)
                def _(b):
                    here = pl.ds(pl.multiple_of(sums_start + b * 16, 16), 16)
                    tile = pl.ds(pl.multiple_of(start + b * 16, 16), 16)
                    out = pl.ds(pl.multiple_of(k_own * ROWS + start + b * 16, 16), 16)
                    y_sum = tiles[2, tile].astype(jnp.float32) + sib_ld[tile].astype(jnp.float32)
                    y_sum = y_sum + (sums[0, here] + sums[1, here])
                    h = res_ld[tile].astype(jnp.float32) + y_sum
                    mean_sq = jnp.mean(h * h, axis=-1, keepdims=True)
                    h_ref[out] = h.astype(jnp.bfloat16)
                    n_ref[out] = (h * lax.rsqrt(mean_sq + EPS) * gain_ref[...]).astype(jnp.bfloat16)

            for d in range(2):
                sum_load(d, 0).wait()
            finish(0, HALF, sum_ld, 0)

            @pl.when(k_own < STEPS - 1)
            def _():
                for d in range(2):
                    sum_load(d, 1).wait()
                finish(HALF, HALF, sum_ld, HALF)

            @pl.when(k_own == STEPS - 1)
            def _():
                for part, rows in ((2, HALF - LATE), (3, LATE)):
                    for d in range(2):
                        sum_arrival(d, STEPS - 1, part).wait_recv()
                    start = (part - 2) * (HALF - LATE)
                    finish(HALF + start, rows, sum_last, start)

    for n in range(CHUNKS):
        w_relay_copy(n).wait_send()
    for s in range(HID_SLOTS):
        relay_copy(FIRST - HID_SLOTS + s).wait_send()
    for s in range(2):
        sib_copy(s, 0, 0).wait_send()
    for j in range(2):
        for k in range(STEPS - SUM_SLOTS, STEPS):
            for part in ((0, 1) if k < STEPS - 1 else (0, 2, 3)):
                sum_copy(j, k, part).wait_send()


def store_kernel(h_ref, n_ref, h_hbm, n_hbm, sem):
    copies = []
    for b in range(4):
        rows = pl.ds(b * (BLOCK // 4), BLOCK // 4)
        copies.append(pltpu.make_async_copy(h_ref.at[rows], h_hbm.at[rows], sem.at[0, b]))
        copies.append(pltpu.make_async_copy(n_ref.at[rows], n_hbm.at[rows], sem.at[1, b]))
    for copy in copies:
        copy.start()
    for copy in copies:
        copy.wait()


def solution(mesh):
    def local_block(x_in, w_gate, w_up, w_down, residual, norm_gain):
        hbm = pl.BlockSpec(memory_space=pltpu.HBM)
        vmem = pl.BlockSpec(memory_space=pltpu.VMEM)
        h, n, _, _ = pl.pallas_call(
            kernel,
            out_shape=(
                pltpu.VMEM((BLOCK, D), jnp.bfloat16),
                pltpu.VMEM((BLOCK, D), jnp.bfloat16),
                jax.ShapeDtypeStruct((2, STEPS, 2, HALF, D), jnp.float32),
                jax.ShapeDtypeStruct((STEPS, ROWS, D), jnp.bfloat16),
            ),
            in_specs=[hbm] * 6,
            out_specs=(vmem, vmem, hbm, hbm),
            scratch_shapes=[
                pltpu.VMEM((2, ROWS, D), jnp.bfloat16),
                pltpu.VMEM((D, F), jnp.bfloat16),
                pltpu.VMEM((D, F), jnp.bfloat16),
                pltpu.VMEM((F, D), jnp.bfloat16),
                pltpu.VMEM((F, D), jnp.bfloat16),
                pltpu.VMEM((HID_SLOTS + 1, ROWS, F), jnp.bfloat16),
                pltpu.VMEM((3, ROWS, D), jnp.bfloat16),
                pltpu.VMEM((2, STEPS, ROWS, F), jnp.bfloat16),
                pltpu.VMEM((2, STEPS, ROWS, D), jnp.bfloat16),
                pltpu.VMEM((2, SUM_SLOTS, ROWS, D), jnp.float32),
                pltpu.VMEM((2, HALF, D), jnp.float32),
                pltpu.VMEM((2, ROWS, D), jnp.float32),
                pltpu.VMEM((ROWS, D), jnp.bfloat16),
                pltpu.VMEM((ROWS, D), jnp.bfloat16),
                pltpu.VMEM((1, D), jnp.float32),
                pltpu.SemaphoreType.DMA((2,)),
                pltpu.SemaphoreType.DMA((2 + CHUNKS,)),
                pltpu.SemaphoreType.DMA((2, CHUNKS)),
                pltpu.SemaphoreType.DMA((HID_SLOTS,)),
                pltpu.SemaphoreType.DMA((2, STEPS)),
                pltpu.SemaphoreType.DMA((2,)),
                pltpu.SemaphoreType.DMA((3, STEPS)),
                pltpu.SemaphoreType.DMA((2, SUM_SLOTS, 4)),
                pltpu.SemaphoreType.DMA((2, STEPS, 4)),
                pltpu.SemaphoreType.DMA((2, 2)),
                pltpu.SemaphoreType.DMA,
                pltpu.SemaphoreType.DMA,
                pltpu.SemaphoreType.DMA,
            ],
            compiler_params=pltpu.CompilerParams(collective_id=0, has_side_effects=True, vmem_limit_bytes=58000000),
            name="mlp_reduce",
        )(x_in, w_gate, w_up, w_down, residual, norm_gain.reshape(1, D))
        return pl.pallas_call(
            store_kernel,
            out_shape=(jax.ShapeDtypeStruct((BLOCK, D), jnp.bfloat16), jax.ShapeDtypeStruct((BLOCK, D), jnp.bfloat16)),
            in_specs=[vmem, vmem],
            out_specs=(hbm, hbm),
            scratch_shapes=[pltpu.SemaphoreType.DMA((2, 4))],
            compiler_params=pltpu.CompilerParams(vmem_limit_bytes=1048576),
            name="store",
        )(*(pltpu.with_memory_space_constraint(a, pltpu.VMEM) for a in (h, n)))

    row_spec = P(("data", "tp"), None)
    return jax.shard_map(local_block, mesh=mesh, in_specs=(P("data", None), P(None, "tp"), P(None, "tp"), P("tp", None), row_spec, P(None)), out_specs=(row_spec, row_spec), check_vma=False)
```

```python
import functools

import jax
import jax.numpy as jnp
from jax import lax
from jax.experimental import pallas as pl
from jax.experimental.pallas import tpu as pltpu
from jax.sharding import PartitionSpec as P

EPS = 1e-5
ROWS = 256
CHUNKS = 4
HALF = 128
LATE = 32
BLOCK = 1024
STEPS = BLOCK // ROWS
D = 2048
F = 1024
HID_COLS = F // CHUNKS
OUT_COLS = D // CHUNKS
HID_SLOTS = 8
SUM_SLOTS = 2
FIRST = 2 * STEPS
SECOND = FIRST + STEPS
THIRD = SECOND + 4 * STEPS
TILES = 8 * STEPS


def kernel(x_hbm, wg_hbm, wu_hbm, wd_hbm, res_hbm, gain_hbm, h_ref, n_ref, sum_in, sib_own, x_buf, wg, wu, wd, wd_relay, hid, tiles, hid_in, sib_in, sum_out, sum_last, sum_ld, res_ld, sib_ld, gain_ref,
           x_sem, w_sem, wr_sem, relay_ssem, relay_rsem, sib_ssem, sib_rsem, sum_ssem, sum_rsem, ld_sem, res_sem, sibld_sem):
    me = lax.axis_index("tp")
    c, cx, cy = me % 2, (me // 2) % 2, me // 4
    sib = cy * 4 + cx * 2 + (1 - c)
    xn = cy * 4 + (1 - cx) * 2
    yn = (1 - cy) * 4 + cx * 2

    barrier = pltpu.get_barrier_semaphore()
    for dev in (sib, (1 - c) * (yn + 1) + c * xn, (1 - c) * xn + c * (yn + 1)):
        pl.semaphore_signal(barrier, inc=1, device_id={"tp": dev}, device_id_type=pl.DeviceIdType.MESH)

    def kinds(i):
        past_first, past_second, past_third = (i + TILES - FIRST) // TILES, (i + TILES - SECOND) // TILES, (i + TILES - THIRD) // TILES
        return 1 - past_first, past_first - past_second, past_second - past_third, past_third

    def row_of(i):
        diag, to_sib, to_chip, kept = kinds(i)
        q = i % 4
        direction = (1 - c) + (q // 2) * (2 * c - 1)
        ty = diag * (1 - cy) + to_chip * (cy + direction * (1 - 2 * cy)) + (to_sib + kept) * cy
        tx = diag * (1 - cx) + to_chip * (cx + (1 - direction) * (1 - 2 * cx)) + (to_sib + kept) * cx
        tc = (diag + to_chip) * (i % 2) + to_sib * (1 - c) + kept * c
        k = diag * (i // 2) + to_chip * ((i - SECOND) // 4) + (to_sib + kept) * (i % STEPS)
        return pl.multiple_of((ty * 4 + tx * 2 + tc) * BLOCK + k * ROWS, ROWS)

    def x_copy(i):
        return pltpu.make_async_copy(x_hbm.at[pl.ds(row_of(i), ROWS)], x_buf.at[i % 2], x_sem.at[i % 2])

    early = [pltpu.make_async_copy(src, dst, w_sem.at[n]) for n, (src, dst) in enumerate(((wg_hbm, wg), (wu_hbm, wu), (wd_hbm, wd), (gain_hbm, gain_ref)))]
    for copy in early:
        copy.start()
    x_copy(0).start()

    out_chip = (1 - c) * xn + c * yn

    def w_relay_copy(n):
        rows = (pl.ds(0, 128), pl.ds(128, F - 128))[n]
        return pltpu.make_async_remote_copy(
            src_ref=wd_hbm.at[rows], dst_ref=wd_relay.at[rows], send_sem=wr_sem.at[0, n], recv_sem=wr_sem.at[1, n],
            device_id={"tp": out_chip + 1 - c}, device_id_type=pl.DeviceIdType.MESH)

    def relay_copy(i):
        return pltpu.make_async_remote_copy(
            src_ref=hid.at[i % HID_SLOTS], dst_ref=hid_in.at[i % 2, i // 2], send_sem=relay_ssem.at[i % HID_SLOTS],
            recv_sem=relay_rsem.at[i % 2, i // 2], device_id={"tp": out_chip + 1 - c}, device_id_type=pl.DeviceIdType.MESH)

    def sib_copy(slot, group, k):
        to_hbm = isinstance(group, int) and group == 2
        return pltpu.make_async_remote_copy(
            src_ref=tiles.at[slot], dst_ref=sib_own.at[k] if to_hbm else sib_in.at[group, k], send_sem=sib_ssem.at[slot],
            recv_sem=sib_rsem.at[group, k], device_id={"tp": sib}, device_id_type=pl.DeviceIdType.MESH)

    def piece(part):
        return (pl.ds(0, HALF), pl.ds(HALF, HALF), pl.ds(HALF, HALF - LATE), pl.ds(ROWS - LATE, LATE))[part]

    def landing(d, k, part):
        if part < 2:
            return sum_in.at[d, k, part]
        return sum_last.at[d, pl.ds(0, HALF - LATE) if part == 2 else pl.ds(HALF - LATE, LATE)]

    def sum_copy(j, k, part):
        slot = k % SUM_SLOTS
        return pltpu.make_async_remote_copy(
            src_ref=sum_out.at[j, slot, piece(part)], dst_ref=landing(c, k, part),
            send_sem=sum_ssem.at[j, slot, part], recv_sem=sum_rsem.at[c, k, part],
            device_id={"tp": out_chip + j}, device_id_type=pl.DeviceIdType.MESH)

    def sum_arrival(d, k, part):
        return pltpu.make_async_remote_copy(
            src_ref=landing(d, k, part), dst_ref=landing(d, k, part), send_sem=sum_ssem.at[0, 0, 0], recv_sem=sum_rsem.at[d, k, part],
            device_id={"tp": sib}, device_id_type=pl.DeviceIdType.MESH)

    pl.semaphore_wait(barrier, 3)
    for n in range(2):
        w_relay_copy(n).start()
    w_relay_copy(0).wait_recv()
    for copy in early:
        copy.wait()

    @pl.loop(0, TILES)
    def _(i):
        diag, to_sib, to_chip, kept = kinds(i)
        j = i % 2
        k_chip = (i - SECOND) // 4
        k_own = i % STEPS
        stays = to_chip * (i % 4 // 2) + kept
        is_relay = i < FIRST
        in_chip = jnp.logical_and(i >= SECOND, i < THIRD)
        is_own_sib = jnp.logical_and(i >= FIRST, i < SECOND)
        is_sib = jnp.logical_and(in_chip, i % 4 < 2)
        is_sum = jnp.logical_and(in_chip, i % 4 >= 2)
        is_final = i >= THIRD

        @pl.when(i + 1 < TILES)
        def _():
            x_copy(i + 1).start()

        x_copy(i).wait()

        @pl.when(jnp.logical_and(is_relay, i >= HID_SLOTS))
        def _():
            relay_copy(i - HID_SLOTS).wait_send()

        @pl.when(jnp.logical_and(jnp.logical_or(is_sib, is_own_sib), i >= FIRST + 2))
        def _():
            sib_copy(j, 0, 0).wait_send()

        def res_copy():
            return pltpu.make_async_copy(res_hbm.at[pl.ds(pl.multiple_of(k_own * ROWS, ROWS), ROWS)], res_ld, res_sem)

        def sib_load():
            return pltpu.make_async_copy(sib_own.at[k_own], sib_ld, sibld_sem)

        def sum_load(d, half):
            return pltpu.make_async_copy(sum_in.at[d, k_own, half], sum_ld.at[d, pl.ds(half * HALF, HALF)], ld_sem.at[d, half])

        @pl.when(is_final)
        def _():
            res_copy().start()
            sib_copy(0, 2, k_own).wait_recv()
            sib_load().start()
            for d in range(2):
                sum_arrival(d, k_own, 0).wait_recv()
                sum_load(d, 0).start()

            @pl.when(k_own < STEPS - 1)
            def _():
                for d in range(2):
                    sum_arrival(d, k_own, 1).wait_recv()
                    sum_load(d, 1).start()

        hid_slot = diag * (i % HID_SLOTS) + (1 - diag) * HID_SLOTS
        for n in range(CHUNKS):
            cols = slice(n * HID_COLS, (n + 1) * HID_COLS)
            gate = jnp.dot(x_buf[j], wg[:, cols], preferred_element_type=jnp.float32)
            up = jnp.dot(x_buf[j], wu[:, cols], preferred_element_type=jnp.float32)
            hid[hid_slot, :, cols] = (gate * jax.nn.sigmoid(gate) * up).astype(jnp.bfloat16)

        @pl.when(is_relay)
        def _():
            relay_copy(i).start()

        @pl.when(i >= FIRST)
        def _():
            slot = stays * 2 + (1 - stays) * j
            for n in range(CHUNKS):
                cols = slice(n * OUT_COLS, (n + 1) * OUT_COLS)
                tiles[slot, :, cols] = jnp.dot(hid[HID_SLOTS], wd[:, cols], preferred_element_type=jnp.float32).astype(jnp.bfloat16)

        @pl.when(is_sib)
        def _():
            sib_copy(j, j, k_chip).start()

        @pl.when(is_own_sib)
        def _():
            sib_copy(j, 2, k_own).start()

        @pl.when(is_sum)
        def _():
            sib_copy(0, j, k_chip).wait_recv()
            relay_copy(2 * k_chip + j).wait_recv()

            @pl.when(i == SECOND + 2)
            def _():
                w_relay_copy(1).wait_recv()

            @pl.when(k_chip >= SUM_SLOTS)
            def _():
                for half in range(2):
                    sum_copy(j, k_chip - SUM_SLOTS, half).wait_send()

            for n in range(CHUNKS):
                cols = slice(n * OUT_COLS, (n + 1) * OUT_COLS)
                relayed = jnp.dot(hid_in[j, k_chip], wd_relay[:, cols], preferred_element_type=jnp.float32).astype(jnp.bfloat16)
                total = tiles[2, :, cols].astype(jnp.float32) + sib_in[j, k_chip, :, cols].astype(jnp.float32)
                sum_out[j, k_chip % SUM_SLOTS, :, cols] = total + relayed.astype(jnp.float32)

            sum_copy(j, k_chip, 0).start()

            @pl.when(k_chip < STEPS - 1)
            def _():
                sum_copy(j, k_chip, 1).start()

            @pl.when(k_chip == STEPS - 1)
            def _():
                for part in (2, 3):
                    sum_copy(j, k_chip, part).start()

        @pl.when(is_final)
        def _():
            res_copy().wait()
            sib_load().wait()

            def finish(start, rows, sums, sums_start):
                @pl.loop(0, rows // 16)
                def _(b):
                    here = pl.ds(pl.multiple_of(sums_start + b * 16, 16), 16)
                    tile = pl.ds(pl.multiple_of(start + b * 16, 16), 16)
                    out = pl.ds(pl.multiple_of(k_own * ROWS + start + b * 16, 16), 16)
                    y_sum = tiles[2, tile].astype(jnp.float32) + sib_ld[tile].astype(jnp.float32)
                    y_sum = y_sum + (sums[0, here] + sums[1, here])
                    h = res_ld[tile].astype(jnp.float32) + y_sum
                    mean_sq = jnp.mean(h * h, axis=-1, keepdims=True)
                    h_ref[out] = h.astype(jnp.bfloat16)
                    n_ref[out] = (h * lax.rsqrt(mean_sq + EPS) * gain_ref[...]).astype(jnp.bfloat16)

            for d in range(2):
                sum_load(d, 0).wait()
            finish(0, HALF, sum_ld, 0)

            @pl.when(k_own < STEPS - 1)
            def _():
                for d in range(2):
                    sum_load(d, 1).wait()
                finish(HALF, HALF, sum_ld, HALF)

            @pl.when(k_own == STEPS - 1)
            def _():
                for part, rows in ((2, HALF - LATE), (3, LATE)):
                    for d in range(2):
                        sum_arrival(d, STEPS - 1, part).wait_recv()
                    start = (part - 2) * (HALF - LATE)
                    finish(HALF + start, rows, sum_last, start)

    for n in range(2):
        w_relay_copy(n).wait_send()
    for s in range(HID_SLOTS):
        relay_copy(FIRST - HID_SLOTS + s).wait_send()
    for s in range(2):
        sib_copy(s, 0, 0).wait_send()
    for j in range(2):
        for k in range(STEPS - SUM_SLOTS, STEPS):
            for part in ((0, 1) if k < STEPS - 1 else (0, 2, 3)):
                sum_copy(j, k, part).wait_send()


def store_kernel(h_ref, n_ref, h_hbm, n_hbm, sem):
    copies = []
    for b in range(4):
        rows = pl.ds(b * (BLOCK // 4), BLOCK // 4)
        copies.append(pltpu.make_async_copy(h_ref.at[rows], h_hbm.at[rows], sem.at[0, b]))
        copies.append(pltpu.make_async_copy(n_ref.at[rows], n_hbm.at[rows], sem.at[1, b]))
    for copy in copies:
        copy.start()
    for copy in copies:
        copy.wait()


def solution(mesh):
    def local_block(x_in, w_gate, w_up, w_down, residual, norm_gain):
        hbm = pl.BlockSpec(memory_space=pltpu.HBM)
        vmem = pl.BlockSpec(memory_space=pltpu.VMEM)
        h, n, _, _ = pl.pallas_call(
            kernel,
            out_shape=(
                pltpu.VMEM((BLOCK, D), jnp.bfloat16),
                pltpu.VMEM((BLOCK, D), jnp.bfloat16),
                jax.ShapeDtypeStruct((2, STEPS, 2, HALF, D), jnp.float32),
                jax.ShapeDtypeStruct((STEPS, ROWS, D), jnp.bfloat16),
            ),
            in_specs=[hbm] * 6,
            out_specs=(vmem, vmem, hbm, hbm),
            scratch_shapes=[
                pltpu.VMEM((2, ROWS, D), jnp.bfloat16),
                pltpu.VMEM((D, F), jnp.bfloat16),
                pltpu.VMEM((D, F), jnp.bfloat16),
                pltpu.VMEM((F, D), jnp.bfloat16),
                pltpu.VMEM((F, D), jnp.bfloat16),
                pltpu.VMEM((HID_SLOTS + 1, ROWS, F), jnp.bfloat16),
                pltpu.VMEM((3, ROWS, D), jnp.bfloat16),
                pltpu.VMEM((2, STEPS, ROWS, F), jnp.bfloat16),
                pltpu.VMEM((2, STEPS, ROWS, D), jnp.bfloat16),
                pltpu.VMEM((2, SUM_SLOTS, ROWS, D), jnp.float32),
                pltpu.VMEM((2, HALF, D), jnp.float32),
                pltpu.VMEM((2, ROWS, D), jnp.float32),
                pltpu.VMEM((ROWS, D), jnp.bfloat16),
                pltpu.VMEM((ROWS, D), jnp.bfloat16),
                pltpu.VMEM((1, D), jnp.float32),
                pltpu.SemaphoreType.DMA((2,)),
                pltpu.SemaphoreType.DMA((4,)),
                pltpu.SemaphoreType.DMA((2, 2)),
                pltpu.SemaphoreType.DMA((HID_SLOTS,)),
                pltpu.SemaphoreType.DMA((2, STEPS)),
                pltpu.SemaphoreType.DMA((2,)),
                pltpu.SemaphoreType.DMA((3, STEPS)),
                pltpu.SemaphoreType.DMA((2, SUM_SLOTS, 4)),
                pltpu.SemaphoreType.DMA((2, STEPS, 4)),
                pltpu.SemaphoreType.DMA((2, 2)),
                pltpu.SemaphoreType.DMA,
                pltpu.SemaphoreType.DMA,
            ],
            compiler_params=pltpu.CompilerParams(collective_id=0, has_side_effects=True, vmem_limit_bytes=58000000),
            name="mlp_reduce",
        )(x_in, w_gate, w_up, w_down, residual, norm_gain.reshape(1, D))
        return pl.pallas_call(
            store_kernel,
            out_shape=(jax.ShapeDtypeStruct((BLOCK, D), jnp.bfloat16), jax.ShapeDtypeStruct((BLOCK, D), jnp.bfloat16)),
            in_specs=[vmem, vmem],
            out_specs=(hbm, hbm),
            scratch_shapes=[pltpu.SemaphoreType.DMA((2, 4))],
            compiler_params=pltpu.CompilerParams(vmem_limit_bytes=1048576),
            name="store",
        )(*(pltpu.with_memory_space_constraint(a, pltpu.VMEM) for a in (h, n)))

    row_spec = P(("data", "tp"), None)
    return jax.shard_map(local_block, mesh=mesh, in_specs=(P("data", None), P(None, "tp"), P(None, "tp"), P("tp", None), row_spec, P(None)), out_specs=(row_spec, row_spec), check_vma=False)
```

```python
import functools

import jax
import jax.numpy as jnp
from jax import lax
from jax.experimental import pallas as pl
from jax.experimental.pallas import tpu as pltpu
from jax.sharding import PartitionSpec as P

EPS = 1e-5
ROWS = 256
CHUNKS = 4
HALF = 128
LATE = 16
BLOCK = 1024
STEPS = BLOCK // ROWS
D = 2048
F = 1024
HID_COLS = F // CHUNKS
OUT_COLS = D // CHUNKS
SUM_SLOTS = 2
FIRST = 2 * STEPS
SECOND = FIRST + STEPS
THIRD = SECOND + 4 * STEPS
TILES = 8 * STEPS


def kernel(x_hbm, wg_hbm, wu_hbm, wd_hbm, res_hbm, gain_hbm, h_ref, n_ref, sum_in, sib_own, x_buf, wg, wu, wd, wd_relay, hid, tiles, hid_in, sib_in, sum_out, sum_last, sum_ld, res_ld, sib_ld, gain_ref,
           x_sem, w_sem, wr_sem, relay_ssem, relay_rsem, sib_ssem, sib_rsem, sum_ssem, sum_rsem, ld_sem, res_sem, sibld_sem, ready):
    me = lax.axis_index("tp")
    c, cx, cy = me % 2, (me // 2) % 2, me // 4
    sib = cy * 4 + cx * 2 + (1 - c)
    xn = cy * 4 + (1 - cx) * 2
    yn = (1 - cy) * 4 + cx * 2

    barrier = pltpu.get_barrier_semaphore()
    source = (1 - c) * (yn + 1) + c * xn
    for dev in (sib, source):
        pl.semaphore_signal(barrier, inc=1, device_id={"tp": dev}, device_id_type=pl.DeviceIdType.MESH)

    def kinds(i):
        past_first, past_second, past_third = (i + TILES - FIRST) // TILES, (i + TILES - SECOND) // TILES, (i + TILES - THIRD) // TILES
        return 1 - past_first, past_first - past_second, past_second - past_third, past_third

    def row_of(i):
        diag, to_sib, to_chip, kept = kinds(i)
        q = i % 4
        direction = (1 - c) + (q // 2) * (2 * c - 1)
        ty = diag * (1 - cy) + to_chip * (cy + direction * (1 - 2 * cy)) + (to_sib + kept) * cy
        tx = diag * (1 - cx) + to_chip * (cx + (1 - direction) * (1 - 2 * cx)) + (to_sib + kept) * cx
        tc = (diag + to_chip) * (i % 2) + to_sib * (1 - c) + kept * c
        k = diag * (i // 2) + to_chip * ((i - SECOND) // 4) + (to_sib + kept) * (i % STEPS)
        return pl.multiple_of((ty * 4 + tx * 2 + tc) * BLOCK + k * ROWS, ROWS)

    def x_copy(i):
        return pltpu.make_async_copy(x_hbm.at[pl.ds(row_of(i), ROWS)], x_buf.at[i % 2], x_sem.at[i % 2])

    early = [pltpu.make_async_copy(src, dst, w_sem.at[n]) for n, (src, dst) in enumerate(((wg_hbm, wg), (wu_hbm, wu), (wd_hbm, wd), (gain_hbm, gain_ref)))]
    for copy in early:
        copy.start()
    x_copy(0).start()

    out_chip = (1 - c) * xn + c * yn

    def w_relay_copy(n):
        rows = (pl.ds(0, 128), pl.ds(128, F - 128))[n]
        return pltpu.make_async_remote_copy(
            src_ref=wd_hbm.at[rows], dst_ref=wd_relay.at[rows], send_sem=wr_sem.at[0, n], recv_sem=wr_sem.at[1, n],
            device_id={"tp": out_chip + 1 - c}, device_id_type=pl.DeviceIdType.MESH)

    def relay_copy(i):
        return pltpu.make_async_remote_copy(
            src_ref=hid.at[i], dst_ref=hid_in.at[i % 2, i // 2], send_sem=relay_ssem,
            recv_sem=relay_rsem.at[i % 2, i // 2], device_id={"tp": out_chip + 1 - c}, device_id_type=pl.DeviceIdType.MESH)

    def sib_copy(slot, group, k):
        to_hbm = isinstance(group, int) and group == 2
        return pltpu.make_async_remote_copy(
            src_ref=tiles.at[slot], dst_ref=sib_own.at[k] if to_hbm else sib_in.at[group, k], send_sem=sib_ssem.at[slot],
            recv_sem=sib_rsem.at[group, k], device_id={"tp": sib}, device_id_type=pl.DeviceIdType.MESH)

    last = STEPS - 1
    parts = ((0, HALF), (HALF, HALF - LATE), (ROWS - LATE, LATE))

    def landing(d, k, part):
        if part is None:
            return sum_in.at[d, k]
        start, rows = parts[part]
        return sum_in.at[d, last, pl.ds(0, HALF)] if part == 0 else sum_last.at[d, pl.ds(start - HALF, rows)]

    def sum_copy(j, k, part=None):
        slot = k % SUM_SLOTS
        return pltpu.make_async_remote_copy(
            src_ref=sum_out.at[j, slot] if part is None else sum_out.at[j, slot, pl.ds(*parts[part])], dst_ref=landing(c, k, part),
            send_sem=sum_ssem.at[j, slot + (part or 0)], recv_sem=sum_rsem.at[c, k + (part or 0)],
            device_id={"tp": out_chip + j}, device_id_type=pl.DeviceIdType.MESH)

    def sum_arrival(d, k, part=None):
        return pltpu.make_async_remote_copy(
            src_ref=landing(d, k, part), dst_ref=landing(d, k, part), send_sem=sum_ssem.at[0, 0], recv_sem=sum_rsem.at[d, k + (part or 0)],
            device_id={"tp": sib}, device_id_type=pl.DeviceIdType.MESH)

    pl.semaphore_wait(barrier, 2)
    for n in range(2):
        w_relay_copy(n).start()
    w_relay_copy(0).wait_recv()
    pl.semaphore_signal(ready, inc=1, device_id={"tp": source}, device_id_type=pl.DeviceIdType.MESH)
    for copy in early:
        copy.wait()

    @pl.loop(0, TILES)
    def _(i):
        diag, to_sib, to_chip, kept = kinds(i)
        j = i % 2
        k_chip = (i - SECOND) // 4
        k_own = i % STEPS
        stays = to_chip * (i % 4 // 2) + kept
        is_relay = i < FIRST
        in_chip = jnp.logical_and(i >= SECOND, i < THIRD)
        is_own_sib = jnp.logical_and(i >= FIRST, i < SECOND)
        is_sib = jnp.logical_and(in_chip, i % 4 < 2)
        is_sum = jnp.logical_and(in_chip, i % 4 >= 2)
        is_final = i >= THIRD

        @pl.when(i + 1 < TILES)
        def _():
            x_copy(i + 1).start()

        x_copy(i).wait()

        @pl.when(jnp.logical_and(jnp.logical_or(is_sib, is_own_sib), i >= FIRST + 2))
        def _():
            sib_copy(j, 0, 0).wait_send()

        def res_copy():
            return pltpu.make_async_copy(res_hbm.at[pl.ds(pl.multiple_of(k_own * ROWS, ROWS), ROWS)], res_ld, res_sem)

        def sib_load():
            return pltpu.make_async_copy(sib_own.at[k_own], sib_ld, sibld_sem)

        def sum_load(d, rows):
            return pltpu.make_async_copy(sum_in.at[d, k_own, pl.ds(0, rows)], sum_ld.at[d, pl.ds(0, rows)], ld_sem.at[d])

        @pl.when(is_final)
        def _():
            res_copy().start()
            sib_copy(0, 2, k_own).wait_recv()
            sib_load().start()

            @pl.when(k_own < last)
            def _():
                for d in range(2):
                    sum_arrival(d, k_own).wait_recv()
                    sum_load(d, ROWS).start()

            @pl.when(k_own == last)
            def _():
                for d in range(2):
                    sum_arrival(d, last, 0).wait_recv()
                    sum_load(d, HALF).start()

        hid_slot = diag * i + (1 - diag) * FIRST
        for n in range(CHUNKS):
            cols = slice(n * HID_COLS, (n + 1) * HID_COLS)
            gate = jnp.dot(x_buf[j], wg[:, cols], preferred_element_type=jnp.float32)
            up = jnp.dot(x_buf[j], wu[:, cols], preferred_element_type=jnp.float32)
            hid[hid_slot, :, cols] = (gate * jax.nn.sigmoid(gate) * up).astype(jnp.bfloat16)

        @pl.when(is_relay)
        def _():
            relay_copy(i).start()

        @pl.when(i >= FIRST)
        def _():
            slot = stays * 2 + (1 - stays) * j
            for n in range(CHUNKS):
                cols = slice(n * OUT_COLS, (n + 1) * OUT_COLS)
                tiles[slot, :, cols] = jnp.dot(hid[FIRST], wd[:, cols], preferred_element_type=jnp.float32).astype(jnp.bfloat16)

        @pl.when(is_sib)
        def _():
            sib_copy(j, j, k_chip).start()

        @pl.when(is_own_sib)
        def _():
            sib_copy(j, 2, k_own).start()

        @pl.when(is_sum)
        def _():
            sib_copy(0, j, k_chip).wait_recv()
            relay_copy(2 * k_chip + j).wait_recv()

            @pl.when(i == SECOND + 2)
            def _():
                w_relay_copy(1).wait_recv()
                pl.semaphore_wait(ready, 1)

            @pl.when(k_chip >= SUM_SLOTS)
            def _():
                sum_copy(j, k_chip - SUM_SLOTS).wait_send()

            for n in range(CHUNKS):
                cols = slice(n * OUT_COLS, (n + 1) * OUT_COLS)
                relayed = jnp.dot(hid_in[j, k_chip], wd_relay[:, cols], preferred_element_type=jnp.float32).astype(jnp.bfloat16)
                total = tiles[2, :, cols].astype(jnp.float32) + sib_in[j, k_chip, :, cols].astype(jnp.float32)
                sum_out[j, k_chip % SUM_SLOTS, :, cols] = total + relayed.astype(jnp.float32)

            @pl.when(k_chip < last)
            def _():
                sum_copy(j, k_chip).start()

            @pl.when(k_chip == last)
            def _():
                for part in range(3):
                    sum_copy(j, last, part).start()

        @pl.when(is_final)
        def _():
            res_copy().wait()
            sib_load().wait()

            def finish(start, rows, sums, sums_start):
                @pl.loop(0, rows // 16)
                def _(b):
                    here = pl.ds(pl.multiple_of(sums_start + b * 16, 16), 16)
                    tile = pl.ds(pl.multiple_of(start + b * 16, 16), 16)
                    out = pl.ds(pl.multiple_of(k_own * ROWS + start + b * 16, 16), 16)
                    y_sum = tiles[2, tile].astype(jnp.float32) + sib_ld[tile].astype(jnp.float32)
                    y_sum = y_sum + (sums[0, here] + sums[1, here])
                    h = res_ld[tile].astype(jnp.float32) + y_sum
                    mean_sq = jnp.mean(h * h, axis=-1, keepdims=True)
                    h_ref[out] = h.astype(jnp.bfloat16)
                    n_ref[out] = (h * lax.rsqrt(mean_sq + EPS) * gain_ref[...]).astype(jnp.bfloat16)

            @pl.when(k_own < last)
            def _():
                for d in range(2):
                    sum_load(d, ROWS).wait()
                finish(0, ROWS, sum_ld, 0)

            @pl.when(k_own == last)
            def _():
                for d in range(2):
                    sum_load(d, HALF).wait()
                finish(0, HALF, sum_ld, 0)
                for part in (1, 2):
                    for d in range(2):
                        sum_arrival(d, last, part).wait_recv()
                    start, rows = parts[part]
                    finish(start, rows, sum_last, start - HALF)

    for n in range(2):
        w_relay_copy(n).wait_send()
    sent = hid.at[pl.ds(0, FIRST)]
    pltpu.make_async_copy(sent, sent, relay_ssem).wait()
    for s in range(2):
        sib_copy(s, 0, 0).wait_send()
    for j in range(2):
        sum_copy(j, last - 1).wait_send()
        for part in range(3):
            sum_copy(j, last, part).wait_send()


def store_kernel(h_ref, n_ref, h_hbm, n_hbm, sem):
    copies = []
    for b in range(4):
        rows = pl.ds(b * (BLOCK // 4), BLOCK // 4)
        copies.append(pltpu.make_async_copy(h_ref.at[rows], h_hbm.at[rows], sem.at[0, b]))
        copies.append(pltpu.make_async_copy(n_ref.at[rows], n_hbm.at[rows], sem.at[1, b]))
    for copy in copies:
        copy.start()
    for copy in copies:
        copy.wait()


def solution(mesh):
    def local_block(x_in, w_gate, w_up, w_down, residual, norm_gain):
        hbm = pl.BlockSpec(memory_space=pltpu.HBM)
        vmem = pl.BlockSpec(memory_space=pltpu.VMEM)
        h, n, _, _ = pl.pallas_call(
            kernel,
            out_shape=(
                pltpu.VMEM((BLOCK, D), jnp.bfloat16),
                pltpu.VMEM((BLOCK, D), jnp.bfloat16),
                jax.ShapeDtypeStruct((2, STEPS, ROWS, D), jnp.float32),
                jax.ShapeDtypeStruct((STEPS, ROWS, D), jnp.bfloat16),
            ),
            in_specs=[hbm] * 6,
            out_specs=(vmem, vmem, hbm, hbm),
            scratch_shapes=[
                pltpu.VMEM((2, ROWS, D), jnp.bfloat16),
                pltpu.VMEM((D, F), jnp.bfloat16),
                pltpu.VMEM((D, F), jnp.bfloat16),
                pltpu.VMEM((F, D), jnp.bfloat16),
                pltpu.VMEM((F, D), jnp.bfloat16),
                pltpu.VMEM((FIRST + 1, ROWS, F), jnp.bfloat16),
                pltpu.VMEM((3, ROWS, D), jnp.bfloat16),
                pltpu.VMEM((2, STEPS, ROWS, F), jnp.bfloat16),
                pltpu.VMEM((2, STEPS, ROWS, D), jnp.bfloat16),
                pltpu.VMEM((2, SUM_SLOTS, ROWS, D), jnp.float32),
                pltpu.VMEM((2, HALF, D), jnp.float32),
                pltpu.VMEM((2, ROWS, D), jnp.float32),
                pltpu.VMEM((ROWS, D), jnp.bfloat16),
                pltpu.VMEM((ROWS, D), jnp.bfloat16),
                pltpu.VMEM((1, D), jnp.float32),
                pltpu.SemaphoreType.DMA((2,)),
                pltpu.SemaphoreType.DMA((4,)),
                pltpu.SemaphoreType.DMA((2, 2)),
                pltpu.SemaphoreType.DMA,
                pltpu.SemaphoreType.DMA((2, STEPS)),
                pltpu.SemaphoreType.DMA((2,)),
                pltpu.SemaphoreType.DMA((3, STEPS)),
                pltpu.SemaphoreType.DMA((2, SUM_SLOTS + 2)),
                pltpu.SemaphoreType.DMA((2, STEPS + 2)),
                pltpu.SemaphoreType.DMA((2,)),
                pltpu.SemaphoreType.DMA,
                pltpu.SemaphoreType.DMA,
                pltpu.SemaphoreType.REGULAR,
            ],
            compiler_params=pltpu.CompilerParams(collective_id=0, has_side_effects=True, vmem_limit_bytes=58000000),
            name="mlp_reduce",
        )(x_in, w_gate, w_up, w_down, residual, norm_gain.reshape(1, D))
        return pl.pallas_call(
            store_kernel,
            out_shape=(jax.ShapeDtypeStruct((BLOCK, D), jnp.bfloat16), jax.ShapeDtypeStruct((BLOCK, D), jnp.bfloat16)),
            in_specs=[vmem, vmem],
            out_specs=(hbm, hbm),
            scratch_shapes=[pltpu.SemaphoreType.DMA((2, 4))],
            compiler_params=pltpu.CompilerParams(vmem_limit_bytes=1048576),
            name="store",
        )(*(pltpu.with_memory_space_constraint(a, pltpu.VMEM) for a in (h, n)))

    row_spec = P(("data", "tp"), None)
    return jax.shard_map(local_block, mesh=mesh, in_specs=(P("data", None), P(None, "tp"), P(None, "tp"), P("tp", None), row_spec, P(None)), out_specs=(row_spec, row_spec), check_vma=False)
```

```python
import functools

import jax
import jax.numpy as jnp
from jax import lax
from jax.experimental import pallas as pl
from jax.experimental.pallas import tpu as pltpu
from jax.sharding import PartitionSpec as P

EPS = 1e-5
ROWS = 256
CHUNKS = 4
HALF = 128
LATE = 16
BLOCK = 1024
STEPS = BLOCK // ROWS
D = 2048
F = 1024
HID_COLS = F // CHUNKS
OUT_COLS = D // CHUNKS
SUM_SLOTS = 2
GROUP = 4
FIRST = 2 * STEPS
SECOND = FIRST + STEPS
THIRD = SECOND + 4 * STEPS
TILES = 8 * STEPS


def kernel(x_hbm, wg_hbm, wu_hbm, wd_hbm, res_hbm, gain_hbm, h_ref, n_ref, sum_in, sib_own, x_buf, wg, wu, wd, wd_relay, hid, tiles, hid_in, sib_in, sum_out, sum_last, sum_ld, res_ld, sib_ld, gain_ref,
           x_sem, w_sem, wr_sem, relay_sem, sib_ssem, sib_rsem, sum_ssem, sum_rsem, ld_sem, res_sem, sibld_sem, ready):
    me = lax.axis_index("tp")
    c, cx, cy = me % 2, (me // 2) % 2, me // 4
    sib = cy * 4 + cx * 2 + (1 - c)
    xn = cy * 4 + (1 - cx) * 2
    yn = (1 - cy) * 4 + cx * 2

    barrier = pltpu.get_barrier_semaphore()
    source = (1 - c) * (yn + 1) + c * xn
    for dev in (sib, source):
        pl.semaphore_signal(barrier, inc=1, device_id={"tp": dev}, device_id_type=pl.DeviceIdType.MESH)

    def kinds(i):
        past_first, past_second, past_third = (i + TILES - FIRST) // TILES, (i + TILES - SECOND) // TILES, (i + TILES - THIRD) // TILES
        return 1 - past_first, past_first - past_second, past_second - past_third, past_third

    def row_of(i):
        diag, to_sib, to_chip, kept = kinds(i)
        q = i % 4
        direction = (1 - c) + (q // 2) * (2 * c - 1)
        ty = diag * (1 - cy) + to_chip * (cy + direction * (1 - 2 * cy)) + (to_sib + kept) * cy
        tx = diag * (1 - cx) + to_chip * (cx + (1 - direction) * (1 - 2 * cx)) + (to_sib + kept) * cx
        tc = (diag + to_chip) * (i % 2) + to_sib * (1 - c) + kept * c
        k = diag * (i // 2) + to_chip * ((i - SECOND) // 4) + (to_sib + kept) * (i % STEPS)
        return pl.multiple_of((ty * 4 + tx * 2 + tc) * BLOCK + k * ROWS, ROWS)

    def x_copy(i):
        return pltpu.make_async_copy(x_hbm.at[pl.ds(row_of(i), ROWS)], x_buf.at[i % 2], x_sem.at[i % 2])

    early = [pltpu.make_async_copy(src, dst, w_sem.at[n]) for n, (src, dst) in enumerate(((wg_hbm, wg), (wu_hbm, wu), (wd_hbm, wd), (gain_hbm, gain_ref)))]
    for copy in early:
        copy.start()
    x_copy(0).start()

    out_chip = (1 - c) * xn + c * yn

    def w_relay_copy(n):
        rows = (pl.ds(0, 128), pl.ds(128, F - 128))[n]
        return pltpu.make_async_remote_copy(
            src_ref=wd_hbm.at[rows], dst_ref=wd_relay.at[rows], send_sem=wr_sem.at[0, n], recv_sem=wr_sem.at[1, n],
            device_id={"tp": out_chip + 1 - c}, device_id_type=pl.DeviceIdType.MESH)

    def relay_copy(g):
        group = pl.ds(g * GROUP, GROUP)
        return pltpu.make_async_remote_copy(
            src_ref=hid.at[group], dst_ref=hid_in.at[group], send_sem=relay_sem.at[0, g], recv_sem=relay_sem.at[1, g],
            device_id={"tp": out_chip + 1 - c}, device_id_type=pl.DeviceIdType.MESH)

    def sib_copy(slot, group, k):
        to_hbm = isinstance(group, int) and group == 2
        return pltpu.make_async_remote_copy(
            src_ref=tiles.at[slot], dst_ref=sib_own.at[k] if to_hbm else sib_in.at[group, k], send_sem=sib_ssem.at[slot],
            recv_sem=sib_rsem.at[group, k], device_id={"tp": sib}, device_id_type=pl.DeviceIdType.MESH)

    last = STEPS - 1
    parts = ((0, HALF), (HALF, HALF - LATE), (ROWS - LATE, LATE))

    def landing(d, k, part):
        if part is None:
            return sum_in.at[d, k]
        start, rows = parts[part]
        return sum_in.at[d, last, pl.ds(0, HALF)] if part == 0 else sum_last.at[d, pl.ds(start - HALF, rows)]

    def sum_copy(j, k, part=None):
        slot = k % SUM_SLOTS
        return pltpu.make_async_remote_copy(
            src_ref=sum_out.at[j, slot] if part is None else sum_out.at[j, slot, pl.ds(*parts[part])], dst_ref=landing(c, k, part),
            send_sem=sum_ssem.at[j, slot + (part or 0)], recv_sem=sum_rsem.at[c, k + (part or 0)],
            device_id={"tp": out_chip + j}, device_id_type=pl.DeviceIdType.MESH)

    def sum_arrival(d, k, part=None):
        return pltpu.make_async_remote_copy(
            src_ref=landing(d, k, part), dst_ref=landing(d, k, part), send_sem=sum_ssem.at[0, 0], recv_sem=sum_rsem.at[d, k + (part or 0)],
            device_id={"tp": sib}, device_id_type=pl.DeviceIdType.MESH)

    pl.semaphore_wait(barrier, 2)
    for n in range(2):
        w_relay_copy(n).start()
    w_relay_copy(0).wait_recv()
    pl.semaphore_signal(ready, inc=1, device_id={"tp": source}, device_id_type=pl.DeviceIdType.MESH)
    for copy in early:
        copy.wait()

    @pl.loop(0, TILES)
    def _(i):
        diag, to_sib, to_chip, kept = kinds(i)
        j = i % 2
        k_chip = (i - SECOND) // 4
        k_own = i % STEPS
        stays = to_chip * (i % 4 // 2) + kept
        is_relay = i < FIRST
        in_chip = jnp.logical_and(i >= SECOND, i < THIRD)
        is_own_sib = jnp.logical_and(i >= FIRST, i < SECOND)
        is_sib = jnp.logical_and(in_chip, i % 4 < 2)
        is_sum = jnp.logical_and(in_chip, i % 4 >= 2)
        is_final = i >= THIRD

        @pl.when(i + 1 < TILES)
        def _():
            x_copy(i + 1).start()

        x_copy(i).wait()

        @pl.when(jnp.logical_and(jnp.logical_or(is_sib, is_own_sib), i >= FIRST + 2))
        def _():
            sib_copy(j, 0, 0).wait_send()

        def res_copy():
            return pltpu.make_async_copy(res_hbm.at[pl.ds(pl.multiple_of(k_own * ROWS, ROWS), ROWS)], res_ld, res_sem)

        def sib_load():
            return pltpu.make_async_copy(sib_own.at[k_own], sib_ld, sibld_sem)

        def sum_load(d, rows):
            return pltpu.make_async_copy(sum_in.at[d, k_own, pl.ds(0, rows)], sum_ld.at[d, pl.ds(0, rows)], ld_sem.at[d])

        late_own = jnp.logical_and(k_own == last, c == 1)

        @pl.when(is_final)
        def _():
            res_copy().start()
            sib_copy(0, 2, k_own).wait_recv()
            sib_load().start()

            @pl.when(jnp.logical_not(late_own))
            def _():
                for d in range(2):
                    sum_arrival(d, k_own).wait_recv()
                    sum_load(d, ROWS).start()

            @pl.when(late_own)
            def _():
                for d in range(2):
                    sum_arrival(d, last, 0).wait_recv()
                    sum_load(d, HALF).start()

        hid_slot = diag * i + (1 - diag) * FIRST
        for n in range(CHUNKS):
            cols = slice(n * HID_COLS, (n + 1) * HID_COLS)
            gate = jnp.dot(x_buf[j], wg[:, cols], preferred_element_type=jnp.float32)
            up = jnp.dot(x_buf[j], wu[:, cols], preferred_element_type=jnp.float32)
            hid[hid_slot, :, cols] = (gate * jax.nn.sigmoid(gate) * up).astype(jnp.bfloat16)

        @pl.when(jnp.logical_and(is_relay, i % GROUP == GROUP - 1))
        def _():
            relay_copy(i // GROUP).start()

        @pl.when(i >= FIRST)
        def _():
            slot = stays * 2 + (1 - stays) * j
            for n in range(CHUNKS):
                cols = slice(n * OUT_COLS, (n + 1) * OUT_COLS)
                tiles[slot, :, cols] = jnp.dot(hid[FIRST], wd[:, cols], preferred_element_type=jnp.float32).astype(jnp.bfloat16)

        @pl.when(is_sib)
        def _():
            sib_copy(j, j, k_chip).start()

        @pl.when(is_own_sib)
        def _():
            sib_copy(j, 2, k_own).start()

        @pl.when(is_sum)
        def _():
            sib_copy(0, j, k_chip).wait_recv()

            @pl.when((2 * k_chip + j) % GROUP == 0)
            def _():
                relay_copy((2 * k_chip + j) // GROUP).wait_recv()

            @pl.when(i == SECOND + 2)
            def _():
                w_relay_copy(1).wait_recv()
                pl.semaphore_wait(ready, 1)

            @pl.when(k_chip >= SUM_SLOTS)
            def _():
                sum_copy(j, k_chip - SUM_SLOTS).wait_send()

            for n in range(CHUNKS):
                cols = slice(n * OUT_COLS, (n + 1) * OUT_COLS)
                relayed = jnp.dot(hid_in[2 * k_chip + j], wd_relay[:, cols], preferred_element_type=jnp.float32).astype(jnp.bfloat16)
                total = tiles[2, :, cols].astype(jnp.float32) + sib_in[j, k_chip, :, cols].astype(jnp.float32)
                sum_out[j, k_chip % SUM_SLOTS, :, cols] = total + relayed.astype(jnp.float32)

            late = jnp.logical_and(k_chip == last, j == 1)

            @pl.when(jnp.logical_not(late))
            def _():
                sum_copy(j, k_chip).start()

            @pl.when(late)
            def _():
                for part in range(3):
                    sum_copy(1, last, part).start()

        @pl.when(is_final)
        def _():
            res_copy().wait()
            sib_load().wait()

            def finish(start, rows, sums, sums_start):
                @pl.loop(0, rows // 16)
                def _(b):
                    here = pl.ds(pl.multiple_of(sums_start + b * 16, 16), 16)
                    tile = pl.ds(pl.multiple_of(start + b * 16, 16), 16)
                    out = pl.ds(pl.multiple_of(k_own * ROWS + start + b * 16, 16), 16)
                    y_sum = tiles[2, tile].astype(jnp.float32) + sib_ld[tile].astype(jnp.float32)
                    y_sum = y_sum + (sums[0, here] + sums[1, here])
                    h = res_ld[tile].astype(jnp.float32) + y_sum
                    mean_sq = jnp.mean(h * h, axis=-1, keepdims=True)
                    h_ref[out] = h.astype(jnp.bfloat16)
                    n_ref[out] = (h * lax.rsqrt(mean_sq + EPS) * gain_ref[...]).astype(jnp.bfloat16)

            @pl.when(jnp.logical_not(late_own))
            def _():
                for d in range(2):
                    sum_load(d, ROWS).wait()
                finish(0, ROWS, sum_ld, 0)

            @pl.when(late_own)
            def _():
                for d in range(2):
                    sum_load(d, HALF).wait()
                finish(0, HALF, sum_ld, 0)
                for part in (1, 2):
                    for d in range(2):
                        sum_arrival(d, last, part).wait_recv()
                    start, rows = parts[part]
                    finish(start, rows, sum_last, start - HALF)

    for n in range(2):
        w_relay_copy(n).wait_send()
    for g in range(FIRST // GROUP):
        relay_copy(g).wait_send()
    for s in range(2):
        sib_copy(s, 0, 0).wait_send()
    for j in range(2):
        sum_copy(j, last - 1).wait_send()
    sum_copy(0, last).wait_send()
    for part in range(3):
        sum_copy(1, last, part).wait_send()


def store_kernel(h_ref, n_ref, h_hbm, n_hbm, sem):
    copies = []
    for b in range(4):
        rows = pl.ds(b * (BLOCK // 4), BLOCK // 4)
        copies.append(pltpu.make_async_copy(h_ref.at[rows], h_hbm.at[rows], sem.at[0, b]))
        copies.append(pltpu.make_async_copy(n_ref.at[rows], n_hbm.at[rows], sem.at[1, b]))
    for copy in copies:
        copy.start()
    for copy in copies:
        copy.wait()


def solution(mesh):
    def local_block(x_in, w_gate, w_up, w_down, residual, norm_gain):
        hbm = pl.BlockSpec(memory_space=pltpu.HBM)
        vmem = pl.BlockSpec(memory_space=pltpu.VMEM)
        h, n, _, _ = pl.pallas_call(
            kernel,
            out_shape=(
                pltpu.VMEM((BLOCK, D), jnp.bfloat16),
                pltpu.VMEM((BLOCK, D), jnp.bfloat16),
                jax.ShapeDtypeStruct((2, STEPS, ROWS, D), jnp.float32),
                jax.ShapeDtypeStruct((STEPS, ROWS, D), jnp.bfloat16),
            ),
            in_specs=[hbm] * 6,
            out_specs=(vmem, vmem, hbm, hbm),
            scratch_shapes=[
                pltpu.VMEM((2, ROWS, D), jnp.bfloat16),
                pltpu.VMEM((D, F), jnp.bfloat16),
                pltpu.VMEM((D, F), jnp.bfloat16),
                pltpu.VMEM((F, D), jnp.bfloat16),
                pltpu.VMEM((F, D), jnp.bfloat16),
                pltpu.VMEM((FIRST + 1, ROWS, F), jnp.bfloat16),
                pltpu.VMEM((3, ROWS, D), jnp.bfloat16),
                pltpu.VMEM((FIRST, ROWS, F), jnp.bfloat16),
                pltpu.VMEM((2, STEPS, ROWS, D), jnp.bfloat16),
                pltpu.VMEM((2, SUM_SLOTS, ROWS, D), jnp.float32),
                pltpu.VMEM((2, HALF, D), jnp.float32),
                pltpu.VMEM((2, ROWS, D), jnp.float32),
                pltpu.VMEM((ROWS, D), jnp.bfloat16),
                pltpu.VMEM((ROWS, D), jnp.bfloat16),
                pltpu.VMEM((1, D), jnp.float32),
                pltpu.SemaphoreType.DMA((2,)),
                pltpu.SemaphoreType.DMA((4,)),
                pltpu.SemaphoreType.DMA((2, 2)),
                pltpu.SemaphoreType.DMA((2, FIRST // GROUP)),
                pltpu.SemaphoreType.DMA((2,)),
                pltpu.SemaphoreType.DMA((3, STEPS)),
                pltpu.SemaphoreType.DMA((2, SUM_SLOTS + 2)),
                pltpu.SemaphoreType.DMA((2, STEPS + 2)),
                pltpu.SemaphoreType.DMA((2,)),
                pltpu.SemaphoreType.DMA,
                pltpu.SemaphoreType.DMA,
                pltpu.SemaphoreType.REGULAR,
            ],
            compiler_params=pltpu.CompilerParams(collective_id=0, has_side_effects=True, vmem_limit_bytes=58000000),
            name="mlp_reduce",
        )(x_in, w_gate, w_up, w_down, residual, norm_gain.reshape(1, D))
        return pl.pallas_call(
            store_kernel,
            out_shape=(jax.ShapeDtypeStruct((BLOCK, D), jnp.bfloat16), jax.ShapeDtypeStruct((BLOCK, D), jnp.bfloat16)),
            in_specs=[vmem, vmem],
            out_specs=(hbm, hbm),
            scratch_shapes=[pltpu.SemaphoreType.DMA((2, 4))],
            compiler_params=pltpu.CompilerParams(vmem_limit_bytes=1048576),
            name="store",
        )(*(pltpu.with_memory_space_constraint(a, pltpu.VMEM) for a in (h, n)))

    row_spec = P(("data", "tp"), None)
    return jax.shard_map(local_block, mesh=mesh, in_specs=(P("data", None), P(None, "tp"), P(None, "tp"), P("tp", None), row_spec, P(None)), out_specs=(row_spec, row_spec), check_vma=False)
```

```python
import functools

import jax
import jax.numpy as jnp
from jax import lax
from jax.experimental import pallas as pl
from jax.experimental.pallas import tpu as pltpu
from jax.sharding import PartitionSpec as P

EPS = 1e-5
ROWS = 256
CHUNKS = 4
HALF = 128
LATE = 16
BLOCK = 1024
STEPS = BLOCK // ROWS
D = 2048
F = 1024
HID_COLS = F // CHUNKS
OUT_COLS = D // CHUNKS
SUM_SLOTS = 2
GROUP = 4
FIRST = 2 * STEPS
SECOND = FIRST + STEPS
THIRD = SECOND + 4 * STEPS
TILES = 8 * STEPS


def kernel(x_hbm, wg_hbm, wu_hbm, wd_hbm, res_hbm, gain_hbm, h_ref, n_ref, sum_in, sib_own, x_buf, wg, wu, wd, wd_relay, hid, tiles, hid_in, sib_in, sum_out, sum_last, sum_ld, res_ld, sib_ld, gain_ref,
           x_sem, w_sem, wr_sem, relay_sem, sib_ssem, sib_rsem, sum_ssem, sum_rsem, ready):
    me = lax.axis_index("tp")
    c, cx, cy = me % 2, (me // 2) % 2, me // 4
    sib = cy * 4 + cx * 2 + (1 - c)
    xn = cy * 4 + (1 - cx) * 2
    yn = (1 - cy) * 4 + cx * 2

    barrier = pltpu.get_barrier_semaphore()
    source = (1 - c) * (xn + 1) + c * yn
    for dev in (sib, source):
        pl.semaphore_signal(barrier, inc=1, device_id={"tp": dev}, device_id_type=pl.DeviceIdType.MESH)

    def kinds(i):
        past_first, past_second, past_third = (i + TILES - FIRST) // TILES, (i + TILES - SECOND) // TILES, (i + TILES - THIRD) // TILES
        return 1 - past_first, past_first - past_second, past_second - past_third, past_third

    def row_of(i):
        diag, to_sib, to_chip, kept = kinds(i)
        q = i % 4
        direction = c + (q // 2) * (1 - 2 * c)
        ty = diag * (1 - cy) + to_chip * (cy + direction * (1 - 2 * cy)) + (to_sib + kept) * cy
        tx = diag * (1 - cx) + to_chip * (cx + (1 - direction) * (1 - 2 * cx)) + (to_sib + kept) * cx
        tc = (diag + to_chip) * (i % 2) + to_sib * (1 - c) + kept * c
        k = diag * (i // 2) + to_chip * ((i - SECOND) // 4) + (to_sib + kept) * (i % STEPS)
        return pl.multiple_of((ty * 4 + tx * 2 + tc) * BLOCK + k * ROWS, ROWS)

    def x_copy(i):
        return pltpu.make_async_copy(x_hbm.at[pl.ds(row_of(i), ROWS)], x_buf.at[i % 2], x_sem.at[i % 2])

    early = [pltpu.make_async_copy(src, dst, w_sem.at[n]) for n, (src, dst) in enumerate(((wg_hbm, wg), (wu_hbm, wu), (wd_hbm, wd), (gain_hbm, gain_ref)))]
    for copy in early:
        copy.start()
    x_copy(0).start()

    out_chip = (1 - c) * yn + c * xn

    def w_relay_copy(n):
        rows = (pl.ds(0, 128), pl.ds(128, F - 128))[n]
        return pltpu.make_async_remote_copy(
            src_ref=wd_hbm.at[rows], dst_ref=wd_relay.at[rows], send_sem=wr_sem.at[0, n], recv_sem=wr_sem.at[1, n],
            device_id={"tp": out_chip + 1 - c}, device_id_type=pl.DeviceIdType.MESH)

    def relay_copy(g):
        group = pl.ds(g * GROUP, GROUP)
        return pltpu.make_async_remote_copy(
            src_ref=hid.at[group], dst_ref=hid_in.at[group], send_sem=relay_sem.at[0, g], recv_sem=relay_sem.at[1, g],
            device_id={"tp": out_chip + 1 - c}, device_id_type=pl.DeviceIdType.MESH)

    def sib_copy(slot, group, k):
        to_hbm = isinstance(group, int) and group == 2
        return pltpu.make_async_remote_copy(
            src_ref=tiles.at[slot], dst_ref=sib_own.at[k] if to_hbm else sib_in.at[group, k], send_sem=sib_ssem.at[slot],
            recv_sem=sib_rsem.at[group, k], device_id={"tp": sib}, device_id_type=pl.DeviceIdType.MESH)

    last = STEPS - 1
    parts = ((0, HALF), (HALF, HALF - LATE), (ROWS - LATE, LATE))

    def landing(d, k, part):
        if part is None:
            return sum_in.at[d, k]
        start, rows = parts[part]
        return sum_in.at[d, last, pl.ds(0, HALF)] if part == 0 else sum_last.at[d, pl.ds(start - HALF, rows)]

    def sum_copy(j, k, part=None):
        slot = k % SUM_SLOTS
        return pltpu.make_async_remote_copy(
            src_ref=sum_out.at[j, slot] if part is None else sum_out.at[j, slot, pl.ds(*parts[part])], dst_ref=landing(c, k, part),
            send_sem=sum_ssem.at[j, slot + (part or 0)], recv_sem=sum_rsem.at[c, k + (part or 0)],
            device_id={"tp": out_chip + j}, device_id_type=pl.DeviceIdType.MESH)

    def sum_arrival(d, k, part=None):
        return pltpu.make_async_remote_copy(
            src_ref=landing(d, k, part), dst_ref=landing(d, k, part), send_sem=sum_ssem.at[0, 0], recv_sem=sum_rsem.at[d, k + (part or 0)],
            device_id={"tp": sib}, device_id_type=pl.DeviceIdType.MESH)

    pl.semaphore_wait(barrier, 2)
    for n in range(2):
        w_relay_copy(n).start()
    w_relay_copy(0).wait_recv()
    pl.semaphore_signal(ready, inc=1, device_id={"tp": source}, device_id_type=pl.DeviceIdType.MESH)
    for copy in early:
        copy.wait()

    @pl.loop(0, TILES)
    def _(i):
        diag, to_sib, to_chip, kept = kinds(i)
        j = i % 2
        k_chip = (i - SECOND) // 4
        k_own = i % STEPS
        stays = to_chip * (i % 4 // 2) + kept
        is_relay = i < FIRST
        in_chip = jnp.logical_and(i >= SECOND, i < THIRD)
        is_own_sib = jnp.logical_and(i >= FIRST, i < SECOND)
        is_sib = jnp.logical_and(in_chip, i % 4 < 2)
        is_sum = jnp.logical_and(in_chip, i % 4 >= 2)
        is_final = i >= THIRD

        @pl.when(i + 1 < TILES)
        def _():
            x_copy(i + 1).start()

        x_copy(i).wait()

        @pl.when(jnp.logical_and(jnp.logical_or(is_sib, is_own_sib), i >= FIRST + 2))
        def _():
            sib_copy(j, 0, 0).wait_send()

        def res_copy():
            return pltpu.make_async_copy(res_hbm.at[pl.ds(pl.multiple_of(k_own * ROWS, ROWS), ROWS)], res_ld, w_sem.at[2])

        def sib_load():
            return pltpu.make_async_copy(sib_own.at[k_own], sib_ld, w_sem.at[3])

        def sum_load(d, rows):
            return pltpu.make_async_copy(sum_in.at[d, k_own, pl.ds(0, rows)], sum_ld.at[d, pl.ds(0, rows)], w_sem.at[d])

        late_own = jnp.logical_and(k_own == last, c == 1)

        @pl.when(is_final)
        def _():
            res_copy().start()
            sib_copy(0, 2, k_own).wait_recv()
            sib_load().start()

            @pl.when(jnp.logical_not(late_own))
            def _():
                for d in range(2):
                    sum_arrival(d, k_own).wait_recv()
                    sum_load(d, ROWS).start()

            @pl.when(late_own)
            def _():
                for d in range(2):
                    sum_arrival(d, last, 0).wait_recv()
                    sum_load(d, HALF).start()

        hid_slot = diag * i + (1 - diag) * FIRST
        for n in range(CHUNKS):
            cols = slice(n * HID_COLS, (n + 1) * HID_COLS)
            gate = jnp.dot(x_buf[j], wg[:, cols], preferred_element_type=jnp.float32)
            up = jnp.dot(x_buf[j], wu[:, cols], preferred_element_type=jnp.float32)
            hid[hid_slot, :, cols] = (gate * jax.nn.sigmoid(gate) * up).astype(jnp.bfloat16)

        @pl.when(jnp.logical_and(is_relay, i % GROUP == GROUP - 1))
        def _():
            relay_copy(i // GROUP).start()

        @pl.when(i >= FIRST)
        def _():
            slot = stays * 2 + (1 - stays) * j
            for n in range(CHUNKS):
                cols = slice(n * OUT_COLS, (n + 1) * OUT_COLS)
                tiles[slot, :, cols] = jnp.dot(hid[FIRST], wd[:, cols], preferred_element_type=jnp.float32).astype(jnp.bfloat16)

        @pl.when(is_sib)
        def _():
            sib_copy(j, j, k_chip).start()

        @pl.when(is_own_sib)
        def _():
            sib_copy(j, 2, k_own).start()

        @pl.when(is_sum)
        def _():
            sib_copy(0, j, k_chip).wait_recv()

            @pl.when((2 * k_chip + j) % GROUP == 0)
            def _():
                relay_copy((2 * k_chip + j) // GROUP).wait_recv()

            @pl.when(i == SECOND + 2)
            def _():
                w_relay_copy(1).wait_recv()
                pl.semaphore_wait(ready, 1)

            @pl.when(k_chip >= SUM_SLOTS)
            def _():
                sum_copy(j, k_chip - SUM_SLOTS).wait_send()

            for n in range(CHUNKS):
                cols = slice(n * OUT_COLS, (n + 1) * OUT_COLS)
                relayed = jnp.dot(hid_in[2 * k_chip + j], wd_relay[:, cols], preferred_element_type=jnp.float32).astype(jnp.bfloat16)
                total = tiles[2, :, cols].astype(jnp.float32) + sib_in[j, k_chip, :, cols].astype(jnp.float32)
                sum_out[j, k_chip % SUM_SLOTS, :, cols] = total + relayed.astype(jnp.float32)

            late = jnp.logical_and(k_chip == last, j == 1)

            @pl.when(jnp.logical_not(late))
            def _():
                sum_copy(j, k_chip).start()

            @pl.when(late)
            def _():
                for part in range(3):
                    sum_copy(1, last, part).start()

        @pl.when(is_final)
        def _():
            res_copy().wait()
            sib_load().wait()

            def finish(start, rows, sums, sums_start):
                @pl.loop(0, rows // 16)
                def _(b):
                    here = pl.ds(pl.multiple_of(sums_start + b * 16, 16), 16)
                    tile = pl.ds(pl.multiple_of(start + b * 16, 16), 16)
                    out = pl.ds(pl.multiple_of(k_own * ROWS + start + b * 16, 16), 16)
                    y_sum = tiles[2, tile].astype(jnp.float32) + sib_ld[tile].astype(jnp.float32)
                    y_sum = y_sum + (sums[0, here] + sums[1, here])
                    h = res_ld[tile].astype(jnp.float32) + y_sum
                    mean_sq = jnp.mean(h * h, axis=-1, keepdims=True)
                    h_ref[out] = h.astype(jnp.bfloat16)
                    n_ref[out] = (h * lax.rsqrt(mean_sq + EPS) * gain_ref[...]).astype(jnp.bfloat16)

            @pl.when(jnp.logical_not(late_own))
            def _():
                for d in range(2):
                    sum_load(d, ROWS).wait()
                finish(0, ROWS, sum_ld, 0)

            @pl.when(late_own)
            def _():
                for d in range(2):
                    sum_load(d, HALF).wait()
                finish(0, HALF, sum_ld, 0)
                for part in (1, 2):
                    for d in range(2):
                        sum_arrival(d, last, part).wait_recv()
                    start, rows = parts[part]
                    finish(start, rows, sum_last, start - HALF)

    for n in range(2):
        w_relay_copy(n).wait_send()
    for g in range(FIRST // GROUP):
        relay_copy(g).wait_send()
    for s in range(2):
        sib_copy(s, 0, 0).wait_send()
    for j in range(2):
        sum_copy(j, last - 1).wait_send()
    sum_copy(0, last).wait_send()
    for part in range(3):
        sum_copy(1, last, part).wait_send()


def store_kernel(h_ref, n_ref, h_hbm, n_hbm, sem):
    copies = [pltpu.make_async_copy(h_ref, h_hbm, sem.at[0]), pltpu.make_async_copy(n_ref, n_hbm, sem.at[1])]
    for copy in copies:
        copy.start()
    for copy in copies:
        copy.wait()


def solution(mesh):
    def local_block(x_in, w_gate, w_up, w_down, residual, norm_gain):
        hbm = pl.BlockSpec(memory_space=pltpu.HBM)
        vmem = pl.BlockSpec(memory_space=pltpu.VMEM)
        h, n, _, _ = pl.pallas_call(
            kernel,
            out_shape=(
                pltpu.VMEM((BLOCK, D), jnp.bfloat16),
                pltpu.VMEM((BLOCK, D), jnp.bfloat16),
                jax.ShapeDtypeStruct((2, STEPS, ROWS, D), jnp.float32),
                jax.ShapeDtypeStruct((STEPS, ROWS, D), jnp.bfloat16),
            ),
            in_specs=[hbm] * 6,
            out_specs=(vmem, vmem, hbm, hbm),
            scratch_shapes=[
                pltpu.VMEM((2, ROWS, D), jnp.bfloat16),
                pltpu.VMEM((D, F), jnp.bfloat16),
                pltpu.VMEM((D, F), jnp.bfloat16),
                pltpu.VMEM((F, D), jnp.bfloat16),
                pltpu.VMEM((F, D), jnp.bfloat16),
                pltpu.VMEM((FIRST + 1, ROWS, F), jnp.bfloat16),
                pltpu.VMEM((3, ROWS, D), jnp.bfloat16),
                pltpu.VMEM((FIRST, ROWS, F), jnp.bfloat16),
                pltpu.VMEM((2, STEPS, ROWS, D), jnp.bfloat16),
                pltpu.VMEM((2, SUM_SLOTS, ROWS, D), jnp.float32),
                pltpu.VMEM((2, HALF, D), jnp.float32),
                pltpu.VMEM((2, ROWS, D), jnp.float32),
                pltpu.VMEM((ROWS, D), jnp.bfloat16),
                pltpu.VMEM((ROWS, D), jnp.bfloat16),
                pltpu.VMEM((1, D), jnp.float32),
                pltpu.SemaphoreType.DMA((2,)),
                pltpu.SemaphoreType.DMA((4,)),
                pltpu.SemaphoreType.DMA((2, 2)),
                pltpu.SemaphoreType.DMA((2, FIRST // GROUP)),
                pltpu.SemaphoreType.DMA((2,)),
                pltpu.SemaphoreType.DMA((3, STEPS)),
                pltpu.SemaphoreType.DMA((2, SUM_SLOTS + 2)),
                pltpu.SemaphoreType.DMA((2, STEPS + 2)),
                pltpu.SemaphoreType.REGULAR,
            ],
            compiler_params=pltpu.CompilerParams(collective_id=0, has_side_effects=True, vmem_limit_bytes=58000000),
            name="mlp_reduce",
        )(x_in, w_gate, w_up, w_down, residual, norm_gain.reshape(1, D))
        return pl.pallas_call(
            store_kernel,
            out_shape=(jax.ShapeDtypeStruct((BLOCK, D), jnp.bfloat16), jax.ShapeDtypeStruct((BLOCK, D), jnp.bfloat16)),
            in_specs=[vmem, vmem],
            out_specs=(hbm, hbm),
            scratch_shapes=[pltpu.SemaphoreType.DMA((2,))],
            compiler_params=pltpu.CompilerParams(vmem_limit_bytes=1048576),
            name="store",
        )(*(pltpu.with_memory_space_constraint(a, pltpu.VMEM) for a in (h, n)))

    row_spec = P(("data", "tp"), None)
    return jax.shard_map(local_block, mesh=mesh, in_specs=(P("data", None), P(None, "tp"), P(None, "tp"), P("tp", None), row_spec, P(None)), out_specs=(row_spec, row_spec), check_vma=False)
```

```python
import functools

import jax
import jax.numpy as jnp
from jax import lax
from jax.experimental import pallas as pl
from jax.experimental.pallas import tpu as pltpu
from jax.sharding import PartitionSpec as P

EPS = 1e-5
ROWS = 256
CHUNKS = 4
HALF = 128
LATE = 16
BLOCK = 1024
STEPS = BLOCK // ROWS
D = 2048
F = 1024
HID_COLS = F // CHUNKS
OUT_COLS = D // CHUNKS
SUM_SLOTS = 2
GROUP = 4
FIRST = 2 * STEPS
SECOND = FIRST + STEPS
THIRD = SECOND + 4 * STEPS
TILES = 8 * STEPS


def kernel(x_hbm, wg_hbm, wu_hbm, wd_hbm, res_hbm, gain_hbm, h_ref, n_ref, sum_in, sib_own, x_buf, wg, wu, wd, wd_relay, hid, tiles, hid_in, sib_in, sum_out, sum_last, sum_ld, res_ld, sib_ld, gain_ref,
           x_sem, w_sem, wr_sem, relay_sem, sib_ssem, sib_rsem, sum_ssem, sum_rsem, ready):
    me = lax.axis_index("tp")
    c, cx, cy = me % 2, (me // 2) % 2, me // 4
    sib = cy * 4 + cx * 2 + (1 - c)
    xn = cy * 4 + (1 - cx) * 2
    yn = (1 - cy) * 4 + cx * 2

    barrier = pltpu.get_barrier_semaphore()
    source = (1 - c) * (xn + 1) + c * yn
    for dev in (sib, source):
        pl.semaphore_signal(barrier, inc=1, device_id={"tp": dev}, device_id_type=pl.DeviceIdType.MESH)

    def kinds(i):
        past_first, past_second, past_third = (i + TILES - FIRST) // TILES, (i + TILES - SECOND) // TILES, (i + TILES - THIRD) // TILES
        return 1 - past_first, past_first - past_second, past_second - past_third, past_third

    def row_of(i):
        diag, to_sib, to_chip, kept = kinds(i)
        q = i % 4
        direction = c + (q // 2) * (1 - 2 * c)
        ty = diag * (1 - cy) + to_chip * (cy + direction * (1 - 2 * cy)) + (to_sib + kept) * cy
        tx = diag * (1 - cx) + to_chip * (cx + (1 - direction) * (1 - 2 * cx)) + (to_sib + kept) * cx
        tc = (diag + to_chip) * (i % 2) + to_sib * (1 - c) + kept * c
        k = diag * (i // 2) + to_chip * ((i - SECOND) // 4) + (to_sib + kept) * (i % STEPS)
        return pl.multiple_of((ty * 4 + tx * 2 + tc) * BLOCK + k * ROWS, ROWS)

    def x_copy(i):
        return pltpu.make_async_copy(x_hbm.at[pl.ds(row_of(i), ROWS)], x_buf.at[i % 2], x_sem.at[i % 2])

    early = [pltpu.make_async_copy(src, dst, w_sem.at[n]) for n, (src, dst) in enumerate(((wg_hbm, wg), (wu_hbm, wu), (wd_hbm, wd), (gain_hbm, gain_ref)))]
    for copy in early:
        copy.start()
    x_copy(0).start()

    out_chip = (1 - c) * yn + c * xn

    def w_relay_copy(n):
        rows = (pl.ds(0, 128), pl.ds(128, F - 128))[n]
        return pltpu.make_async_remote_copy(
            src_ref=wd_hbm.at[rows], dst_ref=wd_relay.at[rows], send_sem=wr_sem.at[0, n], recv_sem=wr_sem.at[1, n],
            device_id={"tp": out_chip + 1 - c}, device_id_type=pl.DeviceIdType.MESH)

    def relay_copy(g):
        group = pl.ds(g * GROUP, GROUP)
        return pltpu.make_async_remote_copy(
            src_ref=hid.at[group], dst_ref=hid_in.at[group], send_sem=relay_sem.at[0, g], recv_sem=relay_sem.at[1, g],
            device_id={"tp": out_chip + 1 - c}, device_id_type=pl.DeviceIdType.MESH)

    def sib_copy(slot, group, k):
        to_hbm = isinstance(group, int) and group == 2
        return pltpu.make_async_remote_copy(
            src_ref=tiles.at[slot], dst_ref=sib_own.at[k] if to_hbm else sib_in.at[group, k], send_sem=sib_ssem.at[slot],
            recv_sem=sib_rsem.at[group, k], device_id={"tp": sib}, device_id_type=pl.DeviceIdType.MESH)

    last = STEPS - 1
    parts = ((0, HALF), (HALF, HALF - LATE), (ROWS - LATE, LATE))

    def landing(d, k, part):
        if part is None:
            return sum_in.at[d, k]
        start, rows = parts[part]
        return sum_in.at[d, last, pl.ds(0, HALF)] if part == 0 else sum_last.at[d, pl.ds(start - HALF, rows)]

    def sum_copy(j, k, part=None):
        slot = k % SUM_SLOTS
        return pltpu.make_async_remote_copy(
            src_ref=sum_out.at[j, slot] if part is None else sum_out.at[j, slot, pl.ds(*parts[part])], dst_ref=landing(c, k, part),
            send_sem=sum_ssem.at[j, slot + (part or 0)], recv_sem=sum_rsem.at[c, k + (part or 0)],
            device_id={"tp": out_chip + j}, device_id_type=pl.DeviceIdType.MESH)

    def sum_arrival(d, k, part=None):
        return pltpu.make_async_remote_copy(
            src_ref=landing(d, k, part), dst_ref=landing(d, k, part), send_sem=sum_ssem.at[0, 0], recv_sem=sum_rsem.at[d, k + (part or 0)],
            device_id={"tp": sib}, device_id_type=pl.DeviceIdType.MESH)

    pl.semaphore_wait(barrier, 2)
    for n in range(2):
        w_relay_copy(n).start()
    w_relay_copy(0).wait_recv()
    pl.semaphore_signal(ready, inc=1, device_id={"tp": source}, device_id_type=pl.DeviceIdType.MESH)
    for copy in early:
        copy.wait()

    @pl.loop(0, TILES)
    def _(i):
        diag, to_sib, to_chip, kept = kinds(i)
        j = i % 2
        k_chip = (i - SECOND) // 4
        k_own = i % STEPS
        stays = to_chip * (i % 4 // 2) + kept
        is_relay = i < FIRST
        in_chip = jnp.logical_and(i >= SECOND, i < THIRD)
        is_own_sib = jnp.logical_and(i >= FIRST, i < SECOND)
        is_sib = jnp.logical_and(in_chip, i % 4 < 2)
        is_sum = jnp.logical_and(in_chip, i % 4 >= 2)
        is_final = i >= THIRD

        @pl.when(i + 1 < TILES)
        def _():
            x_copy(i + 1).start()

        x_copy(i).wait()

        @pl.when(jnp.logical_and(jnp.logical_or(is_sib, is_own_sib), i >= FIRST + 2))
        def _():
            sib_copy(j, 0, 0).wait_send()

        def res_copy():
            return pltpu.make_async_copy(res_hbm.at[pl.ds(pl.multiple_of(k_own * ROWS, ROWS), ROWS)], res_ld, w_sem.at[2])

        def sib_load():
            return pltpu.make_async_copy(sib_own.at[k_own], sib_ld, w_sem.at[3])

        def sum_load(d, rows):
            return pltpu.make_async_copy(sum_in.at[d, k_own, pl.ds(0, rows)], sum_ld.at[d, pl.ds(0, rows)], w_sem.at[d])

        late_own = jnp.logical_and(k_own == last, c == 1)

        @pl.when(is_final)
        def _():
            res_copy().start()
            sib_copy(0, 2, k_own).wait_recv()
            sib_load().start()

            @pl.when(jnp.logical_not(late_own))
            def _():
                for d in range(2):
                    sum_arrival(d, k_own).wait_recv()
                    sum_load(d, ROWS).start()

            @pl.when(late_own)
            def _():
                for d in range(2):
                    sum_arrival(d, last, 0).wait_recv()
                    sum_load(d, HALF).start()

        hid_slot = diag * i + (1 - diag) * FIRST
        for n in range(CHUNKS):
            cols = slice(n * HID_COLS, (n + 1) * HID_COLS)
            gate = jnp.dot(x_buf[j], wg[:, cols], preferred_element_type=jnp.float32)
            up = jnp.dot(x_buf[j], wu[:, cols], preferred_element_type=jnp.float32)
            hid[hid_slot, :, cols] = (gate * jax.nn.sigmoid(gate) * up).astype(jnp.bfloat16)

        @pl.when(jnp.logical_and(is_relay, i % GROUP == GROUP - 1))
        def _():
            relay_copy(i // GROUP).start()

        @pl.when(i >= FIRST)
        def _():
            slot = stays * 2 + (1 - stays) * j
            for n in range(CHUNKS):
                cols = slice(n * OUT_COLS, (n + 1) * OUT_COLS)
                tiles[slot, :, cols] = jnp.dot(hid[FIRST], wd[:, cols], preferred_element_type=jnp.float32).astype(jnp.bfloat16)

        @pl.when(is_sib)
        def _():
            sib_copy(j, j, k_chip).start()

        @pl.when(is_own_sib)
        def _():
            sib_copy(j, 2, k_own).start()

        @pl.when(is_sum)
        def _():
            sib_copy(0, j, k_chip).wait_recv()

            @pl.when((2 * k_chip + j) % GROUP == 0)
            def _():
                relay_copy((2 * k_chip + j) // GROUP).wait_recv()

            @pl.when(i == SECOND + 2)
            def _():
                w_relay_copy(1).wait_recv()
                pl.semaphore_wait(ready, 1)

            @pl.when(k_chip >= SUM_SLOTS)
            def _():
                sum_copy(j, k_chip - SUM_SLOTS).wait_send()

            for n in range(CHUNKS):
                cols = slice(n * OUT_COLS, (n + 1) * OUT_COLS)
                relayed = jnp.dot(hid_in[2 * k_chip + j], wd_relay[:, cols], preferred_element_type=jnp.float32).astype(jnp.bfloat16)
                total = tiles[2, :, cols].astype(jnp.float32) + sib_in[j, k_chip, :, cols].astype(jnp.float32)
                sum_out[j, k_chip % SUM_SLOTS, :, cols] = total + relayed.astype(jnp.float32)

            late = jnp.logical_and(k_chip == last, j == 1)

            @pl.when(jnp.logical_not(late))
            def _():
                sum_copy(j, k_chip).start()

            @pl.when(late)
            def _():
                for part in range(3):
                    sum_copy(1, last, part).start()

        @pl.when(is_final)
        def _():
            res_copy().wait()
            sib_load().wait()

            def finish(start, rows, sums, sums_start):
                @pl.loop(0, rows // 16)
                def _(b):
                    here = pl.ds(pl.multiple_of(sums_start + b * 16, 16), 16)
                    tile = pl.ds(pl.multiple_of(start + b * 16, 16), 16)
                    out = pl.ds(pl.multiple_of(k_own * ROWS + start + b * 16, 16), 16)
                    y_sum = tiles[2, tile].astype(jnp.float32) + sib_ld[tile].astype(jnp.float32)
                    y_sum = y_sum + (sums[0, here] + sums[1, here])
                    h = res_ld[tile].astype(jnp.float32) + y_sum
                    mean_sq = jnp.mean(h * h, axis=-1, keepdims=True)
                    h_ref[out] = h.astype(jnp.bfloat16)
                    n_ref[out] = (h * lax.rsqrt(mean_sq + EPS) * gain_ref[...]).astype(jnp.bfloat16)

            @pl.when(jnp.logical_not(late_own))
            def _():
                for d in range(2):
                    sum_load(d, ROWS).wait()
                finish(0, ROWS, sum_ld, 0)

            @pl.when(late_own)
            def _():
                for d in range(2):
                    sum_load(d, HALF).wait()
                finish(0, HALF, sum_ld, 0)
                for part in (1, 2):
                    for d in range(2):
                        sum_arrival(d, last, part).wait_recv()
                    start, rows = parts[part]
                    finish(start, rows, sum_last, start - HALF)

    for n in range(2):
        w_relay_copy(n).wait_send()
    for g in range(FIRST // GROUP):
        relay_copy(g).wait_send()
    for s in range(2):
        sib_copy(s, 0, 0).wait_send()
    for j in range(2):
        sum_copy(j, last - 1).wait_send()
    sum_copy(0, last).wait_send()
    for part in range(3):
        sum_copy(1, last, part).wait_send()


def store_kernel(h_ref, n_ref, h_hbm, n_hbm, sem):
    for b in range(8):
        rows = pl.ds(b * (BLOCK // 8), BLOCK // 8)
        pltpu.make_async_copy(h_ref.at[rows], h_hbm.at[rows], sem.at[0]).start()
        pltpu.make_async_copy(n_ref.at[rows], n_hbm.at[rows], sem.at[1]).start()
    pltpu.make_async_copy(h_ref, h_hbm, sem.at[0]).wait()
    pltpu.make_async_copy(n_ref, n_hbm, sem.at[1]).wait()


def solution(mesh):
    def local_block(x_in, w_gate, w_up, w_down, residual, norm_gain):
        hbm = pl.BlockSpec(memory_space=pltpu.HBM)
        vmem = pl.BlockSpec(memory_space=pltpu.VMEM)
        h, n, _, _ = pl.pallas_call(
            kernel,
            out_shape=(
                pltpu.VMEM((BLOCK, D), jnp.bfloat16),
                pltpu.VMEM((BLOCK, D), jnp.bfloat16),
                jax.ShapeDtypeStruct((2, STEPS, ROWS, D), jnp.float32),
                jax.ShapeDtypeStruct((STEPS, ROWS, D), jnp.bfloat16),
            ),
            in_specs=[hbm] * 6,
            out_specs=(vmem, vmem, hbm, hbm),
            scratch_shapes=[
                pltpu.VMEM((2, ROWS, D), jnp.bfloat16),
                pltpu.VMEM((D, F), jnp.bfloat16),
                pltpu.VMEM((D, F), jnp.bfloat16),
                pltpu.VMEM((F, D), jnp.bfloat16),
                pltpu.VMEM((F, D), jnp.bfloat16),
                pltpu.VMEM((FIRST + 1, ROWS, F), jnp.bfloat16),
                pltpu.VMEM((3, ROWS, D), jnp.bfloat16),
                pltpu.VMEM((FIRST, ROWS, F), jnp.bfloat16),
                pltpu.VMEM((2, STEPS, ROWS, D), jnp.bfloat16),
                pltpu.VMEM((2, SUM_SLOTS, ROWS, D), jnp.float32),
                pltpu.VMEM((2, HALF, D), jnp.float32),
                pltpu.VMEM((2, ROWS, D), jnp.float32),
                pltpu.VMEM((ROWS, D), jnp.bfloat16),
                pltpu.VMEM((ROWS, D), jnp.bfloat16),
                pltpu.VMEM((1, D), jnp.float32),
                pltpu.SemaphoreType.DMA((2,)),
                pltpu.SemaphoreType.DMA((4,)),
                pltpu.SemaphoreType.DMA((2, 2)),
                pltpu.SemaphoreType.DMA((2, FIRST // GROUP)),
                pltpu.SemaphoreType.DMA((2,)),
                pltpu.SemaphoreType.DMA((3, STEPS)),
                pltpu.SemaphoreType.DMA((2, SUM_SLOTS + 2)),
                pltpu.SemaphoreType.DMA((2, STEPS + 2)),
                pltpu.SemaphoreType.REGULAR,
            ],
            compiler_params=pltpu.CompilerParams(collective_id=0, has_side_effects=True, vmem_limit_bytes=58000000),
            name="mlp_reduce",
        )(x_in, w_gate, w_up, w_down, residual, norm_gain.reshape(1, D))
        return pl.pallas_call(
            store_kernel,
            out_shape=(jax.ShapeDtypeStruct((BLOCK, D), jnp.bfloat16), jax.ShapeDtypeStruct((BLOCK, D), jnp.bfloat16)),
            in_specs=[vmem, vmem],
            out_specs=(hbm, hbm),
            scratch_shapes=[pltpu.SemaphoreType.DMA((2,))],
            compiler_params=pltpu.CompilerParams(vmem_limit_bytes=1048576),
            name="store",
        )(*(pltpu.with_memory_space_constraint(a, pltpu.VMEM) for a in (h, n)))

    row_spec = P(("data", "tp"), None)
    return jax.shard_map(local_block, mesh=mesh, in_specs=(P("data", None), P(None, "tp"), P(None, "tp"), P("tp", None), row_spec, P(None)), out_specs=(row_spec, row_spec), check_vma=False)
```

```python
import functools

import jax
import jax.numpy as jnp
from jax import lax
from jax.experimental import pallas as pl
from jax.experimental.pallas import tpu as pltpu
from jax.sharding import PartitionSpec as P

EPS = 1e-5
ROWS = 256
CHUNKS = 4
HALF = 128
LATE = 16
BLOCK = 1024
STEPS = BLOCK // ROWS
D = 2048
F = 1024
HID_COLS = F // CHUNKS
OUT_COLS = D // CHUNKS
SUM_SLOTS = 2
GROUP = 4
FIRST = 2 * STEPS
SECOND = FIRST + STEPS
THIRD = SECOND + 4 * STEPS
TILES = 8 * STEPS


def kernel(x_hbm, wg_hbm, wu_hbm, wd_hbm, res_hbm, gain_hbm, h_ref, n_ref, sum_in, sib_own, x_buf, wg, wu, wd, wd_relay, hid, tiles, hid_in, sib_in, sum_out, sum_last, sum_ld, res_ld, sib_ld, gain_ref,
           x_sem, w_sem, wr_sem, relay_sem, sib_ssem, sib_rsem, sum_ssem, sum_rsem, ready):
    me = lax.axis_index("tp")
    c, cx, cy = me % 2, (me // 2) % 2, me // 4
    sib = cy * 4 + cx * 2 + (1 - c)
    xn = cy * 4 + (1 - cx) * 2
    yn = (1 - cy) * 4 + cx * 2

    barrier = pltpu.get_barrier_semaphore()
    source = (1 - c) * (xn + 1) + c * yn
    for dev in (sib, source):
        pl.semaphore_signal(barrier, inc=1, device_id={"tp": dev}, device_id_type=pl.DeviceIdType.MESH)

    def kinds(i):
        past_first, past_second, past_third = (i + TILES - FIRST) // TILES, (i + TILES - SECOND) // TILES, (i + TILES - THIRD) // TILES
        return 1 - past_first, past_first - past_second, past_second - past_third, past_third

    def row_of(i):
        diag, to_sib, to_chip, kept = kinds(i)
        q = i % 4
        direction = c + (q // 2) * (1 - 2 * c)
        ty = diag * (1 - cy) + to_chip * (cy + direction * (1 - 2 * cy)) + (to_sib + kept) * cy
        tx = diag * (1 - cx) + to_chip * (cx + (1 - direction) * (1 - 2 * cx)) + (to_sib + kept) * cx
        tc = (diag + to_chip) * (i % 2) + to_sib * (1 - c) + kept * c
        k = diag * (i // 2) + to_chip * ((i - SECOND) // 4) + (to_sib + kept) * (i % STEPS)
        return pl.multiple_of((ty * 4 + tx * 2 + tc) * BLOCK + k * ROWS, ROWS)

    def x_copy(i):
        return pltpu.make_async_copy(x_hbm.at[pl.ds(row_of(i), ROWS)], x_buf.at[i % 2], x_sem.at[i % 2])

    early = [pltpu.make_async_copy(src, dst, w_sem.at[n]) for n, (src, dst) in enumerate(((wg_hbm, wg), (wu_hbm, wu), (wd_hbm, wd), (gain_hbm, gain_ref)))]
    for copy in early:
        copy.start()
    x_copy(0).start()

    out_chip = (1 - c) * yn + c * xn

    def w_relay_copy(n):
        rows = (pl.ds(0, 128), pl.ds(128, F - 128))[n]
        return pltpu.make_async_remote_copy(
            src_ref=wd_hbm.at[rows], dst_ref=wd_relay.at[rows], send_sem=wr_sem.at[0, n], recv_sem=wr_sem.at[1, n],
            device_id={"tp": out_chip + 1 - c}, device_id_type=pl.DeviceIdType.MESH)

    def relay_copy(g):
        group = pl.ds(g * GROUP, GROUP)
        return pltpu.make_async_remote_copy(
            src_ref=hid.at[group], dst_ref=hid_in.at[group], send_sem=relay_sem.at[0, g], recv_sem=relay_sem.at[1, g],
            device_id={"tp": out_chip + 1 - c}, device_id_type=pl.DeviceIdType.MESH)

    def sib_copy(slot, group, k):
        to_hbm = isinstance(group, int) and group == 2
        return pltpu.make_async_remote_copy(
            src_ref=tiles.at[slot], dst_ref=sib_own.at[k] if to_hbm else sib_in.at[group, k], send_sem=sib_ssem.at[slot],
            recv_sem=sib_rsem.at[group, k], device_id={"tp": sib}, device_id_type=pl.DeviceIdType.MESH)

    last = STEPS - 1
    parts = ((0, HALF), (HALF, HALF - LATE), (ROWS - LATE, LATE))

    def landing(d, k, part):
        if part is None:
            return sum_in.at[d, k]
        start, rows = parts[part]
        return sum_in.at[d, last, pl.ds(0, HALF)] if part == 0 else sum_last.at[d, pl.ds(start - HALF, rows)]

    def sum_copy(j, k, part=None):
        slot = k % SUM_SLOTS
        return pltpu.make_async_remote_copy(
            src_ref=sum_out.at[j, slot] if part is None else sum_out.at[j, slot, pl.ds(*parts[part])], dst_ref=landing(c, k, part),
            send_sem=sum_ssem.at[j, slot + (part or 0)], recv_sem=sum_rsem.at[c, k + (part or 0)],
            device_id={"tp": out_chip + j}, device_id_type=pl.DeviceIdType.MESH)

    def sum_arrival(d, k, part=None):
        return pltpu.make_async_remote_copy(
            src_ref=landing(d, k, part), dst_ref=landing(d, k, part), send_sem=sum_ssem.at[0, 0], recv_sem=sum_rsem.at[d, k + (part or 0)],
            device_id={"tp": sib}, device_id_type=pl.DeviceIdType.MESH)

    pl.semaphore_wait(barrier, 2)
    for n in range(2):
        w_relay_copy(n).start()
    w_relay_copy(0).wait_recv()
    pl.semaphore_signal(ready, inc=1, device_id={"tp": source}, device_id_type=pl.DeviceIdType.MESH)
    for copy in early:
        copy.wait()

    @pl.loop(0, TILES)
    def _(i):
        diag, to_sib, to_chip, kept = kinds(i)
        j = i % 2
        k_chip = (i - SECOND) // 4
        k_own = i % STEPS
        stays = to_chip * (i % 4 // 2) + kept
        is_relay = i < FIRST
        in_chip = jnp.logical_and(i >= SECOND, i < THIRD)
        is_own_sib = jnp.logical_and(i >= FIRST, i < SECOND)
        is_sib = jnp.logical_and(in_chip, i % 4 < 2)
        is_sum = jnp.logical_and(in_chip, i % 4 >= 2)
        is_final = i >= THIRD

        @pl.when(i + 1 < TILES)
        def _():
            x_copy(i + 1).start()

        x_copy(i).wait()

        @pl.when(jnp.logical_and(jnp.logical_or(is_sib, is_own_sib), i >= FIRST + 2))
        def _():
            sib_copy(j, 0, 0).wait_send()

        def res_copy():
            return pltpu.make_async_copy(res_hbm.at[pl.ds(pl.multiple_of(k_own * ROWS, ROWS), ROWS)], res_ld, w_sem.at[2])

        def sib_load():
            return pltpu.make_async_copy(sib_own.at[k_own], sib_ld, w_sem.at[3])

        def sum_load(d, rows):
            return pltpu.make_async_copy(sum_in.at[d, k_own, pl.ds(0, rows)], sum_ld.at[d, pl.ds(0, rows)], w_sem.at[d])

        late_own = jnp.logical_and(k_own == last, c == 1)

        @pl.when(is_final)
        def _():
            res_copy().start()
            sib_copy(0, 2, k_own).wait_recv()
            sib_load().start()

            @pl.when(jnp.logical_not(late_own))
            def _():
                for d in range(2):
                    sum_arrival(d, k_own).wait_recv()
                    sum_load(d, ROWS).start()

            @pl.when(late_own)
            def _():
                for d in range(2):
                    sum_arrival(d, last, 0).wait_recv()
                    sum_load(d, HALF).start()

        hid_slot = diag * i + (1 - diag) * FIRST
        for n in range(CHUNKS):
            cols = slice(n * HID_COLS, (n + 1) * HID_COLS)
            gate = jnp.dot(x_buf[j], wg[:, cols], preferred_element_type=jnp.float32)
            up = jnp.dot(x_buf[j], wu[:, cols], preferred_element_type=jnp.float32)
            hid[hid_slot, :, cols] = (gate * jax.nn.sigmoid(gate) * up).astype(jnp.bfloat16)

        @pl.when(jnp.logical_and(is_relay, i % GROUP == GROUP - 1))
        def _():
            relay_copy(i // GROUP).start()

        @pl.when(i >= FIRST)
        def _():
            slot = stays * 2 + (1 - stays) * j
            for n in range(CHUNKS):
                cols = slice(n * OUT_COLS, (n + 1) * OUT_COLS)
                tiles[slot, :, cols] = jnp.dot(hid[FIRST], wd[:, cols], preferred_element_type=jnp.float32).astype(jnp.bfloat16)

        @pl.when(is_sib)
        def _():
            sib_copy(j, j, k_chip).start()

        @pl.when(is_own_sib)
        def _():
            sib_copy(j, 2, k_own).start()

        @pl.when(is_sum)
        def _():
            sib_copy(0, j, k_chip).wait_recv()

            @pl.when((2 * k_chip + j) % GROUP == 0)
            def _():
                relay_copy((2 * k_chip + j) // GROUP).wait_recv()

            @pl.when(i == SECOND + 2)
            def _():
                w_relay_copy(1).wait_recv()
                pl.semaphore_wait(ready, 1)

            @pl.when(k_chip >= SUM_SLOTS)
            def _():
                sum_copy(j, k_chip - SUM_SLOTS).wait_send()

            for n in range(CHUNKS):
                cols = slice(n * OUT_COLS, (n + 1) * OUT_COLS)
                relayed = jnp.dot(hid_in[2 * k_chip + j], wd_relay[:, cols], preferred_element_type=jnp.float32).astype(jnp.bfloat16)
                total = tiles[2, :, cols].astype(jnp.float32) + sib_in[j, k_chip, :, cols].astype(jnp.float32)
                sum_out[j, k_chip % SUM_SLOTS, :, cols] = total + relayed.astype(jnp.float32)

            late = jnp.logical_and(k_chip == last, j == 1)

            @pl.when(jnp.logical_not(late))
            def _():
                sum_copy(j, k_chip).start()

            @pl.when(late)
            def _():
                for part in range(3):
                    sum_copy(1, last, part).start()

        @pl.when(is_final)
        def _():
            res_copy().wait()
            sib_load().wait()

            def finish(start, rows, sums, sums_start):
                @pl.loop(0, rows // 16)
                def _(b):
                    here = pl.ds(pl.multiple_of(sums_start + b * 16, 16), 16)
                    tile = pl.ds(pl.multiple_of(start + b * 16, 16), 16)
                    out = pl.ds(pl.multiple_of(k_own * ROWS + start + b * 16, 16), 16)
                    y_sum = tiles[2, tile].astype(jnp.float32) + sib_ld[tile].astype(jnp.float32)
                    y_sum = y_sum + (sums[0, here] + sums[1, here])
                    h = res_ld[tile].astype(jnp.float32) + y_sum
                    mean_sq = jnp.mean(h * h, axis=-1, keepdims=True)
                    h_ref[out] = h.astype(jnp.bfloat16)
                    n_ref[out] = (h * lax.rsqrt(mean_sq + EPS) * gain_ref[...]).astype(jnp.bfloat16)

            @pl.when(jnp.logical_not(late_own))
            def _():
                for d in range(2):
                    sum_load(d, ROWS).wait()
                finish(0, ROWS, sum_ld, 0)

            @pl.when(late_own)
            def _():
                for d in range(2):
                    sum_load(d, HALF).wait()
                finish(0, HALF, sum_ld, 0)
                for part in (1, 2):
                    for d in range(2):
                        sum_arrival(d, last, part).wait_recv()
                    start, rows = parts[part]
                    finish(start, rows, sum_last, start - HALF)

    for n in range(2):
        w_relay_copy(n).wait_send()
    for g in range(FIRST // GROUP):
        relay_copy(g).wait_send()
    for s in range(2):
        sib_copy(s, 0, 0).wait_send()
    for j in range(2):
        sum_copy(j, last - 1).wait_send()
    sum_copy(0, last).wait_send()
    for part in range(3):
        sum_copy(1, last, part).wait_send()


def store_kernel(h_ref, n_ref, h_hbm, n_hbm, sem):
    for b in range(16):
        rows = pl.ds(b * (BLOCK // 16), BLOCK // 16)
        pltpu.make_async_copy(h_ref.at[rows], h_hbm.at[rows], sem.at[0]).start()
        pltpu.make_async_copy(n_ref.at[rows], n_hbm.at[rows], sem.at[1]).start()
    pltpu.make_async_copy(h_ref, h_hbm, sem.at[0]).wait()
    pltpu.make_async_copy(n_ref, n_hbm, sem.at[1]).wait()


def solution(mesh):
    def local_block(x_in, w_gate, w_up, w_down, residual, norm_gain):
        hbm = pl.BlockSpec(memory_space=pltpu.HBM)
        vmem = pl.BlockSpec(memory_space=pltpu.VMEM)
        h, n, _, _ = pl.pallas_call(
            kernel,
            out_shape=(
                pltpu.VMEM((BLOCK, D), jnp.bfloat16),
                pltpu.VMEM((BLOCK, D), jnp.bfloat16),
                jax.ShapeDtypeStruct((2, STEPS, ROWS, D), jnp.float32),
                jax.ShapeDtypeStruct((STEPS, ROWS, D), jnp.bfloat16),
            ),
            in_specs=[hbm] * 6,
            out_specs=(vmem, vmem, hbm, hbm),
            scratch_shapes=[
                pltpu.VMEM((2, ROWS, D), jnp.bfloat16),
                pltpu.VMEM((D, F), jnp.bfloat16),
                pltpu.VMEM((D, F), jnp.bfloat16),
                pltpu.VMEM((F, D), jnp.bfloat16),
                pltpu.VMEM((F, D), jnp.bfloat16),
                pltpu.VMEM((FIRST + 1, ROWS, F), jnp.bfloat16),
                pltpu.VMEM((3, ROWS, D), jnp.bfloat16),
                pltpu.VMEM((FIRST, ROWS, F), jnp.bfloat16),
                pltpu.VMEM((2, STEPS, ROWS, D), jnp.bfloat16),
                pltpu.VMEM((2, SUM_SLOTS, ROWS, D), jnp.float32),
                pltpu.VMEM((2, HALF, D), jnp.float32),
                pltpu.VMEM((2, ROWS, D), jnp.float32),
                pltpu.VMEM((ROWS, D), jnp.bfloat16),
                pltpu.VMEM((ROWS, D), jnp.bfloat16),
                pltpu.VMEM((1, D), jnp.float32),
                pltpu.SemaphoreType.DMA((2,)),
                pltpu.SemaphoreType.DMA((4,)),
                pltpu.SemaphoreType.DMA((2, 2)),
                pltpu.SemaphoreType.DMA((2, FIRST // GROUP)),
                pltpu.SemaphoreType.DMA((2,)),
                pltpu.SemaphoreType.DMA((3, STEPS)),
                pltpu.SemaphoreType.DMA((2, SUM_SLOTS + 2)),
                pltpu.SemaphoreType.DMA((2, STEPS + 2)),
                pltpu.SemaphoreType.REGULAR,
            ],
            compiler_params=pltpu.CompilerParams(collective_id=0, has_side_effects=True, vmem_limit_bytes=58000000),
            name="mlp_reduce",
        )(x_in, w_gate, w_up, w_down, residual, norm_gain.reshape(1, D))
        return pl.pallas_call(
            store_kernel,
            out_shape=(jax.ShapeDtypeStruct((BLOCK, D), jnp.bfloat16), jax.ShapeDtypeStruct((BLOCK, D), jnp.bfloat16)),
            in_specs=[vmem, vmem],
            out_specs=(hbm, hbm),
            scratch_shapes=[pltpu.SemaphoreType.DMA((2,))],
            compiler_params=pltpu.CompilerParams(vmem_limit_bytes=1048576),
            name="store",
        )(*(pltpu.with_memory_space_constraint(a, pltpu.VMEM) for a in (h, n)))

    row_spec = P(("data", "tp"), None)
    return jax.shard_map(local_block, mesh=mesh, in_specs=(P("data", None), P(None, "tp"), P(None, "tp"), P("tp", None), row_spec, P(None)), out_specs=(row_spec, row_spec), check_vma=False)
```

```python
import functools

import jax
import jax.numpy as jnp
from jax import lax
from jax.experimental import pallas as pl
from jax.experimental.pallas import tpu as pltpu
from jax.sharding import PartitionSpec as P

EPS = 1e-5
ROWS = 256
CHUNKS = 4
HALF = 128
LATE = 16
BLOCK = 1024
STEPS = BLOCK // ROWS
D = 2048
F = 1024
HID_COLS = F // CHUNKS
OUT_COLS = D // CHUNKS
SUM_SLOTS = 2
GROUP = 4
FIRST = 2 * STEPS
SECOND = FIRST + STEPS
THIRD = SECOND + 4 * STEPS
TILES = 8 * STEPS


def kernel(x_hbm, wg_hbm, wu_hbm, wd_hbm, res_hbm, gain_hbm, h_ref, n_ref, sum_in, sib_own, x_buf, wg, wu, wd, wd_relay, hid, tiles, hid_in, sib_in, sum_out, sum_last, sum_ld, res_ld, sib_ld, gain_ref,
           x_sem, w_sem, wr_sem, relay_sem, sib_ssem, sib_rsem, sum_ssem, sum_rsem, ready):
    me = lax.axis_index("tp")
    c, cx, cy = me % 2, (me // 2) % 2, me // 4
    sib = cy * 4 + cx * 2 + (1 - c)
    xn = cy * 4 + (1 - cx) * 2
    yn = (1 - cy) * 4 + cx * 2

    barrier = pltpu.get_barrier_semaphore()
    source = (1 - c) * (xn + 1) + c * yn
    for dev in (source, sib):
        pl.semaphore_signal(barrier, inc=1, device_id={"tp": dev}, device_id_type=pl.DeviceIdType.MESH)

    def kinds(i):
        past_first, past_second, past_third = (i + TILES - FIRST) // TILES, (i + TILES - SECOND) // TILES, (i + TILES - THIRD) // TILES
        return 1 - past_first, past_first - past_second, past_second - past_third, past_third

    def row_of(i):
        diag, to_sib, to_chip, kept = kinds(i)
        q = i % 4
        direction = c + (q // 2) * (1 - 2 * c)
        ty = diag * (1 - cy) + to_chip * (cy + direction * (1 - 2 * cy)) + (to_sib + kept) * cy
        tx = diag * (1 - cx) + to_chip * (cx + (1 - direction) * (1 - 2 * cx)) + (to_sib + kept) * cx
        tc = (diag + to_chip) * (i % 2) + to_sib * (1 - c) + kept * c
        k = diag * (i // 2) + to_chip * ((i - SECOND) // 4) + (to_sib + kept) * (i % STEPS)
        return pl.multiple_of((ty * 4 + tx * 2 + tc) * BLOCK + k * ROWS, ROWS)

    def x_copy(i):
        return pltpu.make_async_copy(x_hbm.at[pl.ds(row_of(i), ROWS)], x_buf.at[i % 2], x_sem.at[i % 2])

    early = [pltpu.make_async_copy(src, dst, w_sem.at[n]) for n, (src, dst) in enumerate(((wg_hbm, wg), (wu_hbm, wu), (wd_hbm, wd), (gain_hbm, gain_ref)))]
    for copy in early:
        copy.start()
    x_copy(0).start()

    out_chip = (1 - c) * yn + c * xn

    def w_relay_copy(n):
        rows = (pl.ds(0, 128), pl.ds(128, F - 128))[n]
        return pltpu.make_async_remote_copy(
            src_ref=wd_hbm.at[rows], dst_ref=wd_relay.at[rows], send_sem=wr_sem.at[0, n], recv_sem=wr_sem.at[1, n],
            device_id={"tp": out_chip + 1 - c}, device_id_type=pl.DeviceIdType.MESH)

    def relay_copy(g):
        group = pl.ds(g * GROUP, GROUP)
        return pltpu.make_async_remote_copy(
            src_ref=hid.at[group], dst_ref=hid_in.at[group], send_sem=relay_sem.at[0, g], recv_sem=relay_sem.at[1, g],
            device_id={"tp": out_chip + 1 - c}, device_id_type=pl.DeviceIdType.MESH)

    def sib_copy(slot, group, k):
        to_hbm = isinstance(group, int) and group == 2
        return pltpu.make_async_remote_copy(
            src_ref=tiles.at[slot], dst_ref=sib_own.at[k] if to_hbm else sib_in.at[group, k], send_sem=sib_ssem.at[slot],
            recv_sem=sib_rsem.at[group, k], device_id={"tp": sib}, device_id_type=pl.DeviceIdType.MESH)

    last = STEPS - 1
    parts = ((0, HALF), (HALF, HALF - LATE), (ROWS - LATE, LATE))

    def landing(d, k, part):
        if part is None:
            return sum_in.at[d, k]
        start, rows = parts[part]
        return sum_in.at[d, last, pl.ds(0, HALF)] if part == 0 else sum_last.at[d, pl.ds(start - HALF, rows)]

    def sum_copy(j, k, part=None):
        slot = k % SUM_SLOTS
        return pltpu.make_async_remote_copy(
            src_ref=sum_out.at[j, slot] if part is None else sum_out.at[j, slot, pl.ds(*parts[part])], dst_ref=landing(c, k, part),
            send_sem=sum_ssem.at[j * SUM_SLOTS + slot + (part or 0)], recv_sem=sum_rsem.at[c, k + (part or 0)],
            device_id={"tp": out_chip + j}, device_id_type=pl.DeviceIdType.MESH)

    def sum_arrival(d, k, part=None):
        return pltpu.make_async_remote_copy(
            src_ref=landing(d, k, part), dst_ref=landing(d, k, part), send_sem=sum_ssem.at[0], recv_sem=sum_rsem.at[d, k + (part or 0)],
            device_id={"tp": sib}, device_id_type=pl.DeviceIdType.MESH)

    pl.semaphore_wait(barrier, 2)
    for n in range(2):
        w_relay_copy(n).start()
    w_relay_copy(0).wait_recv()
    pl.semaphore_signal(ready, inc=1, device_id={"tp": source}, device_id_type=pl.DeviceIdType.MESH)
    for copy in early:
        copy.wait()

    @pl.loop(0, TILES)
    def _(i):
        diag, to_sib, to_chip, kept = kinds(i)
        j = i % 2
        k_chip = (i - SECOND) // 4
        k_own = i % STEPS
        stays = to_chip * (i % 4 // 2) + kept
        is_relay = i < FIRST
        in_chip = jnp.logical_and(i >= SECOND, i < THIRD)
        is_own_sib = jnp.logical_and(i >= FIRST, i < SECOND)
        is_sib = jnp.logical_and(in_chip, i % 4 < 2)
        is_sum = jnp.logical_and(in_chip, i % 4 >= 2)
        is_final = i >= THIRD

        @pl.when(i + 1 < TILES)
        def _():
            x_copy(i + 1).start()

        x_copy(i).wait()

        @pl.when(jnp.logical_and(jnp.logical_or(is_sib, is_own_sib), i >= FIRST + 2))
        def _():
            sib_copy(j, 0, 0).wait_send()

        def res_copy():
            return pltpu.make_async_copy(res_hbm.at[pl.ds(pl.multiple_of(k_own * ROWS, ROWS), ROWS)], res_ld, w_sem.at[2])

        def sib_load():
            return pltpu.make_async_copy(sib_own.at[k_own], sib_ld, w_sem.at[3])

        def sum_load(d, rows):
            return pltpu.make_async_copy(sum_in.at[d, k_own, pl.ds(0, rows)], sum_ld.at[d, pl.ds(0, rows)], w_sem.at[d])

        late_own = jnp.logical_and(k_own == last, c == 1)

        @pl.when(is_final)
        def _():
            res_copy().start()
            sib_copy(0, 2, k_own).wait_recv()
            sib_load().start()

            @pl.when(jnp.logical_not(late_own))
            def _():
                for d in range(2):
                    sum_arrival(d, k_own).wait_recv()
                    sum_load(d, ROWS).start()

            @pl.when(late_own)
            def _():
                for d in range(2):
                    sum_arrival(d, last, 0).wait_recv()
                    sum_load(d, HALF).start()

        hid_slot = diag * i + (1 - diag) * FIRST
        for n in range(CHUNKS):
            cols = slice(n * HID_COLS, (n + 1) * HID_COLS)
            gate = jnp.dot(x_buf[j], wg[:, cols], preferred_element_type=jnp.float32)
            up = jnp.dot(x_buf[j], wu[:, cols], preferred_element_type=jnp.float32)
            hid[hid_slot, :, cols] = (gate * jax.nn.sigmoid(gate) * up).astype(jnp.bfloat16)

        @pl.when(jnp.logical_and(is_relay, i % GROUP == GROUP - 1))
        def _():
            relay_copy(i // GROUP).start()

        @pl.when(i >= FIRST)
        def _():
            slot = stays * 2 + (1 - stays) * j
            for n in range(CHUNKS):
                cols = slice(n * OUT_COLS, (n + 1) * OUT_COLS)
                tiles[slot, :, cols] = jnp.dot(hid[FIRST], wd[:, cols], preferred_element_type=jnp.float32).astype(jnp.bfloat16)

        @pl.when(is_sib)
        def _():
            sib_copy(j, j, k_chip).start()

        @pl.when(is_own_sib)
        def _():
            sib_copy(j, 2, k_own).start()

        @pl.when(is_sum)
        def _():
            sib_copy(0, j, k_chip).wait_recv()

            @pl.when((2 * k_chip + j) % GROUP == 0)
            def _():
                relay_copy((2 * k_chip + j) // GROUP).wait_recv()

            @pl.when(i == SECOND + 2)
            def _():
                w_relay_copy(1).wait_recv()
                pl.semaphore_wait(ready, 1)

            @pl.when(k_chip >= SUM_SLOTS)
            def _():
                sum_copy(j, k_chip - SUM_SLOTS).wait_send()

            for n in range(CHUNKS):
                cols = slice(n * OUT_COLS, (n + 1) * OUT_COLS)
                relayed = jnp.dot(hid_in[2 * k_chip + j], wd_relay[:, cols], preferred_element_type=jnp.float32).astype(jnp.bfloat16)
                total = tiles[2, :, cols].astype(jnp.float32) + sib_in[j, k_chip, :, cols].astype(jnp.float32)
                sum_out[j, k_chip % SUM_SLOTS, :, cols] = total + relayed.astype(jnp.float32)

            late = jnp.logical_and(k_chip == last, j == 1)

            @pl.when(jnp.logical_not(late))
            def _():
                sum_copy(j, k_chip).start()

            @pl.when(late)
            def _():
                for part in range(3):
                    sum_copy(1, last, part).start()

        @pl.when(is_final)
        def _():
            res_copy().wait()
            sib_load().wait()

            def finish(start, rows, sums, sums_start):
                @pl.loop(0, rows // 16)
                def _(b):
                    here = pl.ds(pl.multiple_of(sums_start + b * 16, 16), 16)
                    tile = pl.ds(pl.multiple_of(start + b * 16, 16), 16)
                    out = pl.ds(pl.multiple_of(k_own * ROWS + start + b * 16, 16), 16)
                    y_sum = tiles[2, tile].astype(jnp.float32) + sib_ld[tile].astype(jnp.float32)
                    y_sum = y_sum + (sums[0, here] + sums[1, here])
                    h = res_ld[tile].astype(jnp.float32) + y_sum
                    mean_sq = jnp.mean(h * h, axis=-1, keepdims=True)
                    h_ref[out] = h.astype(jnp.bfloat16)
                    n_ref[out] = (h * lax.rsqrt(mean_sq + EPS) * gain_ref[...]).astype(jnp.bfloat16)

            @pl.when(jnp.logical_not(late_own))
            def _():
                for d in range(2):
                    sum_load(d, ROWS).wait()
                finish(0, ROWS, sum_ld, 0)

            @pl.when(late_own)
            def _():
                for d in range(2):
                    sum_load(d, HALF).wait()
                finish(0, HALF, sum_ld, 0)
                for part in (1, 2):
                    for d in range(2):
                        sum_arrival(d, last, part).wait_recv()
                    start, rows = parts[part]
                    finish(start, rows, sum_last, start - HALF)

    for n in range(2):
        w_relay_copy(n).wait_send()
    for g in range(FIRST // GROUP):
        relay_copy(g).wait_send()
    for s in range(2):
        sib_copy(s, 0, 0).wait_send()
    for j in range(2):
        sum_copy(j, last - 1).wait_send()
    sum_copy(0, last).wait_send()
    for part in range(3):
        sum_copy(1, last, part).wait_send()


def store_kernel(h_ref, n_ref, h_hbm, n_hbm, sem):
    for b in range(32):
        rows = pl.ds(b * (BLOCK // 32), BLOCK // 32)
        pltpu.make_async_copy(h_ref.at[rows], h_hbm.at[rows], sem.at[0]).start()
        pltpu.make_async_copy(n_ref.at[rows], n_hbm.at[rows], sem.at[1]).start()
    pltpu.make_async_copy(h_ref, h_hbm, sem.at[0]).wait()
    pltpu.make_async_copy(n_ref, n_hbm, sem.at[1]).wait()


def solution(mesh):
    def local_block(x_in, w_gate, w_up, w_down, residual, norm_gain):
        hbm = pl.BlockSpec(memory_space=pltpu.HBM)
        vmem = pl.BlockSpec(memory_space=pltpu.VMEM)
        h, n, _, _ = pl.pallas_call(
            kernel,
            out_shape=(
                pltpu.VMEM((BLOCK, D), jnp.bfloat16),
                pltpu.VMEM((BLOCK, D), jnp.bfloat16),
                jax.ShapeDtypeStruct((2, STEPS, ROWS, D), jnp.float32),
                jax.ShapeDtypeStruct((STEPS, ROWS, D), jnp.bfloat16),
            ),
            in_specs=[hbm] * 6,
            out_specs=(vmem, vmem, hbm, hbm),
            scratch_shapes=[
                pltpu.VMEM((2, ROWS, D), jnp.bfloat16),
                pltpu.VMEM((D, F), jnp.bfloat16),
                pltpu.VMEM((D, F), jnp.bfloat16),
                pltpu.VMEM((F, D), jnp.bfloat16),
                pltpu.VMEM((F, D), jnp.bfloat16),
                pltpu.VMEM((FIRST + 1, ROWS, F), jnp.bfloat16),
                pltpu.VMEM((3, ROWS, D), jnp.bfloat16),
                pltpu.VMEM((FIRST, ROWS, F), jnp.bfloat16),
                pltpu.VMEM((2, STEPS, ROWS, D), jnp.bfloat16),
                pltpu.VMEM((2, SUM_SLOTS, ROWS, D), jnp.float32),
                pltpu.VMEM((2, HALF, D), jnp.float32),
                pltpu.VMEM((2, ROWS, D), jnp.float32),
                pltpu.VMEM((ROWS, D), jnp.bfloat16),
                pltpu.VMEM((ROWS, D), jnp.bfloat16),
                pltpu.VMEM((1, D), jnp.float32),
                pltpu.SemaphoreType.DMA((2,)),
                pltpu.SemaphoreType.DMA((4,)),
                pltpu.SemaphoreType.DMA((2, 2)),
                pltpu.SemaphoreType.DMA((2, FIRST // GROUP)),
                pltpu.SemaphoreType.DMA((2,)),
                pltpu.SemaphoreType.DMA((3, STEPS)),
                pltpu.SemaphoreType.DMA((2 * SUM_SLOTS + 2,)),
                pltpu.SemaphoreType.DMA((2, STEPS + 2)),
                pltpu.SemaphoreType.REGULAR,
            ],
            compiler_params=pltpu.CompilerParams(collective_id=0, has_side_effects=True, vmem_limit_bytes=58000000),
            name="mlp_reduce",
        )(x_in, w_gate, w_up, w_down, residual, norm_gain.reshape(1, D))
        return pl.pallas_call(
            store_kernel,
            out_shape=(jax.ShapeDtypeStruct((BLOCK, D), jnp.bfloat16), jax.ShapeDtypeStruct((BLOCK, D), jnp.bfloat16)),
            in_specs=[vmem, vmem],
            out_specs=(hbm, hbm),
            scratch_shapes=[pltpu.SemaphoreType.DMA((2,))],
            compiler_params=pltpu.CompilerParams(vmem_limit_bytes=1048576),
            name="store",
        )(*(pltpu.with_memory_space_constraint(a, pltpu.VMEM) for a in (h, n)))

    row_spec = P(("data", "tp"), None)
    return jax.shard_map(local_block, mesh=mesh, in_specs=(P("data", None), P(None, "tp"), P(None, "tp"), P("tp", None), row_spec, P(None)), out_specs=(row_spec, row_spec), check_vma=False)
```

```python
import functools

import jax
import jax.numpy as jnp
from jax import lax
from jax.experimental import pallas as pl
from jax.experimental.pallas import tpu as pltpu
from jax.sharding import PartitionSpec as P

EPS = 1e-5
ROWS = 256
CHUNKS = 4
HALF = 128
LATE = 16
BLOCK = 1024
STEPS = BLOCK // ROWS
D = 2048
F = 1024
HID_COLS = F // CHUNKS
OUT_COLS = D // CHUNKS
SUM_SLOTS = 2
GROUP = 4
FIRST = 2 * STEPS
SECOND = FIRST + STEPS
THIRD = SECOND + 4 * STEPS
TILES = 8 * STEPS


def kernel(x_hbm, wg_hbm, wu_hbm, wd_hbm, res_hbm, gain_hbm, h_ref, n_ref, sum_in, sib_own, x_buf, wg, wu, wd, wd_relay, hid, tiles, hid_in, sib_in, sum_out, sum_last, sum_ld, res_ld, sib_ld, gain_ref,
           x_sem, w_sem, wr_sem, relay_sem, sib_ssem, sib_rsem, sum_ssem, sum_rsem, ready):
    me = lax.axis_index("tp")
    c, cx, cy = me % 2, (me // 2) % 2, me // 4
    sib = cy * 4 + cx * 2 + (1 - c)
    xn = cy * 4 + (1 - cx) * 2
    yn = (1 - cy) * 4 + cx * 2

    barrier = pltpu.get_barrier_semaphore()
    source = (1 - c) * (xn + 1) + c * yn
    for dev in (source, sib):
        pl.semaphore_signal(barrier, inc=1, device_id={"tp": dev}, device_id_type=pl.DeviceIdType.MESH)

    def kinds(i):
        past_first, past_second, past_third = (i + TILES - FIRST) // TILES, (i + TILES - SECOND) // TILES, (i + TILES - THIRD) // TILES
        return 1 - past_first, past_first - past_second, past_second - past_third, past_third

    def row_of(i):
        diag, to_sib, to_chip, kept = kinds(i)
        q = i % 4
        direction = c + (q // 2) * (1 - 2 * c)
        ty = diag * (1 - cy) + to_chip * (cy + direction * (1 - 2 * cy)) + (to_sib + kept) * cy
        tx = diag * (1 - cx) + to_chip * (cx + (1 - direction) * (1 - 2 * cx)) + (to_sib + kept) * cx
        tc = (diag + to_chip) * (i % 2) + to_sib * (1 - c) + kept * c
        k = diag * (i // 2) + to_chip * ((i - SECOND) // 4) + (to_sib + kept) * (i % STEPS)
        return pl.multiple_of((ty * 4 + tx * 2 + tc) * BLOCK + k * ROWS, ROWS)

    def x_copy(i):
        return pltpu.make_async_copy(x_hbm.at[pl.ds(row_of(i), ROWS)], x_buf.at[i % 2], x_sem.at[i % 2])

    early = [pltpu.make_async_copy(src, dst, w_sem.at[n]) for n, (src, dst) in enumerate(((wg_hbm, wg), (wu_hbm, wu), (wd_hbm, wd), (gain_hbm, gain_ref)))]
    for copy in early:
        copy.start()
    x_copy(0).start()

    out_chip = (1 - c) * yn + c * xn

    def w_relay_copy(n):
        rows = (pl.ds(0, 128), pl.ds(128, F - 128))[n]
        return pltpu.make_async_remote_copy(
            src_ref=wd_hbm.at[rows], dst_ref=wd_relay.at[rows], send_sem=wr_sem.at[0, n], recv_sem=wr_sem.at[1, n],
            device_id={"tp": out_chip + 1 - c}, device_id_type=pl.DeviceIdType.MESH)

    def relay_copy(g):
        group = pl.ds(g * GROUP, GROUP)
        return pltpu.make_async_remote_copy(
            src_ref=hid.at[group], dst_ref=hid_in.at[group], send_sem=relay_sem.at[0, g], recv_sem=relay_sem.at[1, g],
            device_id={"tp": out_chip + 1 - c}, device_id_type=pl.DeviceIdType.MESH)

    def sib_copy(slot, group, k):
        to_hbm = isinstance(group, int) and group == 2
        return pltpu.make_async_remote_copy(
            src_ref=tiles.at[slot], dst_ref=sib_own.at[k] if to_hbm else sib_in.at[group, k], send_sem=sib_ssem.at[slot],
            recv_sem=sib_rsem.at[group, k], device_id={"tp": sib}, device_id_type=pl.DeviceIdType.MESH)

    last = STEPS - 1
    parts = ((0, HALF), (HALF, HALF - LATE), (ROWS - LATE, LATE))

    def landing(d, k, part):
        if part is None:
            return sum_in.at[d, k]
        start, rows = parts[part]
        return sum_in.at[d, last, pl.ds(0, HALF)] if part == 0 else sum_last.at[d, pl.ds(start - HALF, rows)]

    def sum_copy(j, k, part=None):
        slot = k % SUM_SLOTS
        return pltpu.make_async_remote_copy(
            src_ref=sum_out.at[j, slot] if part is None else sum_out.at[j, slot, pl.ds(*parts[part])], dst_ref=landing(c, k, part),
            send_sem=sum_ssem.at[j * SUM_SLOTS + slot + (part or 0)], recv_sem=sum_rsem.at[c, k + (part or 0)],
            device_id={"tp": out_chip + j}, device_id_type=pl.DeviceIdType.MESH)

    def sum_arrival(d, k, part=None):
        return pltpu.make_async_remote_copy(
            src_ref=landing(d, k, part), dst_ref=landing(d, k, part), send_sem=sum_ssem.at[0], recv_sem=sum_rsem.at[d, k + (part or 0)],
            device_id={"tp": sib}, device_id_type=pl.DeviceIdType.MESH)

    pl.semaphore_wait(barrier, 2)
    for n in range(2):
        w_relay_copy(n).start()
    w_relay_copy(0).wait_recv()
    pl.semaphore_signal(ready, inc=1, device_id={"tp": source}, device_id_type=pl.DeviceIdType.MESH)
    for copy in early:
        copy.wait()

    @pl.loop(0, TILES)
    def _(i):
        diag, to_sib, to_chip, kept = kinds(i)
        j = i % 2
        k_chip = (i - SECOND) // 4
        k_own = i % STEPS
        stays = to_chip * (i % 4 // 2) + kept
        is_relay = i < FIRST
        in_chip = jnp.logical_and(i >= SECOND, i < THIRD)
        is_own_sib = jnp.logical_and(i >= FIRST, i < SECOND)
        is_sib = jnp.logical_and(in_chip, i % 4 < 2)
        is_sum = jnp.logical_and(in_chip, i % 4 >= 2)
        is_final = i >= THIRD

        @pl.when(i + 1 < TILES)
        def _():
            x_copy(i + 1).start()

        x_copy(i).wait()

        @pl.when(jnp.logical_and(jnp.logical_or(is_sib, is_own_sib), i >= FIRST + 2))
        def _():
            sib_copy(j, 0, 0).wait_send()

        def res_copy():
            return pltpu.make_async_copy(res_hbm.at[pl.ds(pl.multiple_of(k_own * ROWS, ROWS), ROWS)], res_ld, w_sem.at[2])

        def sib_load():
            return pltpu.make_async_copy(sib_own.at[k_own], sib_ld, w_sem.at[3])

        def sum_load(d, rows):
            return pltpu.make_async_copy(sum_in.at[d, k_own, pl.ds(0, rows)], sum_ld.at[d, pl.ds(0, rows)], w_sem.at[d])

        late_own = jnp.logical_and(k_own == last, c == 1)

        @pl.when(is_final)
        def _():
            res_copy().start()
            sib_copy(0, 2, k_own).wait_recv()
            sib_load().start()

            @pl.when(jnp.logical_not(late_own))
            def _():
                for d in range(2):
                    sum_arrival(d, k_own).wait_recv()
                    sum_load(d, ROWS).start()

            @pl.when(late_own)
            def _():
                for d in range(2):
                    sum_arrival(d, last, 0).wait_recv()
                    sum_load(d, HALF).start()

        hid_slot = diag * i + (1 - diag) * FIRST
        for n in range(CHUNKS):
            cols = slice(n * HID_COLS, (n + 1) * HID_COLS)
            gate = jnp.dot(x_buf[j], wg[:, cols], preferred_element_type=jnp.float32)
            up = jnp.dot(x_buf[j], wu[:, cols], preferred_element_type=jnp.float32)
            hid[hid_slot, :, cols] = (gate * jax.nn.sigmoid(gate) * up).astype(jnp.bfloat16)

        @pl.when(jnp.logical_and(is_relay, i % GROUP == GROUP - 1))
        def _():
            relay_copy(i // GROUP).start()

        @pl.when(i >= FIRST)
        def _():
            slot = stays * 2 + (1 - stays) * j
            for n in range(CHUNKS):
                cols = slice(n * OUT_COLS, (n + 1) * OUT_COLS)
                tiles[slot, :, cols] = jnp.dot(hid[FIRST], wd[:, cols], preferred_element_type=jnp.float32).astype(jnp.bfloat16)

        @pl.when(is_sib)
        def _():
            sib_copy(j, j, k_chip).start()

        @pl.when(is_own_sib)
        def _():
            sib_copy(j, 2, k_own).start()

        @pl.when(is_sum)
        def _():
            sib_copy(0, j, k_chip).wait_recv()

            @pl.when((2 * k_chip + j) % GROUP == 0)
            def _():
                relay_copy((2 * k_chip + j) // GROUP).wait_recv()

            @pl.when(i == SECOND + 2)
            def _():
                w_relay_copy(1).wait_recv()
                pl.semaphore_wait(ready, 1)

            @pl.when(k_chip >= SUM_SLOTS)
            def _():
                sum_copy(j, k_chip - SUM_SLOTS).wait_send()

            for n in range(CHUNKS):
                cols = slice(n * OUT_COLS, (n + 1) * OUT_COLS)
                relayed = jnp.dot(hid_in[2 * k_chip + j], wd_relay[:, cols], preferred_element_type=jnp.float32).astype(jnp.bfloat16)
                total = tiles[2, :, cols].astype(jnp.float32) + sib_in[j, k_chip, :, cols].astype(jnp.float32)
                sum_out[j, k_chip % SUM_SLOTS, :, cols] = total + relayed.astype(jnp.float32)

            late = jnp.logical_and(k_chip == last, j == 1)

            @pl.when(jnp.logical_not(late))
            def _():
                sum_copy(j, k_chip).start()

            @pl.when(late)
            def _():
                for part in range(3):
                    sum_copy(1, last, part).start()

        @pl.when(is_final)
        def _():
            res_copy().wait()
            sib_load().wait()

            def finish(start, rows, sums, sums_start):
                @pl.loop(0, rows // 16)
                def _(b):
                    here = pl.ds(pl.multiple_of(sums_start + b * 16, 16), 16)
                    tile = pl.ds(pl.multiple_of(start + b * 16, 16), 16)
                    out = pl.ds(pl.multiple_of(k_own * ROWS + start + b * 16, 16), 16)
                    y_sum = tiles[2, tile].astype(jnp.float32) + sib_ld[tile].astype(jnp.float32)
                    y_sum = y_sum + (sums[0, here] + sums[1, here])
                    h = res_ld[tile].astype(jnp.float32) + y_sum
                    mean_sq = jnp.mean(h * h, axis=-1, keepdims=True)
                    h_ref[out] = h.astype(jnp.bfloat16)
                    n_ref[out] = (h * lax.rsqrt(mean_sq + EPS) * gain_ref[...]).astype(jnp.bfloat16)

            @pl.when(jnp.logical_not(late_own))
            def _():
                for d in range(2):
                    sum_load(d, ROWS).wait()
                finish(0, ROWS, sum_ld, 0)

            @pl.when(late_own)
            def _():
                for d in range(2):
                    sum_load(d, HALF).wait()
                finish(0, HALF, sum_ld, 0)
                for part in (1, 2):
                    for d in range(2):
                        sum_arrival(d, last, part).wait_recv()
                    start, rows = parts[part]
                    finish(start, rows, sum_last, start - HALF)

    for n in range(2):
        w_relay_copy(n).wait_send()
    for g in range(FIRST // GROUP):
        relay_copy(g).wait_send()
    for s in range(2):
        sib_copy(s, 0, 0).wait_send()
    for j in range(2):
        sum_copy(j, last - 1).wait_send()
    sum_copy(0, last).wait_send()
    for part in range(3):
        sum_copy(1, last, part).wait_send()


def store_kernel(h_ref, n_ref, h_hbm, n_hbm, sem):
    for b in range(64):
        rows = pl.ds(b * (BLOCK // 64), BLOCK // 64)
        pltpu.make_async_copy(h_ref.at[rows], h_hbm.at[rows], sem.at[0]).start()
        pltpu.make_async_copy(n_ref.at[rows], n_hbm.at[rows], sem.at[1]).start()
    pltpu.make_async_copy(h_ref, h_hbm, sem.at[0]).wait()
    pltpu.make_async_copy(n_ref, n_hbm, sem.at[1]).wait()


def solution(mesh):
    def local_block(x_in, w_gate, w_up, w_down, residual, norm_gain):
        hbm = pl.BlockSpec(memory_space=pltpu.HBM)
        vmem = pl.BlockSpec(memory_space=pltpu.VMEM)
        h, n, _, _ = pl.pallas_call(
            kernel,
            out_shape=(
                pltpu.VMEM((BLOCK, D), jnp.bfloat16),
                pltpu.VMEM((BLOCK, D), jnp.bfloat16),
                jax.ShapeDtypeStruct((2, STEPS, ROWS, D), jnp.float32),
                jax.ShapeDtypeStruct((STEPS, ROWS, D), jnp.bfloat16),
            ),
            in_specs=[hbm] * 6,
            out_specs=(vmem, vmem, hbm, hbm),
            scratch_shapes=[
                pltpu.VMEM((2, ROWS, D), jnp.bfloat16),
                pltpu.VMEM((D, F), jnp.bfloat16),
                pltpu.VMEM((D, F), jnp.bfloat16),
                pltpu.VMEM((F, D), jnp.bfloat16),
                pltpu.VMEM((F, D), jnp.bfloat16),
                pltpu.VMEM((FIRST + 1, ROWS, F), jnp.bfloat16),
                pltpu.VMEM((3, ROWS, D), jnp.bfloat16),
                pltpu.VMEM((FIRST, ROWS, F), jnp.bfloat16),
                pltpu.VMEM((2, STEPS, ROWS, D), jnp.bfloat16),
                pltpu.VMEM((2, SUM_SLOTS, ROWS, D), jnp.float32),
                pltpu.VMEM((2, HALF, D), jnp.float32),
                pltpu.VMEM((2, ROWS, D), jnp.float32),
                pltpu.VMEM((ROWS, D), jnp.bfloat16),
                pltpu.VMEM((ROWS, D), jnp.bfloat16),
                pltpu.VMEM((1, D), jnp.float32),
                pltpu.SemaphoreType.DMA((2,)),
                pltpu.SemaphoreType.DMA((4,)),
                pltpu.SemaphoreType.DMA((2, 2)),
                pltpu.SemaphoreType.DMA((2, FIRST // GROUP)),
                pltpu.SemaphoreType.DMA((2,)),
                pltpu.SemaphoreType.DMA((3, STEPS)),
                pltpu.SemaphoreType.DMA((2 * SUM_SLOTS + 2,)),
                pltpu.SemaphoreType.DMA((2, STEPS + 2)),
                pltpu.SemaphoreType.REGULAR,
            ],
            compiler_params=pltpu.CompilerParams(collective_id=0, has_side_effects=True, vmem_limit_bytes=58000000),
            name="mlp_reduce",
        )(x_in, w_gate, w_up, w_down, residual, norm_gain.reshape(1, D))
        return pl.pallas_call(
            store_kernel,
            out_shape=(jax.ShapeDtypeStruct((BLOCK, D), jnp.bfloat16), jax.ShapeDtypeStruct((BLOCK, D), jnp.bfloat16)),
            in_specs=[vmem, vmem],
            out_specs=(hbm, hbm),
            scratch_shapes=[pltpu.SemaphoreType.DMA((2,))],
            compiler_params=pltpu.CompilerParams(vmem_limit_bytes=1048576),
            name="store",
        )(*(pltpu.with_memory_space_constraint(a, pltpu.VMEM) for a in (h, n)))

    row_spec = P(("data", "tp"), None)
    return jax.shard_map(local_block, mesh=mesh, in_specs=(P("data", None), P(None, "tp"), P(None, "tp"), P("tp", None), row_spec, P(None)), out_specs=(row_spec, row_spec), check_vma=False)
```
